16 devices in a mesh: dp: 4 (over z, y), tp: 4 (over x, core).
Axes of the slice: x: 2, y: 2, z: 2, core: 2. Of those that a mesh axis runs over, the one named last changes fastest.
Arguments:
- y_one: float32 [16, 256, 768], P('dp'), parts along dimension 0
- y_two: float32 [16, 256, 768], P('dp'), parts along dimension 0
- dy_one: float32 [16, 256, 768], P('dp'), parts along dimension 0
- dy_two: float32 [16, 256, 768], P('dp'), parts along dimension 0
- saved_one: float32 [4, 16, 256, 768], P(None, 'dp'), parts along dimension 1
- saved_two: float32 [4, 16, 256, 768], P(None, 'dp'), parts along dimension 1
- w_qkv: bfloat16 [9, 768, 3, 12, 64], P(None, None, None, 'tp')
- w_o: bfloat16 [9, 12, 64, 768], P(None, 'tp')
- w_in: bfloat16 [9, 768, 3072], P(None, None, 'tp')
- w_out: bfloat16 [9, 3072, 768], P(None, 'tp')
Outputs:
- output 1: float32 [16, 256, 768], P('dp'), parts along dimension 0
- output 2: float32 [16, 256, 768], P('dp'), parts along dimension 0
- output 3: float32 [16, 256, 768], P('dp'), parts along dimension 0
- output 4: float32 [16, 256, 768], P('dp'), parts along dimension 0
- output 5: float32 [36, 768, 3, 12, 64], P('dp', None, None, 'tp'), parts along dimension 0
- output 6: float32 [36, 12, 64, 768], P('dp', 'tp'), parts along dimension 0
- output 7: float32 [36, 768, 3072], P('dp', None, 'tp'), parts along dimension 0
- output 8: float32 [36, 3072, 768], P('dp', 'tp'), parts along dimension 0
There are 4 independent parts. The reference program is written for one: setup_inputs(seed, part) draws one part's arguments, and reference() takes and returns one part's arrays. A program takes and returns all parts, laid end to end along the dimension named above; an argument that names none is the same for every part.
All inputs are finite; a program needn't handle non-finite values.
Results may differ from the reference program's by a relative error of at most 0.0148571.
Values are sent between devices in bfloat16 or wider.
A program may use at most 1 GiB of HBM per device.

```python
import jax
import jax.numpy as jnp
from jax import lax

SEQS = 4
SEQ = 256
HIDDEN = 768
HEADS = 12
FF = 3072
PAIRS = 4

LAYERS = 2 * PAIRS + 1
HEAD = HIDDEN // HEADS
EPS = 1e-6


def setup_inputs(seed: int = 0, part: int = 0) -> dict:
    base_keys = jax.random.split(jax.random.key(seed), 2)
    act_keys = jax.random.split(jax.random.fold_in(base_keys[0], part), 6)
    w_keys = jax.random.split(base_keys[1], 4)
    state_shape = (SEQS, SEQ, HIDDEN)
    saved_shape = (PAIRS, SEQS, SEQ, HIDDEN)
    qk_gain = jnp.array([2.0 ** 0.5, 2.0 ** 0.5, 1.0], jnp.float32).reshape(1, 1, 3, 1, 1)
    wo_gain = 0.3 * (SEQ / 55.0) ** 0.5
    w_qkv = jax.random.normal(w_keys[0], (LAYERS, HIDDEN, 3, HEADS, HEAD), jnp.float32) * (HIDDEN ** -0.5) * qk_gain
    w_o = jax.random.normal(w_keys[1], (LAYERS, HEADS, HEAD, HIDDEN), jnp.float32) * (HIDDEN ** -0.5 * wo_gain)
    w_in = jax.random.normal(w_keys[2], (LAYERS, HIDDEN, FF), jnp.float32) * (HIDDEN ** -0.5)
    w_out = jax.random.normal(w_keys[3], (LAYERS, FF, HIDDEN), jnp.float32) * (0.45 * FF ** -0.5)
    return {
        "y_one": jax.random.normal(act_keys[0], state_shape, jnp.float32),
        "y_two": jax.random.normal(act_keys[1], state_shape, jnp.float32),
        "dy_one": jax.random.normal(act_keys[2], state_shape, jnp.float32),
        "dy_two": jax.random.normal(act_keys[3], state_shape, jnp.float32),
        "saved_one": jax.random.normal(act_keys[4], saved_shape, jnp.float32),
        "saved_two": jax.random.normal(act_keys[5], saved_shape, jnp.float32),
        "w_qkv": w_qkv.astype(jnp.bfloat16),
        "w_o": w_o.astype(jnp.bfloat16),
        "w_in": w_in.astype(jnp.bfloat16),
        "w_out": w_out.astype(jnp.bfloat16),
    }


def rms_norm(state):
    return state * lax.rsqrt(jnp.mean(state * state, axis=-1, keepdims=True) + EPS)


def to_bf(values):
    return values.astype(jnp.bfloat16).astype(jnp.float32)


def attend_one(qkv_one):
    q_one, k_one, v_one = qkv_one
    scores = jnp.einsum("qne,kne->nqk", q_one, k_one) * HEAD ** -0.5
    attn_probs = jax.nn.softmax(scores, axis=-1)
    return jnp.einsum("nqk,kne->qne", to_bf(attn_probs), v_one)


def branch_f(state, w_qkv, w_o):
    normed = to_bf(rms_norm(state))
    qkv_all = to_bf(jnp.einsum("bsh,hkne->kbsne", normed, w_qkv))
    heads_out = lax.map(jax.checkpoint(attend_one), (qkv_all[0], qkv_all[1], qkv_all[2]))
    return jnp.einsum("bsne,neh->bsh", to_bf(heads_out), w_o)


def branch_g(state, w_in, w_out):
    normed = to_bf(rms_norm(state))
    hidden = jnp.einsum("bsh,hf->bsf", normed, w_in)
    return jnp.einsum("bsf,fh->bsh", to_bf(jax.nn.gelu(hidden, approximate=True)), w_out)


def reversible_back(block_w, y_one, y_two, d_one, d_two):
    w_qkv, w_o, w_in, w_out = block_w
    g_val, g_pull = jax.vjp(branch_g, y_one, w_in, w_out)
    x_two = y_two - g_val
    g_dx, g_win, g_wout = g_pull(d_two)
    d_one = d_one + g_dx
    f_val, f_pull = jax.vjp(branch_f, x_two, w_qkv, w_o)
    x_one = y_one - f_val
    f_dx, f_wqkv, f_wo = f_pull(d_one)
    return x_one, x_two, d_one, d_two + f_dx, (f_wqkv, f_wo, g_win, g_wout)


def plain_back(block_w, x_one, x_two, d_one, d_two):
    w_qkv, w_o, w_in, w_out = block_w
    f_pull = jax.vjp(branch_f, x_two, w_qkv, w_o)[1]
    f_dx, f_wqkv, f_wo = f_pull(d_one)
    g_pull = jax.vjp(branch_g, x_one, w_in, w_out)[1]
    g_dx, g_win, g_wout = g_pull(d_two)
    return d_one + g_dx, d_two + f_dx, (f_wqkv, f_wo, g_win, g_wout)


def reference(y_one, y_two, dy_one, dy_two, saved_one, saved_two, w_qkv, w_o, w_in, w_out):
    weights = tuple(weight.astype(jnp.float32) for weight in (w_qkv, w_o, w_in, w_out))
    top_w = tuple(weight[LAYERS - 1] for weight in weights)
    x_one, x_two, d_one, d_two, top_grads = reversible_back(top_w, y_one, y_two, dy_one, dy_two)
    paired = tuple(weight[: 2 * PAIRS].reshape((PAIRS, 2) + weight.shape[1:]) for weight in weights)
    rev_w = tuple(weight[:, 0] for weight in paired)
    plain_w = tuple(weight[:, 1] for weight in paired)

    def pair_step(carry_in, scan_in):
        rev_block_w, plain_block_w, s_one, s_two = scan_in
        d_mid_one, d_mid_two, plain_grads = plain_back(plain_block_w, s_one, s_two, carry_in[2], carry_in[3])
        carry_out = reversible_back(rev_block_w, s_one, s_two, d_mid_one, d_mid_two)
        return carry_out[:4], (carry_out[4], plain_grads)

    final_state, scan_grads = lax.scan(pair_step, (x_one, x_two, d_one, d_two), (rev_w, plain_w, saved_one, saved_two), reverse=True)
    grad_out = tuple(
        jnp.concatenate([jnp.stack([rev_g, plain_g], axis=1).reshape((2 * PAIRS,) + rev_g.shape[1:]), top_g[None]], axis=0)
        for rev_g, plain_g, top_g in zip(scan_grads[0], scan_grads[1], top_grads)
    )
    return (final_state[0], final_state[1], final_state[2], final_state[3], grad_out[0], grad_out[1], grad_out[2], grad_out[3])
```

```python
import jax
import jax.numpy as jnp
from jax import lax
from jax.sharding import PartitionSpec as P

EPS = 1e-6


def rms_norm(state):
    return state * lax.rsqrt(jnp.mean(state * state, axis=-1, keepdims=True) + EPS)


def gelu_tanh(hidden):
    return jax.nn.gelu(hidden, approximate=True)


def attn_forward(normed, w_qkv):
    head_dim = w_qkv.shape[-1]
    qkv_all = jnp.einsum("bsh,hkne->kbsne", normed, w_qkv, preferred_element_type=jnp.float32).astype(jnp.bfloat16)
    scores = jnp.einsum("bqne,bkne->bnqk", qkv_all[0], qkv_all[1], preferred_element_type=jnp.float32) * head_dim ** -0.5
    attn_probs = jax.nn.softmax(scores, axis=-1)
    probs_bf = attn_probs.astype(jnp.bfloat16)
    heads_out = jnp.einsum("bnqk,bkne->bqne", probs_bf, qkv_all[2], preferred_element_type=jnp.float32).astype(jnp.bfloat16)
    return qkv_all, attn_probs, probs_bf, heads_out


def attn_backward(normed, w_qkv, w_o, attn_cache, d_out):
    qkv_all, attn_probs, probs_bf, heads_out = attn_cache
    head_dim = w_qkv.shape[-1]
    d_bf = d_out.astype(jnp.bfloat16)
    d_wo = jnp.einsum("bqne,bqh->neh", heads_out, d_bf, preferred_element_type=jnp.float32)
    d_heads = jnp.einsum("bqh,neh->bqne", d_bf, w_o, preferred_element_type=jnp.float32).astype(jnp.bfloat16)
    d_v = jnp.einsum("bnqk,bqne->bkne", probs_bf, d_heads, preferred_element_type=jnp.float32)
    d_probs = jnp.einsum("bqne,bkne->bnqk", d_heads, qkv_all[2], preferred_element_type=jnp.float32)
    d_scores = attn_probs * (d_probs - jnp.sum(d_probs * attn_probs, axis=-1, keepdims=True)) * head_dim ** -0.5
    ds_bf = d_scores.astype(jnp.bfloat16)
    d_q = jnp.einsum("bnqk,bkne->bqne", ds_bf, qkv_all[1], preferred_element_type=jnp.float32)
    d_k = jnp.einsum("bnqk,bqne->bkne", ds_bf, qkv_all[0], preferred_element_type=jnp.float32)
    d_qkv = jnp.stack([d_q.astype(jnp.bfloat16), d_k.astype(jnp.bfloat16), d_v.astype(jnp.bfloat16)], axis=2)
    d_wqkv = jnp.einsum("bsh,bskne->hkne", normed, d_qkv, preferred_element_type=jnp.float32)
    d_normed = jnp.einsum("bskne,hkne->bsh", d_qkv, w_qkv, preferred_element_type=jnp.float32)
    return d_normed, d_wqkv, d_wo


def mlp_forward(normed, w_in):
    hidden = jnp.einsum("bsh,hf->bsf", normed, w_in, preferred_element_type=jnp.float32)
    gelu_out, gelu_pull = jax.vjp(gelu_tanh, hidden)
    return gelu_out.astype(jnp.bfloat16), gelu_pull


def mlp_backward(normed, w_in, w_out, act_bf, gelu_pull, d_out):
    d_bf = d_out.astype(jnp.bfloat16)
    d_wout = jnp.einsum("bsf,bsh->fh", act_bf, d_bf, preferred_element_type=jnp.float32)
    d_act = jnp.einsum("bsh,fh->bsf", d_bf, w_out, preferred_element_type=jnp.float32)
    d_hidden = gelu_pull(d_act)[0].astype(jnp.bfloat16)
    d_win = jnp.einsum("bsh,bsf->hf", normed, d_hidden, preferred_element_type=jnp.float32)
    d_normed = jnp.einsum("bsf,hf->bsh", d_hidden, w_in, preferred_element_type=jnp.float32)
    return d_normed, d_win, d_wout


def reversible_block(block_w, y_one, y_two, d_one, d_two, want_x_one):
    w_qkv, w_o, w_in, w_out = block_w
    g_norm, g_norm_pull = jax.vjp(rms_norm, y_one)
    g_in = g_norm.astype(jnp.bfloat16)
    act_bf, gelu_pull = mlp_forward(g_in, w_in)
    g_part = jnp.einsum("bsf,fh->bsh", act_bf, w_out, preferred_element_type=jnp.float32)
    x_two = y_two - lax.psum(g_part, "tp")
    g_back, d_win, d_wout = mlp_backward(g_in, w_in, w_out, act_bf, gelu_pull, d_two)
    d_one = d_one + g_norm_pull(lax.psum(g_back.astype(jnp.bfloat16), "tp").astype(jnp.float32))[0]
    f_norm, f_norm_pull = jax.vjp(rms_norm, x_two)
    f_in = f_norm.astype(jnp.bfloat16)
    attn_cache = attn_forward(f_in, w_qkv)
    x_one = None
    if want_x_one:
        f_part = jnp.einsum("bqne,neh->bqh", attn_cache[3], w_o, preferred_element_type=jnp.float32)
        x_one = y_one - lax.psum(f_part, "tp")
    f_back, d_wqkv, d_wo = attn_backward(f_in, w_qkv, w_o, attn_cache, d_one)
    d_two = d_two + f_norm_pull(lax.psum(f_back.astype(jnp.bfloat16), "tp").astype(jnp.float32))[0]
    return x_one, x_two, d_one, d_two, (d_wqkv, d_wo, d_win, d_wout)


def plain_block(block_w, x_one, x_two, d_one, d_two):
    w_qkv, w_o, w_in, w_out = block_w
    f_norm, f_norm_pull = jax.vjp(rms_norm, x_two)
    f_in = f_norm.astype(jnp.bfloat16)
    attn_cache = attn_forward(f_in, w_qkv)
    f_back, d_wqkv, d_wo = attn_backward(f_in, w_qkv, w_o, attn_cache, d_one)
    g_norm, g_norm_pull = jax.vjp(rms_norm, x_one)
    g_in = g_norm.astype(jnp.bfloat16)
    act_bf, gelu_pull = mlp_forward(g_in, w_in)
    g_back, d_win, d_wout = mlp_backward(g_in, w_in, w_out, act_bf, gelu_pull, d_two)
    new_one = d_one + g_norm_pull(lax.psum(g_back.astype(jnp.bfloat16), "tp").astype(jnp.float32))[0]
    new_two = d_two + f_norm_pull(lax.psum(f_back.astype(jnp.bfloat16), "tp").astype(jnp.float32))[0]
    return new_one, new_two, (d_wqkv, d_wo, d_win, d_wout)


def solution(mesh):
    act_spec = P("dp", None, None)
    saved_spec = P(None, "dp", None, None)
    weight_specs = (P(None, None, None, "tp", None), P(None, "tp", None, None), P(None, None, "tp"), P(None, "tp", None))
    grad_specs = (P("dp", None, None, "tp", None), P("dp", "tp", None, None), P("dp", None, "tp"), P("dp", "tp", None))

    def per_device(y_one, y_two, dy_one, dy_two, saved_one, saved_two, w_qkv, w_o, w_in, w_out):
        all_w = (w_qkv, w_o, w_in, w_out)
        n_layers = w_qkv.shape[0]
        n_pairs = saved_one.shape[0]
        grad_list = [None] * n_layers
        top_w = tuple(weight[n_layers - 1] for weight in all_w)
        x_one, x_two, d_one, d_two, top_grads = reversible_block(top_w, y_one, y_two, dy_one, dy_two, n_pairs == 0)
        grad_list[n_layers - 1] = top_grads
        for pair_idx in reversed(range(n_pairs)):
            plain_w = tuple(weight[2 * pair_idx + 1] for weight in all_w)
            d_one, d_two, plain_grads = plain_block(plain_w, saved_one[pair_idx], saved_two[pair_idx], d_one, d_two)
            grad_list[2 * pair_idx + 1] = plain_grads
            rev_w = tuple(weight[2 * pair_idx] for weight in all_w)
            x_one, x_two, d_one, d_two, rev_grads = reversible_block(rev_w, saved_one[pair_idx], saved_two[pair_idx], d_one, d_two, pair_idx == 0)
            grad_list[2 * pair_idx] = rev_grads
        stacked = tuple(jnp.stack([entry[slot_idx] for entry in grad_list]) for slot_idx in range(4))
        return (x_one, x_two, d_one, d_two) + stacked

    return jax.shard_map(
        per_device,
        mesh=mesh,
        in_specs=(act_spec,) * 4 + (saved_spec,) * 2 + weight_specs,
        out_specs=(act_spec,) * 4 + grad_specs,
        check_vma=False,
    )
```

```python
import functools

import jax
import jax.numpy as jnp
from jax import lax
from jax.experimental import pallas as pl
from jax.experimental.pallas import tpu as pltpu
from jax.sharding import PartitionSpec as P

EPS = 1e-6
BF = jnp.bfloat16
F32 = jnp.float32
MESH = pl.DeviceIdType.MESH
GELU_C = 0.7978845608028654
GELU_A = 0.044715

NN = (((1,), (0,)), ((), ()))
NT = (((1,), (1,)), ((), ()))
TN = (((0,), (0,)), ((), ()))


def dot(lhs, rhs, dims):
    return lax.dot_general(lhs, rhs, dims, preferred_element_type=F32)


def rms_scale(state):
    return lax.rsqrt(jnp.mean(state * state, axis=-1, keepdims=True) + EPS)


def rms_pull(state, grad):
    scale = rms_scale(state)
    normed = state * scale
    return scale * (grad - normed * jnp.mean(normed * grad, axis=-1, keepdims=True))


def gelu_parts(hidden, want_grad):
    sq = hidden * hidden
    tanh = jnp.tanh(GELU_C * (hidden + GELU_A * (sq * hidden)))
    half = 0.5 * (1.0 + tanh)
    value = hidden * half
    if not want_grad:
        return value, None
    grad = half + 0.5 * hidden * (1.0 - tanh * tanh) * (GELU_C * (1.0 + 3.0 * GELU_A * sq))
    return value, grad


def chain_kernel(
    seq, hid, heads, hdim, n_pairs,
    y1, y2, dy1, dy2, s1, s2, wq_h, wo_h, wi_h, wu_h,
    ox1, ox2, od1, od2, gq, go, gi, gu,
    wq, wo, wi, wu, a_g, act, gp, dhb, finp, finr, qkvt, dqkvt, pt, ot,
    d1b, d2b, d1f, d2f, vbuf, x2r, xl, pbuf, e1r, xs, xr, gbuf, g1r, g2r, stage,
    e1s_s, e1r_s, e2s_s, e2r_s, e3s_s, e3r_s, g1s_s, g1r_s, g2s_s, g2r_s, g3s_s, g3r_s,
    os_s, or_s, ol_s, w_s, xl_s, v_s, x2_s, st_s, d_s, gcred,
):
    me = lax.axis_index("tp")
    dp = lax.axis_index("dp")
    ci = lax.rem(me, 2)
    core_peer = (dp, me + 1 - 2 * ci)
    x_peer = (dp, lax.rem(me + 2, 4))
    qw = heads * hdim
    npc = 4
    prow = seq // npc

    barrier = pltpu.get_barrier_semaphore()
    pl.semaphore_signal(barrier, inc=1, device_id=core_peer, device_id_type=MESH)
    pl.semaphore_signal(barrier, inc=1, device_id=x_peer, device_id_type=MESH)
    pl.semaphore_wait(barrier, 2)

    def rows(seq_idx):
        return pl.ds(pl.multiple_of(seq_idx * seq, seq), seq)

    def mine(c):
        return 2 * c + ci

    def theirs(c):
        return 2 * c + 1 - ci

    def local(src, dst, sem):
        return pltpu.make_async_copy(src, dst, sem)

    def remote(src, dst, ssem, rsem, dev):
        return pltpu.make_async_remote_copy(src_ref=src, dst_ref=dst, send_sem=ssem, recv_sem=rsem, device_id=dev, device_id_type=MESH)

    def weight_copies(slot, blk, which):
        pairs = {"q": (wq_h, wq), "o": (wo_h, wo), "i": (wi_h, wi), "u": (wu_h, wu)}
        return [local(pairs[k][0].at[blk], pairs[k][1].at[slot], w_s.at[slot, "qoiu".index(k)]) for k in which]

    def w_start(slot, blk, which):
        for cp in weight_copies(slot, blk, which):
            cp.start()

    def w_wait(slot, which):
        for cp in weight_copies(slot, 0, which):
            cp.wait()

    def state_start(first, one, pair, rws, dst, sem):
        top, saved = (y1, s1) if one else (y2, s2)
        if first is True:
            local(top.at[rws], dst, sem).start()
        elif first is False:
            local(saved.at[pair, rws], dst, sem).start()
        else:
            @pl.when(first)
            def _():
                local(top.at[rws], dst, sem).start()

            @pl.when(jnp.logical_not(first))
            def _():
                local(saved.at[jnp.minimum(pair, n_pairs - 1), rws], dst, sem).start()

    def state_wait(dst, sem):
        local(y1.at[rows(0)], dst, sem).wait()

    def each_seq(first, one, pair, body, order=lambda i: i):
        for i in (0, 1):
            state_start(first, one, pair, rows(order(i)), xl.at[i], xl_s.at[i])

        @pl.loop(0, 4)
        def _(i):
            slot = lax.rem(i, 2)
            state_wait(xl.at[slot], xl_s.at[slot])
            body(i, order(i), xl[slot])

            @pl.when(i < 2)
            def _():
                state_start(first, one, pair, rows(order(i + 2)), xl.at[slot], xl_s.at[slot])

    def mlp_fwd(slot, first, pair):
        def body(i, s, state):
            normed = (state * rms_scale(state)).astype(BF)
            a_g[rows(s), :] = normed
            value, grad = gelu_parts(dot(normed, wi[slot], NN), True)
            act[rows(s), :] = value.astype(BF)
            gp[rows(s), :] = grad
        each_seq(first, True, pair, body)

    def attn_fwd_seq(slot, fin, s):
        cols = rows(s)
        qkv = dot(wq[slot], fin[cols, :], NT).astype(BF)
        qkvt[:, cols] = qkv
        for h in range(heads):
            q_t = qkv[h * hdim:(h + 1) * hdim]
            k_t = qkv[qw + h * hdim:qw + (h + 1) * hdim]
            v_t = qkv[2 * qw + h * hdim:2 * qw + (h + 1) * hdim]
            sc = dot(k_t, q_t, TN) * (hdim ** -0.5)
            ex = jnp.exp(sc - jnp.max(sc, axis=0, keepdims=True))
            prob = ex * (1.0 / jnp.sum(ex, axis=0, keepdims=True))
            pt[s * heads + h] = prob
            ot[h * hdim:(h + 1) * hdim, cols] = dot(v_t, prob.astype(BF), NN).astype(BF)

    def attn_fwd_plain(pair):
        def body(i, s, state):
            finp[rows(s), :] = (state * rms_scale(state)).astype(BF)
            attn_fwd_seq(0, finp, s)
        each_seq(False, False, pair, body)

    def attn_fwd_rev():
        @pl.loop(0, 4)
        def _(s):
            attn_fwd_seq(1, finr, s)

    def e1(slot, c):
        return remote(pbuf.at[c, 0], e1r.at[slot, c], e1s_s.at[slot, c], e1r_s.at[slot, c], core_peer)

    def e2(t, c):
        return remote(xs.at[t, c], xr.at[t, c], e2s_s.at[t, c], e2r_s.at[t, c], x_peer)

    def part_g(slot, ver, t, c):
        @pl.loop(0, 2)
        def _(i):
            s = 2 * c + jnp.where(i == 0, 1 - ci, ci)
            d_act = dot(d2b[ver, rows(s), :], wu[slot], NT)
            dh = (d_act * gp[rows(s), :]).astype(BF)
            dhb[rows(s), :] = dh
            pbuf[c, i] = dot(dh, wi[slot], NT)

            @pl.when(i == 0)
            def _():
                e1(t % 2, c).start()

    def part_f(slot, t, c):
        @pl.loop(0, 2)
        def _(i):
            s = 2 * c + jnp.where(i == 0, 1 - ci, ci)
            cols = rows(s)
            do_t = dot(wo[slot], d1b[cols, :], NT).astype(BF)
            for h in range(heads):
                lo = h * hdim
                do_h = do_t[lo:lo + hdim]
                prob = pt[s * heads + h]
                q_t = qkvt[lo:lo + hdim, cols]
                k_t = qkvt[qw + lo:qw + lo + hdim, cols]
                v_t = qkvt[2 * qw + lo:2 * qw + lo + hdim, cols]
                dqkvt[2 * qw + lo:2 * qw + lo + hdim, cols] = dot(do_h, prob.astype(BF), NT).astype(BF)
                dp_t = dot(v_t, do_h, TN)
                inner = jnp.sum(prob * dp_t, axis=0, keepdims=True)
                ds = (prob * (dp_t - inner) * (hdim ** -0.5)).astype(BF)
                dqkvt[lo:lo + hdim, cols] = dot(k_t, ds, NN).astype(BF)
                dqkvt[qw + lo:qw + lo + hdim, cols] = dot(q_t, ds, NT).astype(BF)
            pbuf[c, i] = dot(dqkvt[:, cols], wq[slot], TN)

            @pl.when(i == 0)
            def _():
                e1(t % 2, c).start()

    def to_x(t, c):
        e1(t % 2, c).wait()
        xs[t, c] = (pbuf[c, 1] + e1r[t % 2, c]).astype(BF)
        e2(t, c).start()

    def summed(t, c):
        e2(t, c).wait()
        return xs[t, c].astype(F32) + xr[t, c].astype(F32)

    def e3(kind, c):
        ref = d1b.at[rows(mine(c))] if kind == 0 else d2b.at[kind - 1, rows(mine(c))]
        return remote(ref, ref, e3s_s.at[kind, c], e3r_s.at[kind, c], core_peer)

    def finish(t, c, kind, acc, state):
        total = acc[c] + rms_pull(state, summed(t, c))
        acc[c] = total
        if kind is not None:
            if kind == 0:
                d1b[rows(mine(c)), :] = total.astype(BF)
            else:
                d2b[kind - 1, rows(mine(c)), :] = total.astype(BF)
            e3(kind, c).start()

    def g1(c):
        return remote(gbuf.at[c, 0], g1r.at[c], g1s_s.at[c], g1r_s.at[c], core_peer)

    def g2(k):
        c, q = k // npc, k % npc
        rws = pl.ds(q * prow, prow)
        return remote(gbuf.at[c, 1, rws], g2r.at[c, rws], g2s_s.at[k], g2r_s.at[k], x_peer)

    def g_order(i):
        return 2 * (i // 2) + jnp.where(lax.rem(i, 2) == 0, 1 - ci, ci)

    def g_send_core(i):
        for c in (0, 1):
            @pl.when(i == 2 * c)
            def _():
                g1(c).start()

    def g_part(slot, first, pair):
        def body(i, s, state):
            normed = (state * rms_scale(state)).astype(BF)
            value, _ = gelu_parts(dot(normed, wi[slot], NN), False)
            gbuf[i // 2, lax.rem(i, 2)] = dot(value.astype(BF), wu[slot], NN)
            g_send_core(i)
        each_seq(first, True, pair, body, g_order)

    def f_part(slot):
        @pl.loop(0, 4)
        def _(i):
            gbuf[i // 2, lax.rem(i, 2)] = dot(ot[:, rows(g_order(i))], wo[slot], TN)
            g_send_core(i)

    def g_chip(c):
        g1(c).wait()
        gbuf[c, 1] = gbuf[c, 1] + g1r[c]

    def g_send(*ks):
        for k in ks:
            g2(k).start()

    def g_total(c):
        for q in range(npc):
            g2(c * npc + q).wait()
        return gbuf[c, 1] + g2r[c]

    def g3(c):
        ref = finr.at[rows(mine(c))]
        return remote(ref, ref, g3s_s.at[c], g3r_s.at[c], core_peer)

    def g_finish(c):
        state_wait(x2r.at[c], x2_s.at[c])
        state = x2r[c] - g_total(c)
        x2r[c] = state
        finr[rows(mine(c)), :] = (state * rms_scale(state)).astype(BF)
        g3(c).start()

    def g_credit():
        pl.semaphore_signal(gcred, inc=1, device_id=x_peer, device_id_type=MESH)

    def put(pending, tile, dst, value):
        slot = tile % 3
        height = value.shape[0]
        if pending[slot] is not None:
            pending[slot].wait()
        stage[slot, :height] = value
        cp = local(stage.at[slot, pl.ds(0, height)], dst, st_s.at[slot])
        cp.start()
        pending[slot] = cp

    def flush(pending):
        for cp in pending:
            if cp is not None:
                cp.wait()

    def mlp_grads(blk, ver):
        pending = [None] * 3
        n_t = hid // 256
        for k in range(n_t):
            put(pending, k, gu.at[blk, pl.ds(256 * k, 256)], dot(act[:, 256 * k:256 * (k + 1)], d2b[ver], TN))
        for k in range(n_t):
            put(pending, k, gi.at[blk, pl.ds(256 * k, 256)], dot(a_g[:, 256 * k:256 * (k + 1)], dhb[...], TN))
        flush(pending)

    def attn_grads(blk, fin):
        pending = [None] * 3
        for k in range(3):
            put(pending, k, gq.at[blk, pl.ds(qw * k, qw)], dot(dqkvt[qw * k:qw * (k + 1), :], fin[...], NN))
        put(pending, 3, go.at[blk], dot(ot[...], d1b[...], NN))
        flush(pending)

    def v_start(first, one, pair, c):
        state_start(first, one, pair, rows(mine(c)), vbuf.at[c], v_s.at[c])

    def v_wait(c):
        state_wait(vbuf.at[c], v_s.at[c])

    top = 2 * n_pairs
    w_start(1, top, "iuqo")
    for c in (0, 1):
        local(dy1.at[rows(mine(c))], d1f.at[c], d_s.at[0, c]).start()
        local(dy2.at[rows(mine(c))], d2f.at[c], d_s.at[1, c]).start()
        state_start(True, False, 0, rows(mine(c)), x2r.at[c], x2_s.at[c])
        v_start(True, True, 0, c)
    w_wait(1, "iu")
    g_part(1, True, 0)
    g_chip(0)
    g_send(*range(npc))
    g_chip(1)
    g_send(*range(npc, 2 * npc))
    for i in range(4):
        local(dy2.at[rows(i)], xl.at[i % 2], xl_s.at[i % 2]).start()
        state_wait(xl.at[i % 2], xl_s.at[i % 2])
        d2b[1, rows(i), :] = xl[i % 2].astype(BF)
    for c in (0, 1):
        local(dy1.at[rows(mine(c))], d1f.at[c], d_s.at[0, c]).wait()
        local(dy2.at[rows(mine(c))], d2f.at[c], d_s.at[1, c]).wait()

    @pl.loop(0, n_pairs + 1)
    def _(it):
        pair = n_pairs - it
        is_top = it == 0
        rev = 2 * pair
        plain = 2 * pair + 1

        @pl.when(it > 0)
        def _():
            part_f(0, 0, 0)
            to_x(0, 0)
            g_send(3, 4)
            part_f(0, 0, 1)
            to_x(0, 1)
            g_send(5)
            for c in (0, 1):
                finish(3, c, 1, d2f, x2r[c])
                state_start(False, False, pair, rows(mine(c)), x2r.at[c], x2_s.at[c])
            attn_grads(plain, finp)
            for c in (0, 1):
                e3(1, c).wait()
                part_g(0, 0, 1, c)
                to_x(1, c)
                g_send(6 + c)

            @pl.when(it < n_pairs)
            def _():
                w_start(0, plain - 2, "qoiu")
            mlp_grads(plain, 0)

        mlp_fwd(1, is_top, pair)

        @pl.when(it > 0)
        def _():
            for c in (0, 1):
                v_wait(c)
                finish(0, c, 2, d2f, vbuf[c])
                v_start(False, True, pair, c)
                e3(2, c).wait()
                part_g(1, 1, 2, c)
                to_x(2, c)

        @pl.when(is_top)
        def _():
            for c in (0, 1):
                part_g(1, 1, 2, c)
                to_x(2, c)
            w_wait(1, "qo")

        @pl.when(it < n_pairs)
        def _():
            w_start(1, rev - 2, "iu")

        for c in (0, 1):
            g_finish(c)
        g_credit()
        for c in (0, 1):
            g3(c).wait()

        @pl.when(it > 0)
        def _():
            w_wait(1, "qo")
        attn_fwd_rev()

        @pl.when(it > 0)
        def _():
            for c in (0, 1):
                v_wait(c)
                finish(1, c, None, d1f, vbuf[c])
        mlp_grads(rev, 1)

        @pl.when(it < n_pairs)
        def _():
            w_wait(1, "iu")
            g_part(1, False, pair - 1)

        @pl.when(it == n_pairs)
        def _():
            f_part(1)

        for c in (0, 1):
            @pl.when(is_top)
            def _():
                v_wait(c)
            finish(2, c, 0, d1f, vbuf[c])
            e3(0, c).wait()
            part_f(1, 3, c)
            to_x(3, c)
            g_chip(c)
            if c == 0:
                pl.semaphore_wait(gcred, 1)
                g_send(0)
            else:
                g_send(1, 2)

        @pl.when(it < n_pairs)
        def _():
            for c in (0, 1):
                v_start(False, False, pair - 1, c)
            w_start(1, rev - 2, "qo")

            @pl.when(is_top)
            def _():
                w_start(0, plain - 2, "qoiu")
        attn_grads(rev, finr)

        @pl.when(it < n_pairs)
        def _():
            w_wait(0, "qoiu")
            attn_fwd_plain(pair - 1)
            mlp_fwd(0, False, pair - 1)

    g_send(*range(3, 2 * npc))
    outs = []

    def emit(idx, ref, c, out):
        outs.append(local(ref.at[c], out.at[rows(mine(c))], ol_s.at[idx, c]))
        outs.append(remote(ref.at[c], out.at[rows(mine(c))], os_s.at[idx, c], or_s.at[idx, c], core_peer))
        outs[-2].start()
        outs[-1].start()

    for c in (0, 1):
        finish(3, c, None, d2f, x2r[c])
        emit(3, d2f, c, od2)
        emit(2, d1f, c, od1)
        emit(1, x2r, c, ox2)
    for c in (0, 1):
        v_start(False, True, 0, c)
    for c in (0, 1):
        v_wait(c)
        vbuf[c] = vbuf[c] - g_total(c)
        emit(0, vbuf, c, ox1)
    for cp in outs:
        cp.wait()


def solution(mesh):
    act_spec = P("dp", None, None)
    saved_spec = P(None, "dp", None, None)
    weight_specs = (P(None, None, None, "tp", None), P(None, "tp", None, None), P(None, None, "tp"), P(None, "tp", None))
    grad_specs = (P("dp", None, None, "tp", None), P("dp", "tp", None, None), P("dp", None, "tp"), P("dp", "tp", None))

    def per_device(y_one, y_two, dy_one, dy_two, saved_one, saved_two, w_qkv, w_o, w_in, w_out):
        n_seq, seq, hid = y_one.shape
        n_layers, _, _, heads, hdim = w_qkv.shape
        n_pairs = saved_one.shape[0]
        ff = w_in.shape[-1]
        tok = n_seq * seq
        qkv_w = 3 * heads * hdim
        flat = lambda arr: arr.reshape(arr.shape[:-3] + (tok, hid))
        wq_t = jnp.transpose(w_qkv, (0, 2, 3, 4, 1)).reshape(n_layers, qkv_w, hid)
        wo_t = w_o.reshape(n_layers, heads * hdim, hid)
        sds = jax.ShapeDtypeStruct
        vm = pltpu.VMEM
        dma = pltpu.SemaphoreType.DMA
        half = (2, seq, hid)
        scratch = [
            vm((2, qkv_w, hid), BF), vm((2, heads * hdim, hid), BF), vm((2, hid, ff), BF), vm((2, ff, hid), BF),
            vm((tok, hid), BF), vm((tok, ff), BF), vm((tok, ff), F32), vm((tok, ff), BF),
            vm((tok, hid), BF), vm((tok, hid), BF), vm((qkv_w, tok), BF), vm((qkv_w, tok), BF),
            vm((n_seq * heads, seq, seq), F32), vm((heads * hdim, tok), BF),
            vm((tok, hid), BF), vm((2, tok, hid), BF), vm(half, F32), vm(half, F32),
            vm(half, F32), vm(half, F32), vm(half, F32),
            vm((2,) + half, F32), vm((2,) + half, F32), vm((4,) + half, BF), vm((4,) + half, BF),
            vm((2,) + half, F32), vm(half, F32), vm(half, F32), vm((3, 256, hid), F32),
            dma((2, 2)), dma((2, 2)), dma((4, 2)), dma((4, 2)), dma((3, 2)), dma((3, 2)),
            dma((2,)), dma((2,)), dma((8,)), dma((8,)), dma((2,)), dma((2,)),
            dma((4, 2)), dma((4, 2)), dma((4, 2)), dma((2, 4)), dma((2,)), dma((2,)), dma((2,)), dma((3,)), dma((2, 2)),
            pltpu.SemaphoreType.REGULAR,
        ]
        anyspec = pl.BlockSpec(memory_space=pl.ANY)
        outs = pl.pallas_call(
            functools.partial(chain_kernel, seq, hid, heads, hdim, n_pairs),
            out_shape=[sds((tok, hid), F32)] * 4
            + [sds((n_layers, qkv_w, hid), F32), sds((n_layers, heads * hdim, hid), F32), sds((n_layers, hid, ff), F32), sds((n_layers, ff, hid), F32)],
            in_specs=[anyspec] * 10,
            out_specs=[anyspec] * 8,
            scratch_shapes=scratch,
            name="chain",
            compiler_params=pltpu.CompilerParams(collective_id=0, has_side_effects=True, vmem_limit_bytes=67043328),
        )(flat(y_one), flat(y_two), flat(dy_one), flat(dy_two), flat(saved_one), flat(saved_two), wq_t, wo_t, w_in, w_out)
        states = tuple(out.reshape(n_seq, seq, hid) for out in outs[:4])
        d_qkv = jnp.transpose(outs[4].reshape(n_layers, 3, heads, hdim, hid), (0, 4, 1, 2, 3))
        d_o = outs[5].reshape(n_layers, heads, hdim, hid)
        return states + (d_qkv, d_o, outs[6], outs[7])

    return jax.shard_map(
        per_device,
        mesh=mesh,
        in_specs=(act_spec,) * 4 + (saved_spec,) * 2 + weight_specs,
        out_specs=(act_spec,) * 4 + grad_specs,
        check_vma=False,
    )
```

```python
import functools

import jax
import jax.numpy as jnp
from jax import lax
from jax.experimental import pallas as pl
from jax.experimental.pallas import tpu as pltpu
from jax.sharding import PartitionSpec as P

EPS = 1e-6
BF = jnp.bfloat16
F32 = jnp.float32
MESH = pl.DeviceIdType.MESH
GELU_C = 0.7978845608028654
GELU_A = 0.044715

NN = (((1,), (0,)), ((), ()))
NT = (((1,), (1,)), ((), ()))
TN = (((0,), (0,)), ((), ()))


def dot(lhs, rhs, dims):
    return lax.dot_general(lhs, rhs, dims, preferred_element_type=F32)


def rms_scale(state):
    return lax.rsqrt(jnp.mean(state * state, axis=-1, keepdims=True) + EPS)


def rms_pull(state, grad):
    scale = rms_scale(state)
    normed = state * scale
    return scale * (grad - normed * jnp.mean(normed * grad, axis=-1, keepdims=True))


def gelu_parts(hidden, want_grad):
    sq = hidden * hidden
    tanh = jnp.tanh(GELU_C * (hidden + GELU_A * (sq * hidden)))
    half = 0.5 * (1.0 + tanh)
    value = hidden * half
    if not want_grad:
        return value, None
    grad = half + 0.5 * hidden * (1.0 - tanh * tanh) * (GELU_C * (1.0 + 3.0 * GELU_A * sq))
    return value, grad


def chain_kernel(
    seq, hid, heads, hdim, n_pairs,
    y1, y2, dy1, dy2, s1, s2, wq_h, wo_h, wi_h, wu_h,
    ox1, ox2, od1, od2, gq, go, gi, gu,
    wq, wo, wi, wu, a_g, act, gp, dhb, finp, finr, qkvt, dqkvt, pt, ot,
    d1b, d2b, d1f, d2f, vbuf, x2r, xl, pbuf, e1r, xs, xr, gbuf, g1r, g2r, stage,
    e1s_s, e1r_s, e2s_s, e2r_s, e3s_s, e3r_s, g1s_s, g1r_s, g2s_s, g2r_s, g3s_s, g3r_s,
    os_s, or_s, ol_s, w_s, xl_s, v_s, x2_s, st_s, d_s, gcred,
):
    me = lax.axis_index("tp")
    dp = lax.axis_index("dp")
    ci = lax.rem(me, 2)
    core_peer = (dp, me + 1 - 2 * ci)
    x_peer = (dp, lax.rem(me + 2, 4))
    qw = heads * hdim
    npc = 4
    prow = seq // npc

    barrier = pltpu.get_barrier_semaphore()
    pl.semaphore_signal(barrier, inc=1, device_id=core_peer, device_id_type=MESH)
    pl.semaphore_signal(barrier, inc=1, device_id=x_peer, device_id_type=MESH)
    pl.semaphore_wait(barrier, 2)

    def rows(seq_idx):
        return pl.ds(pl.multiple_of(seq_idx * seq, seq), seq)

    def mine(c):
        return 2 * c + ci

    def theirs(c):
        return 2 * c + 1 - ci

    def local(src, dst, sem):
        return pltpu.make_async_copy(src, dst, sem)

    def remote(src, dst, ssem, rsem, dev):
        return pltpu.make_async_remote_copy(src_ref=src, dst_ref=dst, send_sem=ssem, recv_sem=rsem, device_id=dev, device_id_type=MESH)

    def weight_copies(slot, blk, which):
        pairs = {"q": (wq_h, wq), "o": (wo_h, wo), "i": (wi_h, wi), "u": (wu_h, wu)}
        return [local(pairs[k][0].at[blk], pairs[k][1].at[slot], w_s.at[slot, "qoiu".index(k)]) for k in which]

    def w_start(slot, blk, which):
        for cp in weight_copies(slot, blk, which):
            cp.start()

    def w_wait(slot, which):
        for cp in weight_copies(slot, 0, which):
            cp.wait()

    def state_start(first, one, pair, rws, dst, sem):
        top, saved = (y1, s1) if one else (y2, s2)
        if first is True:
            local(top.at[rws], dst, sem).start()
        elif first is False:
            local(saved.at[pair, rws], dst, sem).start()
        else:
            @pl.when(first)
            def _():
                local(top.at[rws], dst, sem).start()

            @pl.when(jnp.logical_not(first))
            def _():
                local(saved.at[jnp.minimum(pair, n_pairs - 1), rws], dst, sem).start()

    def state_wait(dst, sem):
        local(y1.at[rows(0)], dst, sem).wait()

    def each_seq(first, one, pair, body, order=lambda i: i):
        for i in (0, 1):
            state_start(first, one, pair, rows(order(i)), xl.at[i], xl_s.at[i])

        @pl.loop(0, 4)
        def _(i):
            slot = lax.rem(i, 2)
            state_wait(xl.at[slot], xl_s.at[slot])
            body(i, order(i), xl[slot])

            @pl.when(i < 2)
            def _():
                state_start(first, one, pair, rows(order(i + 2)), xl.at[slot], xl_s.at[slot])

    def mlp_fwd(slot, first, pair):
        def body(i, s, state):
            normed = (state * rms_scale(state)).astype(BF)
            a_g[rows(s), :] = normed
            value, grad = gelu_parts(dot(normed, wi[slot], NN), True)
            act[rows(s), :] = value.astype(BF)
            gp[rows(s), :] = grad
        each_seq(first, True, pair, body)

    def attn_fwd_seq(slot, fin, s):
        cols = rows(s)
        qkv = dot(wq[slot], fin[cols, :], NT).astype(BF)
        qkvt[:, cols] = qkv
        for h in range(heads):
            q_t = qkv[h * hdim:(h + 1) * hdim]
            k_t = qkv[qw + h * hdim:qw + (h + 1) * hdim]
            v_t = qkv[2 * qw + h * hdim:2 * qw + (h + 1) * hdim]
            sc = dot(k_t, q_t, TN) * (hdim ** -0.5)
            ex = jnp.exp(sc - jnp.max(sc, axis=0, keepdims=True))
            prob = ex * (1.0 / jnp.sum(ex, axis=0, keepdims=True))
            pt[s * heads + h] = prob
            ot[h * hdim:(h + 1) * hdim, cols] = dot(v_t, prob.astype(BF), NN).astype(BF)

    def attn_fwd_plain(pair):
        def body(i, s, state):
            finp[rows(s), :] = (state * rms_scale(state)).astype(BF)
            attn_fwd_seq(0, finp, s)
        each_seq(False, False, pair, body)

    def attn_fwd_rev():
        @pl.loop(0, 4)
        def _(s):
            attn_fwd_seq(1, finr, s)

    def e1(slot, c):
        return remote(pbuf.at[c, 0], e1r.at[slot, c], e1s_s.at[slot, c], e1r_s.at[slot, c], core_peer)

    def e2(t, c):
        return remote(xs.at[t, c], xr.at[t, c], e2s_s.at[t, c], e2r_s.at[t, c], x_peer)

    def part_g(slot, ver, c, mode, e1_slot=None):
        @pl.loop(0, 2)
        def _(i):
            s = 2 * c + jnp.where(i == 0, 1 - ci, ci)
            d_act = dot(d2b[ver, rows(s), :], wu[slot], NT)
            dh = (d_act * gp[rows(s), :]).astype(BF)
            dhb[rows(s), :] = dh
            part = dot(dh, wi[slot], NT)
            pbuf[c, i] = pbuf[c, i] + part if mode == "add" else part
            if mode != "hold":
                @pl.when(i == 0)
                def _():
                    e1(e1_slot, c).start()

    def part_f(slot, c, e1_slot):
        @pl.loop(0, 2)
        def _(i):
            s = 2 * c + jnp.where(i == 0, 1 - ci, ci)
            cols = rows(s)
            do_t = dot(wo[slot], d1b[cols, :], NT).astype(BF)
            for h in range(heads):
                lo = h * hdim
                do_h = do_t[lo:lo + hdim]
                prob = pt[s * heads + h]
                q_t = qkvt[lo:lo + hdim, cols]
                k_t = qkvt[qw + lo:qw + lo + hdim, cols]
                v_t = qkvt[2 * qw + lo:2 * qw + lo + hdim, cols]
                dqkvt[2 * qw + lo:2 * qw + lo + hdim, cols] = dot(do_h, prob.astype(BF), NT).astype(BF)
                dp_t = dot(v_t, do_h, TN)
                inner = jnp.sum(prob * dp_t, axis=0, keepdims=True)
                ds = (prob * (dp_t - inner) * (hdim ** -0.5)).astype(BF)
                dqkvt[lo:lo + hdim, cols] = dot(k_t, ds, NN).astype(BF)
                dqkvt[qw + lo:qw + lo + hdim, cols] = dot(q_t, ds, NT).astype(BF)
            pbuf[c, i] = dot(dqkvt[:, cols], wq[slot], TN)

            @pl.when(i == 0)
            def _():
                e1(e1_slot, c).start()

    def to_x(t, c, e1_slot):
        e1(e1_slot, c).wait()
        xs[t, c] = (pbuf[c, 1] + e1r[e1_slot, c]).astype(BF)
        e2(t, c).start()

    def summed(t, c):
        e2(t, c).wait()
        return xs[t, c].astype(F32) + xr[t, c].astype(F32)

    def e3(kind, c):
        ref = d1b.at[rows(mine(c))] if kind == 0 else d2b.at[kind - 1, rows(mine(c))]
        return remote(ref, ref, e3s_s.at[kind, c], e3r_s.at[kind, c], core_peer)

    def finish(t, c, kind, acc, state):
        total = acc[c] + rms_pull(state, summed(t, c))
        acc[c] = total
        if kind is not None:
            if kind == 0:
                d1b[rows(mine(c)), :] = total.astype(BF)
            else:
                d2b[kind - 1, rows(mine(c)), :] = total.astype(BF)
            e3(kind, c).start()

    def g1(c):
        return remote(gbuf.at[c, 0], g1r.at[c], g1s_s.at[c], g1r_s.at[c], core_peer)

    def g2(k):
        c, q = k // npc, k % npc
        rws = pl.ds(q * prow, prow)
        return remote(gbuf.at[c, 1, rws], g2r.at[c, rws], g2s_s.at[k], g2r_s.at[k], x_peer)

    def g_order(i):
        return 2 * (i // 2) + jnp.where(lax.rem(i, 2) == 0, 1 - ci, ci)

    def g_send_core(i):
        for c in (0, 1):
            @pl.when(i == 2 * c)
            def _():
                g1(c).start()

    def g_part(slot, first, pair):
        def body(i, s, state):
            normed = (state * rms_scale(state)).astype(BF)
            value, _ = gelu_parts(dot(normed, wi[slot], NN), False)
            gbuf[i // 2, lax.rem(i, 2)] = dot(value.astype(BF), wu[slot], NN)
            g_send_core(i)
        each_seq(first, True, pair, body, g_order)

    def f_part(slot):
        @pl.loop(0, 4)
        def _(i):
            gbuf[i // 2, lax.rem(i, 2)] = dot(ot[:, rows(g_order(i))], wo[slot], TN)
            g_send_core(i)

    def g_chip(c):
        g1(c).wait()
        gbuf[c, 1] = gbuf[c, 1] + g1r[c]

    def g_send(*ks):
        for k in ks:
            g2(k).start()

    def g_total(c):
        for q in range(npc):
            g2(c * npc + q).wait()
        return gbuf[c, 1] + g2r[c]

    def g3(c):
        ref = finr.at[rows(mine(c))]
        return remote(ref, ref, g3s_s.at[c], g3r_s.at[c], core_peer)

    def g_finish(c):
        state_wait(x2r.at[c], x2_s.at[c])
        state = x2r[c] - g_total(c)
        x2r[c] = state
        finr[rows(mine(c)), :] = (state * rms_scale(state)).astype(BF)
        g3(c).start()

    def g_credit():
        pl.semaphore_signal(gcred, inc=1, device_id=x_peer, device_id_type=MESH)

    def put(pending, tile, dst, value):
        slot = tile % 3
        height = value.shape[0]
        if pending[slot] is not None:
            pending[slot].wait()
        stage[slot, :height] = value
        cp = local(stage.at[slot, pl.ds(0, height)], dst, st_s.at[slot])
        cp.start()
        pending[slot] = cp

    def flush(pending):
        for cp in pending:
            if cp is not None:
                cp.wait()

    def mlp_grads(blk, ver):
        pending = [None] * 3
        n_t = hid // 256
        for k in range(n_t):
            put(pending, k, gu.at[blk, pl.ds(256 * k, 256)], dot(act[:, 256 * k:256 * (k + 1)], d2b[ver], TN))
        for k in range(n_t):
            put(pending, k, gi.at[blk, pl.ds(256 * k, 256)], dot(a_g[:, 256 * k:256 * (k + 1)], dhb[...], TN))
        flush(pending)

    def attn_grads(blk, fin):
        pending = [None] * 3
        for k in range(3):
            put(pending, k, gq.at[blk, pl.ds(qw * k, qw)], dot(dqkvt[qw * k:qw * (k + 1), :], fin[...], NN))
        put(pending, 3, go.at[blk], dot(ot[...], d1b[...], NN))
        flush(pending)

    def v_start(first, one, pair, c):
        state_start(first, one, pair, rows(mine(c)), vbuf.at[c], v_s.at[c])

    def v_wait(c):
        state_wait(vbuf.at[c], v_s.at[c])

    top = 2 * n_pairs
    w_start(1, top, "iuqo")
    for c in (0, 1):
        local(dy1.at[rows(mine(c))], d1f.at[c], d_s.at[0, c]).start()
        local(dy2.at[rows(mine(c))], d2f.at[c], d_s.at[1, c]).start()
        state_start(True, False, 0, rows(mine(c)), x2r.at[c], x2_s.at[c])
        v_start(True, True, 0, c)
    w_wait(1, "iu")
    g_part(1, True, 0)
    g_chip(0)
    g_send(*range(npc))
    g_chip(1)
    g_send(*range(npc, 2 * npc))
    for i in range(4):
        local(dy2.at[rows(i)], xl.at[i % 2], xl_s.at[i % 2]).start()
        state_wait(xl.at[i % 2], xl_s.at[i % 2])
        d2b[1, rows(i), :] = xl[i % 2].astype(BF)
    for c in (0, 1):
        local(dy1.at[rows(mine(c))], d1f.at[c], d_s.at[0, c]).wait()
        local(dy2.at[rows(mine(c))], d2f.at[c], d_s.at[1, c]).wait()

    @pl.loop(0, n_pairs + 1)
    def _(it):
        pair = n_pairs - it
        is_top = it == 0
        rev = 2 * pair
        plain = 2 * pair + 1
        even, odd = lax.rem(it, 2), lax.rem(it + 1, 2)

        @pl.when(it > 0)
        def _():
            part_f(0, 0, even)
            to_x(0, 0, even)
            g_send(3, 4)
            part_f(0, 1, even)
            to_x(0, 1, even)
            g_send(5, 6, 7)
            for c in (0, 1):
                finish(2, c, 1, d2f, x2r[c])
                state_start(False, False, pair, rows(mine(c)), x2r.at[c], x2_s.at[c])
            attn_grads(plain, finp)
            for c in (0, 1):
                e3(1, c).wait()
                part_g(0, 0, c, "hold")

            @pl.when(it < n_pairs)
            def _():
                w_start(0, plain - 2, "qoiu")
            mlp_grads(plain, 0)

        mlp_fwd(1, is_top, pair)

        @pl.when(it > 0)
        def _():
            for c in (0, 1):
                v_wait(c)
                finish(0, c, 2, d2f, vbuf[c])
                v_start(False, True, pair, c)
                e3(2, c).wait()
                part_g(1, 1, c, "add", odd)
                to_x(1, c, odd)

        @pl.when(is_top)
        def _():
            for c in (0, 1):
                part_g(1, 1, c, "first", odd)
                to_x(1, c, odd)
            w_wait(1, "qo")

        @pl.when(it < n_pairs)
        def _():
            w_start(1, rev - 2, "iu")

        for c in (0, 1):
            g_finish(c)
        g_credit()
        for c in (0, 1):
            g3(c).wait()

        @pl.when(it > 0)
        def _():
            w_wait(1, "qo")
        attn_fwd_rev()

        mlp_grads(rev, 1)

        @pl.when(it < n_pairs)
        def _():
            w_wait(1, "iu")
            g_part(1, False, pair - 1)

        @pl.when(it == n_pairs)
        def _():
            f_part(1)

        for c in (0, 1):
            v_wait(c)
            finish(1, c, 0, d1f, vbuf[c])
            e3(0, c).wait()
            part_f(1, c, even)
            to_x(2, c, even)
            g_chip(c)
            if c == 0:
                pl.semaphore_wait(gcred, 1)
                g_send(0)
            else:
                g_send(1, 2)

        @pl.when(it < n_pairs)
        def _():
            for c in (0, 1):
                v_start(False, False, pair - 1, c)
            w_start(1, rev - 2, "qo")

            @pl.when(is_top)
            def _():
                w_start(0, plain - 2, "qoiu")
        attn_grads(rev, finr)

        @pl.when(it < n_pairs)
        def _():
            w_wait(0, "qoiu")
            attn_fwd_plain(pair - 1)
            mlp_fwd(0, False, pair - 1)

    g_send(*range(3, 2 * npc))
    outs = []

    def emit(idx, ref, c, out):
        outs.append(local(ref.at[c], out.at[rows(mine(c))], ol_s.at[idx, c]))
        outs.append(remote(ref.at[c], out.at[rows(mine(c))], os_s.at[idx, c], or_s.at[idx, c], core_peer))
        outs[-2].start()
        outs[-1].start()

    for c in (0, 1):
        finish(2, c, None, d2f, x2r[c])
        emit(3, d2f, c, od2)
        emit(2, d1f, c, od1)
        emit(1, x2r, c, ox2)
    for c in (0, 1):
        v_start(False, True, 0, c)
    for c in (0, 1):
        v_wait(c)
        vbuf[c] = vbuf[c] - g_total(c)
        emit(0, vbuf, c, ox1)
    for cp in outs:
        cp.wait()


def solution(mesh):
    act_spec = P("dp", None, None)
    saved_spec = P(None, "dp", None, None)
    weight_specs = (P(None, None, None, "tp", None), P(None, "tp", None, None), P(None, None, "tp"), P(None, "tp", None))
    grad_specs = (P("dp", None, None, "tp", None), P("dp", "tp", None, None), P("dp", None, "tp"), P("dp", "tp", None))

    def per_device(y_one, y_two, dy_one, dy_two, saved_one, saved_two, w_qkv, w_o, w_in, w_out):
        n_seq, seq, hid = y_one.shape
        n_layers, _, _, heads, hdim = w_qkv.shape
        n_pairs = saved_one.shape[0]
        ff = w_in.shape[-1]
        tok = n_seq * seq
        qkv_w = 3 * heads * hdim
        flat = lambda arr: arr.reshape(arr.shape[:-3] + (tok, hid))
        wq_t = jnp.transpose(w_qkv, (0, 2, 3, 4, 1)).reshape(n_layers, qkv_w, hid)
        wo_t = w_o.reshape(n_layers, heads * hdim, hid)
        sds = jax.ShapeDtypeStruct
        vm = pltpu.VMEM
        dma = pltpu.SemaphoreType.DMA
        half = (2, seq, hid)
        scratch = [
            vm((2, qkv_w, hid), BF), vm((2, heads * hdim, hid), BF), vm((2, hid, ff), BF), vm((2, ff, hid), BF),
            vm((tok, hid), BF), vm((tok, ff), BF), vm((tok, ff), F32), vm((tok, ff), BF),
            vm((tok, hid), BF), vm((tok, hid), BF), vm((qkv_w, tok), BF), vm((qkv_w, tok), BF),
            vm((n_seq * heads, seq, seq), F32), vm((heads * hdim, tok), BF),
            vm((tok, hid), BF), vm((2, tok, hid), BF), vm(half, F32), vm(half, F32),
            vm(half, F32), vm(half, F32), vm(half, F32),
            vm((2,) + half, F32), vm((2,) + half, F32), vm((3,) + half, BF), vm((3,) + half, BF),
            vm((2,) + half, F32), vm(half, F32), vm(half, F32), vm((3, 256, hid), F32),
            dma((2, 2)), dma((2, 2)), dma((3, 2)), dma((3, 2)), dma((3, 2)), dma((3, 2)),
            dma((2,)), dma((2,)), dma((8,)), dma((8,)), dma((2,)), dma((2,)),
            dma((4, 2)), dma((4, 2)), dma((4, 2)), dma((2, 4)), dma((2,)), dma((2,)), dma((2,)), dma((3,)), dma((2, 2)),
            pltpu.SemaphoreType.REGULAR,
        ]
        anyspec = pl.BlockSpec(memory_space=pl.ANY)
        outs = pl.pallas_call(
            functools.partial(chain_kernel, seq, hid, heads, hdim, n_pairs),
            out_shape=[sds((tok, hid), F32)] * 4
            + [sds((n_layers, qkv_w, hid), F32), sds((n_layers, heads * hdim, hid), F32), sds((n_layers, hid, ff), F32), sds((n_layers, ff, hid), F32)],
            in_specs=[anyspec] * 10,
            out_specs=[anyspec] * 8,
            scratch_shapes=scratch,
            name="chain",
            compiler_params=pltpu.CompilerParams(collective_id=0, has_side_effects=True, vmem_limit_bytes=67043328),
        )(flat(y_one), flat(y_two), flat(dy_one), flat(dy_two), flat(saved_one), flat(saved_two), wq_t, wo_t, w_in, w_out)
        states = tuple(out.reshape(n_seq, seq, hid) for out in outs[:4])
        d_qkv = jnp.transpose(outs[4].reshape(n_layers, 3, heads, hdim, hid), (0, 4, 1, 2, 3))
        d_o = outs[5].reshape(n_layers, heads, hdim, hid)
        return states + (d_qkv, d_o, outs[6], outs[7])

    return jax.shard_map(
        per_device,
        mesh=mesh,
        in_specs=(act_spec,) * 4 + (saved_spec,) * 2 + weight_specs,
        out_specs=(act_spec,) * 4 + grad_specs,
        check_vma=False,
    )
```

```python
import functools

import jax
import jax.numpy as jnp
from jax import lax
from jax.experimental import pallas as pl
from jax.experimental.pallas import tpu as pltpu
from jax.sharding import PartitionSpec as P

EPS = 1e-6
BF = jnp.bfloat16
F32 = jnp.float32
MESH = pl.DeviceIdType.MESH
GELU_C = 0.7978845608028654
GELU_A = 0.044715

NN = (((1,), (0,)), ((), ()))
NT = (((1,), (1,)), ((), ()))
TN = (((0,), (0,)), ((), ()))


def dot(lhs, rhs, dims):
    return lax.dot_general(lhs, rhs, dims, preferred_element_type=F32)


def rms_scale(state):
    return lax.rsqrt(jnp.mean(state * state, axis=-1, keepdims=True) + EPS)


def rms_pull(state, grad):
    scale = rms_scale(state)
    normed = state * scale
    return scale * (grad - normed * jnp.mean(normed * grad, axis=-1, keepdims=True))


def gelu_parts(hidden, want_grad):
    sq = hidden * hidden
    tanh = jnp.tanh(GELU_C * (hidden + GELU_A * (sq * hidden)))
    half = 0.5 * (1.0 + tanh)
    value = hidden * half
    if not want_grad:
        return value, None
    grad = half + 0.5 * hidden * (1.0 - tanh * tanh) * (GELU_C * (1.0 + 3.0 * GELU_A * sq))
    return value, grad


def chain_kernel(
    seq, hid, heads, hdim, n_pairs,
    y1, y2, dy1, dy2, s1, s2, wq_h, wo_h, wi_h, wu_h,
    ox1, ox2, od1, od2, gq, go, gi, gu,
    wq, wo, wi, wu, a_g, act, gp, dhb, finp, finr, qkvt, dqkvt, pt, ot,
    d1b, d2b, d1f, d2f, vbuf, x2r, xl, pbuf, e1r, xs, xr, gbuf, g1r, g2r, stage,
    e1s_s, e1r_s, e2s_s, e2r_s, e3s_s, e3r_s, g1s_s, g1r_s, g2s_s, g2r_s, g3s_s, g3r_s,
    os_s, or_s, ol_s, w_s, xl_s, v_s, x2_s, st_s, d_s, gcred,
):
    me = lax.axis_index("tp")
    dp = lax.axis_index("dp")
    ci = lax.rem(me, 2)
    core_peer = (dp, me + 1 - 2 * ci)
    x_peer = (dp, lax.rem(me + 2, 4))
    qw = heads * hdim
    npc = 4
    prow = seq // npc

    barrier = pltpu.get_barrier_semaphore()
    pl.semaphore_signal(barrier, inc=1, device_id=core_peer, device_id_type=MESH)
    pl.semaphore_signal(barrier, inc=1, device_id=x_peer, device_id_type=MESH)
    pl.semaphore_wait(barrier, 2)

    def rows(seq_idx):
        return pl.ds(pl.multiple_of(seq_idx * seq, seq), seq)

    def mine(c):
        return 2 * c + ci

    def theirs(c):
        return 2 * c + 1 - ci

    def local(src, dst, sem):
        return pltpu.make_async_copy(src, dst, sem)

    def remote(src, dst, ssem, rsem, dev):
        return pltpu.make_async_remote_copy(src_ref=src, dst_ref=dst, send_sem=ssem, recv_sem=rsem, device_id=dev, device_id_type=MESH)

    def weight_copies(slot, blk, which):
        pairs = {"q": (wq_h, wq), "o": (wo_h, wo), "i": (wi_h, wi), "u": (wu_h, wu)}
        return [local(pairs[k][0].at[blk], pairs[k][1].at[slot], w_s.at[slot, "qoiu".index(k)]) for k in which]

    def w_start(slot, blk, which):
        for cp in weight_copies(slot, blk, which):
            cp.start()

    def w_wait(slot, which):
        for cp in weight_copies(slot, 0, which):
            cp.wait()

    def state_start(first, one, pair, rws, dst, sem):
        top, saved = (y1, s1) if one else (y2, s2)
        if first is True:
            local(top.at[rws], dst, sem).start()
        elif first is False:
            local(saved.at[pair, rws], dst, sem).start()
        else:
            @pl.when(first)
            def _():
                local(top.at[rws], dst, sem).start()

            @pl.when(jnp.logical_not(first))
            def _():
                local(saved.at[jnp.minimum(pair, n_pairs - 1), rws], dst, sem).start()

    def state_wait(dst, sem):
        local(y1.at[rows(0)], dst, sem).wait()

    def each_seq(first, one, pair, body, order=lambda i: i):
        for i in (0, 1):
            state_start(first, one, pair, rows(order(i)), xl.at[i], xl_s.at[i])

        @pl.loop(0, 4)
        def _(i):
            slot = lax.rem(i, 2)
            state_wait(xl.at[slot], xl_s.at[slot])
            body(i, order(i), xl[slot])

            @pl.when(i < 2)
            def _():
                state_start(first, one, pair, rows(order(i + 2)), xl.at[slot], xl_s.at[slot])

    def mlp_fwd(slot):
        @pl.loop(0, 4)
        def _(s):
            value, grad = gelu_parts(dot(a_g[rows(s), :], wi[slot], NN), True)
            act[rows(s), :] = value.astype(BF)
            gp[rows(s), :] = grad

    def attn_fwd_seq(slot, fin, s):
        cols = rows(s)
        qkv = dot(wq[slot], fin[cols, :], NT).astype(BF)
        qkvt[:, cols] = qkv
        for h in range(heads):
            q_t = qkv[h * hdim:(h + 1) * hdim]
            k_t = qkv[qw + h * hdim:qw + (h + 1) * hdim]
            v_t = qkv[2 * qw + h * hdim:2 * qw + (h + 1) * hdim]
            sc = dot(k_t, q_t, TN) * (hdim ** -0.5)
            ex = jnp.exp(sc - jnp.max(sc, axis=0, keepdims=True))
            prob = ex * (1.0 / jnp.sum(ex, axis=0, keepdims=True))
            pt[s * heads + h] = prob
            ot[h * hdim:(h + 1) * hdim, cols] = dot(v_t, prob.astype(BF), NN).astype(BF)

    def attn_fwd_plain(pair):
        def body(i, s, state):
            finp[rows(s), :] = (state * rms_scale(state)).astype(BF)
            attn_fwd_seq(0, finp, s)
        each_seq(False, False, pair, body)

    def attn_fwd_rev():
        @pl.loop(0, 4)
        def _(s):
            attn_fwd_seq(1, finr, s)

    def e1(slot, c):
        return remote(pbuf.at[c, 0], e1r.at[slot, c], e1s_s.at[slot, c], e1r_s.at[slot, c], core_peer)

    def e2(t, c):
        return remote(xs.at[t, c], xr.at[t, c], e2s_s.at[t, c], e2r_s.at[t, c], x_peer)

    def part_g(slot, ver, c, mode, e1_slot=None):
        @pl.loop(0, 2)
        def _(i):
            s = 2 * c + jnp.where(i == 0, 1 - ci, ci)
            d_act = dot(d2b[ver, rows(s), :], wu[slot], NT)
            dh = (d_act * gp[rows(s), :]).astype(BF)
            dhb[rows(s), :] = dh
            part = dot(dh, wi[slot], NT)
            pbuf[c, i] = pbuf[c, i] + part if mode == "add" else part
            if mode != "hold":
                @pl.when(i == 0)
                def _():
                    e1(e1_slot, c).start()

    def part_f(slot, c, e1_slot):
        @pl.loop(0, 2)
        def _(i):
            s = 2 * c + jnp.where(i == 0, 1 - ci, ci)
            cols = rows(s)
            do_t = dot(wo[slot], d1b[cols, :], NT).astype(BF)
            for h in range(heads):
                lo = h * hdim
                do_h = do_t[lo:lo + hdim]
                prob = pt[s * heads + h]
                q_t = qkvt[lo:lo + hdim, cols]
                k_t = qkvt[qw + lo:qw + lo + hdim, cols]
                v_t = qkvt[2 * qw + lo:2 * qw + lo + hdim, cols]
                dqkvt[2 * qw + lo:2 * qw + lo + hdim, cols] = dot(do_h, prob.astype(BF), NT).astype(BF)
                dp_t = dot(v_t, do_h, TN)
                inner = jnp.sum(prob * dp_t, axis=0, keepdims=True)
                ds = (prob * (dp_t - inner) * (hdim ** -0.5)).astype(BF)
                dqkvt[lo:lo + hdim, cols] = dot(k_t, ds, NN).astype(BF)
                dqkvt[qw + lo:qw + lo + hdim, cols] = dot(q_t, ds, NT).astype(BF)
            pbuf[c, i] = dot(dqkvt[:, cols], wq[slot], TN)

            @pl.when(i == 0)
            def _():
                e1(e1_slot, c).start()

    def to_x(t, c, e1_slot):
        e1(e1_slot, c).wait()
        xs[t, c] = (pbuf[c, 1] + e1r[e1_slot, c]).astype(BF)
        e2(t, c).start()

    def summed(t, c):
        e2(t, c).wait()
        return xs[t, c].astype(F32) + xr[t, c].astype(F32)

    def e3(kind, c):
        ref = d1b.at[rows(mine(c))] if kind == 0 else d2b.at[kind - 1, rows(mine(c))]
        return remote(ref, ref, e3s_s.at[kind, c], e3r_s.at[kind, c], core_peer)

    def finish(t, c, kind, acc, state):
        total = acc[c] + rms_pull(state, summed(t, c))
        acc[c] = total
        if kind is not None:
            if kind == 0:
                d1b[rows(mine(c)), :] = total.astype(BF)
            else:
                d2b[kind - 1, rows(mine(c)), :] = total.astype(BF)
            e3(kind, c).start()

    def g1(c):
        return remote(gbuf.at[c, 0], g1r.at[c], g1s_s.at[c], g1r_s.at[c], core_peer)

    def g2(k):
        c, q = k // npc, k % npc
        rws = pl.ds(q * prow, prow)
        return remote(gbuf.at[c, 1, rws], g2r.at[c, rws], g2s_s.at[k], g2r_s.at[k], x_peer)

    def g_order(i):
        return 2 * (i // 2) + jnp.where(lax.rem(i, 2) == 0, 1 - ci, ci)

    def g_send_core(i):
        for c in (0, 1):
            @pl.when(i == 2 * c)
            def _():
                g1(c).start()

    def g_part(slot, first, pair, keep):
        def body(i, s, state):
            normed = (state * rms_scale(state)).astype(BF)
            a_g[rows(s), :] = normed
            value, grad = gelu_parts(dot(normed, wi[slot], NN), keep)
            value = value.astype(BF)
            if keep:
                act[rows(s), :] = value
                gp[rows(s), :] = grad
            gbuf[i // 2, lax.rem(i, 2)] = dot(value, wu[slot], NN)
            g_send_core(i)
        each_seq(first, True, pair, body, g_order)

    def f_part(slot):
        @pl.loop(0, 4)
        def _(i):
            gbuf[i // 2, lax.rem(i, 2)] = dot(ot[:, rows(g_order(i))], wo[slot], TN)
            g_send_core(i)

    def g_chip(c):
        g1(c).wait()
        gbuf[c, 1] = gbuf[c, 1] + g1r[c]

    def g_send(*ks):
        for k in ks:
            g2(k).start()

    def g_total(c):
        for q in range(npc):
            g2(c * npc + q).wait()
        return gbuf[c, 1] + g2r[c]

    def g3(c):
        ref = finr.at[rows(mine(c))]
        return remote(ref, ref, g3s_s.at[c], g3r_s.at[c], core_peer)

    def g_finish(c):
        state_wait(x2r.at[c], x2_s.at[c])
        state = x2r[c] - g_total(c)
        x2r[c] = state
        finr[rows(mine(c)), :] = (state * rms_scale(state)).astype(BF)
        g3(c).start()

    def g_credit():
        pl.semaphore_signal(gcred, inc=1, device_id=x_peer, device_id_type=MESH)

    def put(pending, tile, dst, value):
        slot = tile % 3
        height = value.shape[0]
        if pending[slot] is not None:
            pending[slot].wait()
        stage[slot, :height] = value
        cp = local(stage.at[slot, pl.ds(0, height)], dst, st_s.at[slot])
        cp.start()
        pending[slot] = cp

    def flush(pending):
        for cp in pending:
            if cp is not None:
                cp.wait()

    def mlp_grads(blk, ver):
        pending = [None] * 3
        n_t = hid // 256
        for k in range(n_t):
            put(pending, k, gu.at[blk, pl.ds(256 * k, 256)], dot(act[:, 256 * k:256 * (k + 1)], d2b[ver], TN))
        for k in range(n_t):
            put(pending, k, gi.at[blk, pl.ds(256 * k, 256)], dot(a_g[:, 256 * k:256 * (k + 1)], dhb[...], TN))
        flush(pending)

    def attn_grads(blk, fin):
        pending = [None] * 3
        for k in range(3):
            put(pending, k, gq.at[blk, pl.ds(qw * k, qw)], dot(dqkvt[qw * k:qw * (k + 1), :], fin[...], NN))
        put(pending, 3, go.at[blk], dot(ot[...], d1b[...], NN))
        flush(pending)

    def v_start(first, one, pair, c):
        state_start(first, one, pair, rows(mine(c)), vbuf.at[c], v_s.at[c])

    def v_wait(c):
        state_wait(vbuf.at[c], v_s.at[c])

    top = 2 * n_pairs
    w_start(1, top, "iuqo")
    for c in (0, 1):
        v_start(True, True, 0, c)
        state_start(True, False, 0, rows(mine(c)), x2r.at[c], x2_s.at[c])
        local(dy1.at[rows(mine(c))], d1f.at[c], d_s.at[0, c]).start()
        local(dy2.at[rows(mine(c))], d2f.at[c], d_s.at[1, c]).start()
    w_wait(1, "iu")
    g_part(1, True, 0, True)
    for c in (0, 1):
        g_chip(c)
        g_send(*range(npc * c, npc * (c + 1)))
    w_start(0, top - 1, "qoiu")
    for i in range(4):
        local(dy2.at[rows(i)], xl.at[i % 2], xl_s.at[i % 2]).start()
        state_wait(xl.at[i % 2], xl_s.at[i % 2])
        d2b[1, rows(i), :] = xl[i % 2].astype(BF)
    for c in (0, 1):
        local(dy1.at[rows(mine(c))], d1f.at[c], d_s.at[0, c]).wait()
        local(dy2.at[rows(mine(c))], d2f.at[c], d_s.at[1, c]).wait()

    @pl.loop(0, n_pairs + 1)
    def _(it):
        pair = n_pairs - it
        is_top = it == 0
        more = it < n_pairs
        rev = 2 * pair
        even, odd = lax.rem(it, 2), lax.rem(it + 1, 2)

        @pl.when(is_top)
        def _():
            for c in (0, 1):
                part_g(1, 1, c, "first", odd)
                to_x(1, c, odd)

        @pl.when(it > 0)
        def _():
            for c in (0, 1):
                v_wait(c)
                finish(0, c, 2, d2f, vbuf[c])
                v_start(False, True, pair, c)
                e3(2, c).wait()
                part_g(1, 1, c, "add", odd)
                to_x(1, c, odd)

        @pl.when(more)
        def _():
            w_start(1, rev - 2, "iu")

        for c in (0, 1):
            g_finish(c)
        g_credit()
        w_wait(1, "qo")
        for c in (0, 1):
            g3(c).wait()
        attn_fwd_rev()

        for c in (0, 1):
            v_wait(c)
            finish(1, c, 0, d1f, vbuf[c])
            e3(0, c).wait()
            part_f(1, c, even)
            to_x(2, c, even)
        attn_grads(rev, finr)

        @pl.when(more)
        def _():
            w_start(1, rev - 2, "qo")
            for c in (0, 1):
                v_start(False, False, pair - 1, c)
            w_wait(0, "qo")
            attn_fwd_plain(pair - 1)
            for c in (0, 1):
                part_f(0, c, odd)
                to_x(0, c, odd)
        mlp_grads(rev, 1)

        @pl.when(more)
        def _():
            w_wait(1, "iu")
            g_part(1, False, pair - 1, False)

        @pl.when(jnp.logical_not(more))
        def _():
            f_part(1)

        pl.semaphore_wait(gcred, 1)
        for c in (0, 1):
            g_chip(c)
            g_send(*range(npc * c, npc * (c + 1)))

        @pl.when(more)
        def _():
            w_wait(0, "iu")
            mlp_fwd(0)
            for c in (0, 1):
                finish(2, c, 1, d2f, x2r[c])
                state_start(False, False, pair - 1, rows(mine(c)), x2r.at[c], x2_s.at[c])
            for c in (0, 1):
                e3(1, c).wait()
                part_g(0, 0, c, "hold")

            @pl.when(it < n_pairs - 1)
            def _():
                w_start(0, rev - 3, "qoiu")
            mlp_grads(rev - 1, 0)
            attn_grads(rev - 1, finp)
            mlp_fwd(1)

    outs = []

    def emit(idx, ref, c, out):
        outs.append(local(ref.at[c], out.at[rows(mine(c))], ol_s.at[idx, c]))
        outs.append(remote(ref.at[c], out.at[rows(mine(c))], os_s.at[idx, c], or_s.at[idx, c], core_peer))
        outs[-2].start()
        outs[-1].start()

    for c in (0, 1):
        finish(2, c, None, d2f, x2r[c])
        emit(3, d2f, c, od2)
        emit(2, d1f, c, od1)
        emit(1, x2r, c, ox2)
    for c in (0, 1):
        v_start(False, True, 0, c)
    for c in (0, 1):
        v_wait(c)
        vbuf[c] = vbuf[c] - g_total(c)
        emit(0, vbuf, c, ox1)
    for cp in outs:
        cp.wait()


def solution(mesh):
    act_spec = P("dp", None, None)
    saved_spec = P(None, "dp", None, None)
    weight_specs = (P(None, None, None, "tp", None), P(None, "tp", None, None), P(None, None, "tp"), P(None, "tp", None))
    grad_specs = (P("dp", None, None, "tp", None), P("dp", "tp", None, None), P("dp", None, "tp"), P("dp", "tp", None))

    def per_device(y_one, y_two, dy_one, dy_two, saved_one, saved_two, w_qkv, w_o, w_in, w_out):
        n_seq, seq, hid = y_one.shape
        n_layers, _, _, heads, hdim = w_qkv.shape
        n_pairs = saved_one.shape[0]
        ff = w_in.shape[-1]
        tok = n_seq * seq
        qkv_w = 3 * heads * hdim
        flat = lambda arr: arr.reshape(arr.shape[:-3] + (tok, hid))
        wq_t = jnp.transpose(w_qkv, (0, 2, 3, 4, 1)).reshape(n_layers, qkv_w, hid)
        wo_t = w_o.reshape(n_layers, heads * hdim, hid)
        sds = jax.ShapeDtypeStruct
        vm = pltpu.VMEM
        dma = pltpu.SemaphoreType.DMA
        half = (2, seq, hid)
        scratch = [
            vm((2, qkv_w, hid), BF), vm((2, heads * hdim, hid), BF), vm((2, hid, ff), BF), vm((2, ff, hid), BF),
            vm((tok, hid), BF), vm((tok, ff), BF), vm((tok, ff), F32), vm((tok, ff), BF),
            vm((tok, hid), BF), vm((tok, hid), BF), vm((qkv_w, tok), BF), vm((qkv_w, tok), BF),
            vm((n_seq * heads, seq, seq), F32), vm((heads * hdim, tok), BF),
            vm((tok, hid), BF), vm((2, tok, hid), BF), vm(half, F32), vm(half, F32),
            vm(half, F32), vm(half, F32), vm(half, F32),
            vm((2,) + half, F32), vm((2,) + half, F32), vm((3,) + half, BF), vm((3,) + half, BF),
            vm((2,) + half, F32), vm(half, F32), vm(half, F32), vm((3, 256, hid), F32),
            dma((2, 2)), dma((2, 2)), dma((3, 2)), dma((3, 2)), dma((3, 2)), dma((3, 2)),
            dma((2,)), dma((2,)), dma((8,)), dma((8,)), dma((2,)), dma((2,)),
            dma((4, 2)), dma((4, 2)), dma((4, 2)), dma((2, 4)), dma((2,)), dma((2,)), dma((2,)), dma((3,)), dma((2, 2)),
            pltpu.SemaphoreType.REGULAR,
        ]
        anyspec = pl.BlockSpec(memory_space=pl.ANY)
        outs = pl.pallas_call(
            functools.partial(chain_kernel, seq, hid, heads, hdim, n_pairs),
            out_shape=[sds((tok, hid), F32)] * 4
            + [sds((n_layers, qkv_w, hid), F32), sds((n_layers, heads * hdim, hid), F32), sds((n_layers, hid, ff), F32), sds((n_layers, ff, hid), F32)],
            in_specs=[anyspec] * 10,
            out_specs=[anyspec] * 8,
            scratch_shapes=scratch,
            name="chain",
            compiler_params=pltpu.CompilerParams(collective_id=0, has_side_effects=True, vmem_limit_bytes=67043328),
        )(flat(y_one), flat(y_two), flat(dy_one), flat(dy_two), flat(saved_one), flat(saved_two), wq_t, wo_t, w_in, w_out)
        states = tuple(out.reshape(n_seq, seq, hid) for out in outs[:4])
        d_qkv = jnp.transpose(outs[4].reshape(n_layers, 3, heads, hdim, hid), (0, 4, 1, 2, 3))
        d_o = outs[5].reshape(n_layers, heads, hdim, hid)
        return states + (d_qkv, d_o, outs[6], outs[7])

    return jax.shard_map(
        per_device,
        mesh=mesh,
        in_specs=(act_spec,) * 4 + (saved_spec,) * 2 + weight_specs,
        out_specs=(act_spec,) * 4 + grad_specs,
        check_vma=False,
    )
```

```python
import functools

import jax
import jax.numpy as jnp
from jax import lax
from jax.experimental import pallas as pl
from jax.experimental.pallas import tpu as pltpu
from jax.sharding import PartitionSpec as P

EPS = 1e-6
BF = jnp.bfloat16
F32 = jnp.float32
MESH = pl.DeviceIdType.MESH
GELU_C = 0.7978845608028654
GELU_A = 0.044715

NN = (((1,), (0,)), ((), ()))
NT = (((1,), (1,)), ((), ()))
TN = (((0,), (0,)), ((), ()))


def dot(lhs, rhs, dims):
    return lax.dot_general(lhs, rhs, dims, preferred_element_type=F32)


def rms_scale(state):
    return lax.rsqrt(jnp.mean(state * state, axis=-1, keepdims=True) + EPS)


def rms_pull(state, grad):
    scale = rms_scale(state)
    normed = state * scale
    return scale * (grad - normed * jnp.mean(normed * grad, axis=-1, keepdims=True))


def gelu_parts(hidden, want_grad):
    sq = hidden * hidden
    tanh = jnp.tanh(GELU_C * (hidden + GELU_A * (sq * hidden)))
    half = 0.5 * (1.0 + tanh)
    value = hidden * half
    if not want_grad:
        return value, None
    grad = half + 0.5 * hidden * (1.0 - tanh * tanh) * (GELU_C * (1.0 + 3.0 * GELU_A * sq))
    return value, grad


def chain_kernel(
    seq, hid, heads, hdim, n_pairs,
    y1, y2, dy1, dy2, s1, s2, wq_h, wo_h, wi_h, wu_h,
    fsum, ox2, od1, od2, gq, go, gi, gu,
    wq, wo, wi, wu, a_g, act, gp, dhb, finp, finr, qkvt, dqkvt, pt, ot,
    d1b, d2b, d1f, d2f, vbuf, x2r, xl, pbuf, e1r, xs, xr, gbuf, g1r, g2r, stage,
    e1s_s, e1r_s, e2s_s, e2r_s, e3s_s, e3r_s, g1s_s, g1r_s, g2s_s, g2r_s, g3s_s, g3r_s,
    os_s, or_s, ol_s, w_s, xl_s, v_s, x2_s, st_s, d_s, gcred,
):
    me = lax.axis_index("tp")
    dp = lax.axis_index("dp")
    ci = lax.rem(me, 2)
    core_peer = (dp, me + 1 - 2 * ci)
    x_peer = (dp, lax.rem(me + 2, 4))
    qw = heads * hdim
    npc = 4
    prow = seq // npc

    barrier = pltpu.get_barrier_semaphore()
    pl.semaphore_signal(barrier, inc=1, device_id=core_peer, device_id_type=MESH)
    pl.semaphore_signal(barrier, inc=1, device_id=x_peer, device_id_type=MESH)
    pl.semaphore_wait(barrier, 2)

    def rows(seq_idx):
        return pl.ds(pl.multiple_of(seq_idx * seq, seq), seq)

    def mine(c):
        return 2 * c + ci

    def theirs(c):
        return 2 * c + 1 - ci

    def local(src, dst, sem):
        return pltpu.make_async_copy(src, dst, sem)

    def remote(src, dst, ssem, rsem, dev):
        return pltpu.make_async_remote_copy(src_ref=src, dst_ref=dst, send_sem=ssem, recv_sem=rsem, device_id=dev, device_id_type=MESH)

    def weight_copies(slot, blk, which):
        pairs = {"q": (wq_h, wq), "o": (wo_h, wo), "i": (wi_h, wi), "u": (wu_h, wu)}
        return [local(pairs[k][0].at[blk], pairs[k][1].at[slot], w_s.at[slot, "qoiu".index(k)]) for k in which]

    def w_start(slot, blk, which):
        for cp in weight_copies(slot, blk, which):
            cp.start()

    def w_wait(slot, which):
        for cp in weight_copies(slot, 0, which):
            cp.wait()

    def state_start(first, one, pair, rws, dst, sem):
        top, saved = (y1, s1) if one else (y2, s2)
        if first is True:
            local(top.at[rws], dst, sem).start()
        elif first is False:
            local(saved.at[pair, rws], dst, sem).start()
        else:
            @pl.when(first)
            def _():
                local(top.at[rws], dst, sem).start()

            @pl.when(jnp.logical_not(first))
            def _():
                local(saved.at[jnp.minimum(pair, n_pairs - 1), rws], dst, sem).start()

    def state_wait(dst, sem):
        local(y1.at[rows(0)], dst, sem).wait()

    def each_seq(first, one, pair, body, order=lambda i: i):
        for i in (0, 1):
            state_start(first, one, pair, rows(order(i)), xl.at[i], xl_s.at[i])

        @pl.loop(0, 4)
        def _(i):
            slot = lax.rem(i, 2)
            state_wait(xl.at[slot], xl_s.at[slot])
            body(i, order(i), xl[slot])

            @pl.when(i < 2)
            def _():
                state_start(first, one, pair, rows(order(i + 2)), xl.at[slot], xl_s.at[slot])

    def mlp_fwd(slot):
        @pl.loop(0, 4)
        def _(s):
            value, grad = gelu_parts(dot(a_g[rows(s), :], wi[slot], NN), True)
            act[rows(s), :] = value.astype(BF)
            gp[rows(s), :] = grad

    def attn_fwd_seq(slot, fin, s):
        cols = rows(s)
        qkv = dot(wq[slot], fin[cols, :], NT).astype(BF)
        qkvt[:, cols] = qkv
        for h in range(heads):
            q_t = qkv[h * hdim:(h + 1) * hdim]
            k_t = qkv[qw + h * hdim:qw + (h + 1) * hdim]
            v_t = qkv[2 * qw + h * hdim:2 * qw + (h + 1) * hdim]
            sc = dot(k_t, q_t, TN) * (hdim ** -0.5)
            ex = jnp.exp(sc - jnp.max(sc, axis=0, keepdims=True))
            prob = ex * (1.0 / jnp.sum(ex, axis=0, keepdims=True))
            pt[s * heads + h] = prob
            ot[h * hdim:(h + 1) * hdim, cols] = dot(v_t, prob.astype(BF), NN).astype(BF)

    def attn_fwd_plain(pair):
        def body(i, s, state):
            finp[rows(s), :] = (state * rms_scale(state)).astype(BF)
            attn_fwd_seq(0, finp, s)
        each_seq(False, False, pair, body)

    def attn_fwd_rev():
        @pl.loop(0, 4)
        def _(s):
            attn_fwd_seq(1, finr, s)

    def e1(slot, c):
        return remote(pbuf.at[c, 0], e1r.at[slot, c], e1s_s.at[slot, c], e1r_s.at[slot, c], core_peer)

    def e2(t, c):
        return remote(xs.at[t, c], xr.at[t, c], e2s_s.at[t, c], e2r_s.at[t, c], x_peer)

    def part_g(slot, ver, c, mode, e1_slot=None):
        @pl.loop(0, 2)
        def _(i):
            s = 2 * c + jnp.where(i == 0, 1 - ci, ci)
            d_act = dot(d2b[ver, rows(s), :], wu[slot], NT)
            dh = (d_act * gp[rows(s), :]).astype(BF)
            dhb[rows(s), :] = dh
            part = dot(dh, wi[slot], NT)
            pbuf[c, i] = pbuf[c, i] + part if mode == "add" else part
            if mode != "hold":
                @pl.when(i == 0)
                def _():
                    e1(e1_slot, c).start()

    def part_f(slot, c, e1_slot):
        @pl.loop(0, 2)
        def _(i):
            s = 2 * c + jnp.where(i == 0, 1 - ci, ci)
            cols = rows(s)
            do_t = dot(wo[slot], d1b[cols, :], NT).astype(BF)
            for h in range(heads):
                lo = h * hdim
                do_h = do_t[lo:lo + hdim]
                prob = pt[s * heads + h]
                q_t = qkvt[lo:lo + hdim, cols]
                k_t = qkvt[qw + lo:qw + lo + hdim, cols]
                v_t = qkvt[2 * qw + lo:2 * qw + lo + hdim, cols]
                dqkvt[2 * qw + lo:2 * qw + lo + hdim, cols] = dot(do_h, prob.astype(BF), NT).astype(BF)
                dp_t = dot(v_t, do_h, TN)
                inner = jnp.sum(prob * dp_t, axis=0, keepdims=True)
                ds = (prob * (dp_t - inner) * (hdim ** -0.5)).astype(BF)
                dqkvt[lo:lo + hdim, cols] = dot(k_t, ds, NN).astype(BF)
                dqkvt[qw + lo:qw + lo + hdim, cols] = dot(q_t, ds, NT).astype(BF)
            pbuf[c, i] = dot(dqkvt[:, cols], wq[slot], TN)

            @pl.when(i == 0)
            def _():
                e1(e1_slot, c).start()

    def to_x(t, c, e1_slot):
        e1(e1_slot, c).wait()
        xs[t, c] = (pbuf[c, 1] + e1r[e1_slot, c]).astype(BF)
        e2(t, c).start()

    def summed(t, c):
        e2(t, c).wait()
        return xs[t, c].astype(F32) + xr[t, c].astype(F32)

    def e3(kind, c):
        ref = d1b.at[rows(mine(c))] if kind == 0 else d2b.at[kind - 1, rows(mine(c))]
        return remote(ref, ref, e3s_s.at[kind, c], e3r_s.at[kind, c], core_peer)

    def finish(t, c, kind, acc, state):
        total = acc[c] + rms_pull(state, summed(t, c))
        acc[c] = total
        if kind is not None:
            if kind == 0:
                d1b[rows(mine(c)), :] = total.astype(BF)
            else:
                d2b[kind - 1, rows(mine(c)), :] = total.astype(BF)
            e3(kind, c).start()

    def g1(c):
        return remote(gbuf.at[c, 0], g1r.at[c], g1s_s.at[c], g1r_s.at[c], core_peer)

    def g2(k):
        c, q = k // npc, k % npc
        rws = pl.ds(q * prow, prow)
        return remote(gbuf.at[c, 1, rws], g2r.at[c, rws], g2s_s.at[k], g2r_s.at[k], x_peer)

    def g_order(i):
        return 2 * (i // 2) + jnp.where(lax.rem(i, 2) == 0, 1 - ci, ci)

    def g_send_core(i):
        for c in (0, 1):
            @pl.when(i == 2 * c)
            def _():
                g1(c).start()

    def g_part(slot, first, pair, keep):
        def body(i, s, state):
            normed = (state * rms_scale(state)).astype(BF)
            a_g[rows(s), :] = normed
            value, grad = gelu_parts(dot(normed, wi[slot], NN), keep)
            value = value.astype(BF)
            if keep:
                act[rows(s), :] = value
                gp[rows(s), :] = grad
            gbuf[i // 2, lax.rem(i, 2)] = dot(value, wu[slot], NN)
            g_send_core(i)
        each_seq(first, True, pair, body, g_order)

    def f_part(slot):
        @pl.loop(0, 4)
        def _(i):
            gbuf[i // 2, lax.rem(i, 2)] = dot(ot[:, rows(g_order(i))], wo[slot], TN)
            g_send_core(i)

    def g_chip(c):
        g1(c).wait()
        gbuf[c, 1] = gbuf[c, 1] + g1r[c]

    def g_send(*ks):
        for k in ks:
            g2(k).start()

    def g_total(c):
        for q in range(npc):
            g2(c * npc + q).wait()
        return gbuf[c, 1] + g2r[c]

    def g3(c):
        ref = finr.at[rows(mine(c))]
        return remote(ref, ref, g3s_s.at[c], g3r_s.at[c], core_peer)

    def g_finish(c):
        state_wait(x2r.at[c], x2_s.at[c])
        state = x2r[c] - g_total(c)
        x2r[c] = state
        finr[rows(mine(c)), :] = (state * rms_scale(state)).astype(BF)
        g3(c).start()

    def f_out(c):
        return local(gbuf.at[c, 1], fsum.at[c], ol_s.at[0, c])

    def g_credit():
        pl.semaphore_signal(gcred, inc=1, device_id=x_peer, device_id_type=MESH)

    def put(pending, tile, dst, value):
        slot = tile % 3
        height = value.shape[0]
        if pending[slot] is not None:
            pending[slot].wait()
        stage[slot, :height] = value
        cp = local(stage.at[slot, pl.ds(0, height)], dst, st_s.at[slot])
        cp.start()
        pending[slot] = cp

    def flush(pending):
        for cp in pending:
            if cp is not None:
                cp.wait()

    def mlp_grads(blk, ver):
        pending = [None] * 3
        n_t = hid // 256
        for k in range(n_t):
            put(pending, k, gu.at[blk, pl.ds(256 * k, 256)], dot(act[:, 256 * k:256 * (k + 1)], d2b[ver], TN))
        for k in range(n_t):
            put(pending, k, gi.at[blk, pl.ds(256 * k, 256)], dot(a_g[:, 256 * k:256 * (k + 1)], dhb[...], TN))
        flush(pending)

    def attn_grads(blk, fin):
        pending = [None] * 3
        for k in range(3):
            put(pending, k, gq.at[blk, pl.ds(qw * k, qw)], dot(dqkvt[qw * k:qw * (k + 1), :], fin[...], NN))
        put(pending, 3, go.at[blk], dot(ot[...], d1b[...], NN))
        flush(pending)

    def v_start(first, one, pair, c):
        state_start(first, one, pair, rows(mine(c)), vbuf.at[c], v_s.at[c])

    def v_wait(c):
        state_wait(vbuf.at[c], v_s.at[c])

    top = 2 * n_pairs
    w_start(1, top, "iuqo")
    for c in (0, 1):
        v_start(True, True, 0, c)
        state_start(True, False, 0, rows(mine(c)), x2r.at[c], x2_s.at[c])
        local(dy1.at[rows(mine(c))], d1f.at[c], d_s.at[0, c]).start()
        local(dy2.at[rows(mine(c))], d2f.at[c], d_s.at[1, c]).start()
    w_wait(1, "iu")
    g_part(1, True, 0, True)
    for c in (0, 1):
        g_chip(c)
        g_send(*range(npc * c, npc * (c + 1)))
    w_start(0, top - 1, "qoiu")
    for i in range(4):
        local(dy2.at[rows(i)], xl.at[i % 2], xl_s.at[i % 2]).start()
        state_wait(xl.at[i % 2], xl_s.at[i % 2])
        d2b[1, rows(i), :] = xl[i % 2].astype(BF)
    for c in (0, 1):
        local(dy1.at[rows(mine(c))], d1f.at[c], d_s.at[0, c]).wait()
        local(dy2.at[rows(mine(c))], d2f.at[c], d_s.at[1, c]).wait()

    @pl.loop(0, n_pairs + 1)
    def _(it):
        pair = n_pairs - it
        is_top = it == 0
        more = it < n_pairs
        rev = 2 * pair
        even, odd = lax.rem(it, 2), lax.rem(it + 1, 2)

        @pl.when(is_top)
        def _():
            for c in (0, 1):
                part_g(1, 1, c, "first", odd)
                to_x(1, c, odd)

        @pl.when(it > 0)
        def _():
            for c in (0, 1):
                v_wait(c)
                finish(0, c, 2, d2f, vbuf[c])
                v_start(False, True, pair, c)
                e3(2, c).wait()
                part_g(1, 1, c, "add", odd)
                to_x(1, c, odd)

        @pl.when(more)
        def _():
            w_start(1, rev - 2, "iu")

        for c in (0, 1):
            g_finish(c)

        @pl.when(more)
        def _():
            g_credit()
        w_wait(1, "qo")
        for c in (0, 1):
            g3(c).wait()
        attn_fwd_rev()

        for c in (0, 1):
            v_wait(c)
            finish(1, c, 0, d1f, vbuf[c])
            e3(0, c).wait()
            part_f(1, c, even)
            to_x(2, c, even)
        attn_grads(rev, finr)

        @pl.when(more)
        def _():
            w_start(1, rev - 2, "qo")
            for c in (0, 1):
                v_start(False, False, pair - 1, c)
            w_wait(0, "qo")
            attn_fwd_plain(pair - 1)
            for c in (0, 1):
                part_f(0, c, odd)
                to_x(0, c, odd)
        mlp_grads(rev, 1)

        @pl.when(more)
        def _():
            w_wait(1, "iu")
            g_part(1, False, pair - 1, False)

        @pl.when(jnp.logical_not(more))
        def _():
            f_part(1)

        for c in (0, 1):
            g_chip(c)

        @pl.when(jnp.logical_not(more))
        def _():
            for c in (0, 1):
                f_out(c).start()

        @pl.when(more)
        def _():
            pl.semaphore_wait(gcred, 1)
            g_send(*range(2 * npc))
            w_wait(0, "iu")
            mlp_fwd(0)
            for c in (0, 1):
                finish(2, c, 1, d2f, x2r[c])
                state_start(False, False, pair - 1, rows(mine(c)), x2r.at[c], x2_s.at[c])
            for c in (0, 1):
                e3(1, c).wait()
                part_g(0, 0, c, "hold")

            @pl.when(it < n_pairs - 1)
            def _():
                w_start(0, rev - 3, "qoiu")
            mlp_grads(rev - 1, 0)
            attn_grads(rev - 1, finp)
            mlp_fwd(1)

    outs = []

    def emit(idx, ref, c, out):
        outs.append(local(ref.at[c], out.at[rows(mine(c))], ol_s.at[idx, c]))
        outs.append(remote(ref.at[c], out.at[rows(mine(c))], os_s.at[idx, c], or_s.at[idx, c], core_peer))
        outs[-2].start()
        outs[-1].start()

    for c in (0, 1):
        finish(2, c, None, d2f, x2r[c])
        emit(3, d2f, c, od2)
        emit(2, d1f, c, od1)
        emit(1, x2r, c, ox2)
    for c in (0, 1):
        f_out(c).wait()
    for cp in outs:
        cp.wait()


def move_kernel(depth, chunk, *refs):
    count = (len(refs) - 3) // 2
    buf, in_s, out_s = refs[-3:]
    jobs = []
    for src, dst in zip(refs[:count], refs[count:2 * count]):
        for lo in range(0, src.shape[0], chunk):
            rws = pl.ds(lo, min(chunk, src.shape[0] - lo))
            slot = len(jobs) % depth
            part = buf.at[slot, pl.ds(0, rws.size)]
            jobs.append((
                pltpu.make_async_copy(src.at[rws], part, in_s.at[slot]),
                pltpu.make_async_copy(part, dst.at[rws], out_s.at[slot]),
            ))
    for load, _ in jobs[:depth]:
        load.start()
    lag = depth // 2
    for k in range(len(jobs)):
        jobs[k][0].wait()
        jobs[k][1].start()
        if k >= lag:
            jobs[k - lag][1].wait()
            if k - lag + depth < len(jobs):
                jobs[k - lag + depth][0].start()
    for k in range(max(len(jobs) - lag, 0), len(jobs)):
        jobs[k][1].wait()


def move(arrays, name, depth=12, chunk=576):
    width = arrays[0].shape[-1]
    size = sum(arr.size for arr in arrays)
    depth = min(depth, sum(-(-arr.shape[0] // chunk) for arr in arrays))
    anyspec = pl.BlockSpec(memory_space=pl.ANY)
    return pl.pallas_call(
        functools.partial(move_kernel, depth, chunk),
        out_shape=[jax.ShapeDtypeStruct(arr.shape, arr.dtype) for arr in arrays],
        in_specs=[anyspec] * len(arrays),
        out_specs=[anyspec] * len(arrays),
        scratch_shapes=[pltpu.VMEM((depth, chunk, width), F32), pltpu.SemaphoreType.DMA((depth,)), pltpu.SemaphoreType.DMA((depth,))],
        name=name,
        cost_estimate=pl.CostEstimate(flops=400 * size, bytes_accessed=8 * size, transcendentals=0),
        compiler_params=pltpu.CompilerParams(vmem_limit_bytes=60 * 2 ** 20),
    )(*arrays)


def join_kernel(y_ref, own_ref, peer_ref, out_ref):
    odd = lax.rem(pl.program_id(0) + lax.axis_index("tp"), 2)

    @pl.when(odd == 0)
    def _():
        out_ref[...] = y_ref[...] - own_ref[...]

    @pl.when(odd != 0)
    def _():
        out_ref[...] = y_ref[...] - peer_ref[...]


def join(y_all, own, peer):
    _, n_seq, seq, hid = y_all.shape
    bottom = pl.BlockSpec((None, 1, seq, hid), lambda s: (0, s, 0, 0))
    whole = pl.BlockSpec((1, seq, hid), lambda s: (s, 0, 0))
    half = pl.BlockSpec((1, seq, hid), lambda s: (s // 2, 0, 0))
    return pl.pallas_call(
        join_kernel,
        out_shape=jax.ShapeDtypeStruct(y_all.shape[1:], F32),
        grid=(n_seq,),
        in_specs=[bottom, half, half],
        out_specs=whole,
        name="join",
    )(y_all, own, peer)


def solution(mesh):
    act_spec = P("dp", None, None)
    saved_spec = P(None, "dp", None, None)
    weight_specs = (P(None, None, None, "tp", None), P(None, "tp", None, None), P(None, None, "tp"), P(None, "tp", None))
    grad_specs = (P("dp", None, None, "tp", None), P("dp", "tp", None, None), P("dp", None, "tp"), P("dp", "tp", None))

    def per_device(y_one, y_two, dy_one, dy_two, saved_one, saved_two, w_qkv, w_o, w_in, w_out):
        n_seq, seq, hid = y_one.shape
        n_layers, _, _, heads, hdim = w_qkv.shape
        n_pairs = saved_one.shape[0]
        ff = w_in.shape[-1]
        tok = n_seq * seq
        qkv_w = 3 * heads * hdim
        flat = lambda arr: arr.reshape(arr.shape[:-3] + (tok, hid))
        wq_t = jnp.transpose(w_qkv, (0, 2, 3, 4, 1)).reshape(n_layers, qkv_w, hid)
        wo_t = w_o.reshape(n_layers, heads * hdim, hid)
        sds = jax.ShapeDtypeStruct
        vm = pltpu.VMEM
        dma = pltpu.SemaphoreType.DMA
        half = (2, seq, hid)
        scratch = [
            vm((2, qkv_w, hid), BF), vm((2, heads * hdim, hid), BF), vm((2, hid, ff), BF), vm((2, ff, hid), BF),
            vm((tok, hid), BF), vm((tok, ff), BF), vm((tok, ff), F32), vm((tok, ff), BF),
            vm((tok, hid), BF), vm((tok, hid), BF), vm((qkv_w, tok), BF), vm((qkv_w, tok), BF),
            vm((n_seq * heads, seq, seq), F32), vm((heads * hdim, tok), BF),
            vm((tok, hid), BF), vm((2, tok, hid), BF), vm(half, F32), vm(half, F32),
            vm(half, F32), vm(half, F32), vm(half, F32),
            vm((2,) + half, F32), vm((2,) + half, F32), vm((3,) + half, BF), vm((3,) + half, BF),
            vm((2,) + half, F32), vm(half, F32), vm(half, F32), vm((3, 256, hid), F32),
            dma((2, 2)), dma((2, 2)), dma((3, 2)), dma((3, 2)), dma((3, 2)), dma((3, 2)),
            dma((2,)), dma((2,)), dma((8,)), dma((8,)), dma((2,)), dma((2,)),
            dma((4, 2)), dma((4, 2)), dma((4, 2)), dma((2, 4)), dma((2,)), dma((2,)), dma((2,)), dma((3,)), dma((2, 2)),
            pltpu.SemaphoreType.REGULAR,
        ]
        anyspec = pl.BlockSpec(memory_space=pl.ANY)
        outs = pl.pallas_call(
            functools.partial(chain_kernel, seq, hid, heads, hdim, n_pairs),
            out_shape=[sds(half, F32)] + [sds((tok, hid), F32)] * 3
            + [sds((n_layers, qkv_w, hid), F32), sds((n_layers, heads * hdim, hid), F32), sds((n_layers, hid, ff), F32), sds((n_layers, ff, hid), F32)],
            in_specs=[anyspec] * 10,
            out_specs=[anyspec] * 8,
            scratch_shapes=scratch,
            name="chain",
            compiler_params=pltpu.CompilerParams(collective_id=0, has_side_effects=True, vmem_limit_bytes=67043328),
        )(flat(y_one), flat(y_two), flat(dy_one), flat(dy_two), flat(saved_one), flat(saved_two), wq_t, wo_t, w_in, w_out)
        f_own = outs[0]
        f_other = lax.ppermute(f_own, "tp", [(0, 2), (2, 0), (1, 3), (3, 1)])
        grads = move([out.reshape(-1, hid) for out in outs[4:]], "move_grads")
        f_other, grads = lax.optimization_barrier((f_other, grads))
        f_sum = f_own + f_other
        f_peer = lax.ppermute(f_sum, "tp", [(0, 1), (1, 0), (2, 3), (3, 2)])
        states = [out.reshape(n_seq, seq, hid) for out in move(outs[1:4], "move_states")]
        x_one = join(saved_one, f_sum, f_peer)
        d_qkv = jnp.transpose(grads[0].reshape(n_layers, 3, heads, hdim, hid), (0, 4, 1, 2, 3))
        d_o = grads[1].reshape(n_layers, heads, hdim, hid)
        return (x_one, *states, d_qkv, d_o, grads[2].reshape(n_layers, hid, ff), grads[3].reshape(n_layers, ff, hid))

    return jax.shard_map(
        per_device,
        mesh=mesh,
        in_specs=(act_spec,) * 4 + (saved_spec,) * 2 + weight_specs,
        out_specs=(act_spec,) * 4 + grad_specs,
        check_vma=False,
    )
```

```python
import functools

import jax
import jax.numpy as jnp
from jax import lax
from jax.experimental import pallas as pl
from jax.experimental.pallas import tpu as pltpu
from jax.sharding import PartitionSpec as P

EPS = 1e-6
BF = jnp.bfloat16
F32 = jnp.float32
MESH = pl.DeviceIdType.MESH
GELU_C = 0.7978845608028654
GELU_A = 0.044715

NN = (((1,), (0,)), ((), ()))
NT = (((1,), (1,)), ((), ()))
TN = (((0,), (0,)), ((), ()))


def dot(lhs, rhs, dims):
    return lax.dot_general(lhs, rhs, dims, preferred_element_type=F32)


def rms_scale(state):
    return lax.rsqrt(jnp.mean(state * state, axis=-1, keepdims=True) + EPS)


def rms_pull(state, grad):
    scale = rms_scale(state)
    normed = state * scale
    return scale * (grad - normed * jnp.mean(normed * grad, axis=-1, keepdims=True))


def gelu_parts(hidden, want_grad):
    sq = hidden * hidden
    tanh = jnp.tanh(GELU_C * (hidden + GELU_A * (sq * hidden)))
    half = 0.5 * (1.0 + tanh)
    value = hidden * half
    if not want_grad:
        return value, None
    grad = half + 0.5 * hidden * (1.0 - tanh * tanh) * (GELU_C * (1.0 + 3.0 * GELU_A * sq))
    return value, grad


def chain_kernel(
    seq, hid, heads, hdim, n_pairs,
    y1, y2, dy1, dy2, s1, s2, wq_h, wo_h, wi_h, wu_h,
    fsum, ox2, od1, od2, gq, go, gi, gu,
    wq, wo, wi, wu, a_g, act, gp, dhb, finp, finr, qkvt, dqkvt, pt, ot,
    d1b, d2b, d1f, d2f, vbuf, x2r, xl, pbuf, e1r, xs, xr, gbuf, g1r, g2r, stage,
    e1s_s, e1r_s, e2s_s, e2r_s, e3s_s, e3r_s, g1s_s, g1r_s, g2s_s, g2r_s, g3s_s, g3r_s,
    os_s, or_s, ol_s, w_s, xl_s, v_s, x2_s, st_s, d_s, gcred,
):
    me = lax.axis_index("tp")
    dp = lax.axis_index("dp")
    ci = lax.rem(me, 2)
    core_peer = (dp, me + 1 - 2 * ci)
    x_peer = (dp, lax.rem(me + 2, 4))
    qw = heads * hdim
    npc = 4
    prow = seq // npc

    barrier = pltpu.get_barrier_semaphore()
    pl.semaphore_signal(barrier, inc=1, device_id=core_peer, device_id_type=MESH)
    pl.semaphore_signal(barrier, inc=1, device_id=x_peer, device_id_type=MESH)
    pl.semaphore_wait(barrier, 2)

    def rows(seq_idx):
        return pl.ds(pl.multiple_of(seq_idx * seq, seq), seq)

    def mine(c):
        return 2 * c + ci

    def theirs(c):
        return 2 * c + 1 - ci

    def local(src, dst, sem):
        return pltpu.make_async_copy(src, dst, sem)

    def remote(src, dst, ssem, rsem, dev):
        return pltpu.make_async_remote_copy(src_ref=src, dst_ref=dst, send_sem=ssem, recv_sem=rsem, device_id=dev, device_id_type=MESH)

    def weight_copies(slot, blk, which):
        pairs = {"q": (wq_h, wq), "o": (wo_h, wo), "i": (wi_h, wi), "u": (wu_h, wu)}
        return [local(pairs[k][0].at[blk], pairs[k][1].at[slot], w_s.at[slot, "qoiu".index(k)]) for k in which]

    def w_start(slot, blk, which):
        for cp in weight_copies(slot, blk, which):
            cp.start()

    def w_wait(slot, which):
        for cp in weight_copies(slot, 0, which):
            cp.wait()

    def state_start(first, one, pair, rws, dst, sem):
        top, saved = (y1, s1) if one else (y2, s2)
        if first is True:
            local(top.at[rws], dst, sem).start()
        elif first is False:
            local(saved.at[pair, rws], dst, sem).start()
        else:
            @pl.when(first)
            def _():
                local(top.at[rws], dst, sem).start()

            @pl.when(jnp.logical_not(first))
            def _():
                local(saved.at[jnp.minimum(pair, n_pairs - 1), rws], dst, sem).start()

    def state_wait(dst, sem):
        local(y1.at[rows(0)], dst, sem).wait()

    def each_seq(first, one, pair, body, order=lambda i: i):
        for i in (0, 1):
            state_start(first, one, pair, rows(order(i)), xl.at[i], xl_s.at[i])

        @pl.loop(0, 4)
        def _(i):
            slot = lax.rem(i, 2)
            state_wait(xl.at[slot], xl_s.at[slot])
            body(i, order(i), xl[slot])

            @pl.when(i < 2)
            def _():
                state_start(first, one, pair, rows(order(i + 2)), xl.at[slot], xl_s.at[slot])

    def mlp_fwd(slot):
        @pl.loop(0, 4)
        def _(s):
            value, grad = gelu_parts(dot(a_g[rows(s), :], wi[slot], NN), True)
            act[rows(s), :] = value.astype(BF)
            gp[rows(s), :] = grad

    def attn_fwd_seq(slot, fin, s):
        cols = rows(s)
        qkv = dot(wq[slot], fin[cols, :], NT).astype(BF)
        qkvt[:, cols] = qkv
        part = lambda j, h: qkv[j * qw + h * hdim:j * qw + (h + 1) * hdim]
        scores = [dot(part(1, h), part(0, h), TN) * (hdim ** -0.5) for h in range(heads)]
        exps = [jnp.exp(sc - jnp.max(sc, axis=0, keepdims=True)) for sc in scores]
        probs = [ex * (1.0 / jnp.sum(ex, axis=0, keepdims=True)) for ex in exps]
        for h in range(heads):
            pt[s * heads + h] = probs[h]
        for h in range(heads):
            ot[h * hdim:(h + 1) * hdim, cols] = dot(part(2, h), probs[h].astype(BF), NN).astype(BF)

    def attn_fwd_plain(pair):
        def body(i, s, state):
            finp[rows(s), :] = (state * rms_scale(state)).astype(BF)
            attn_fwd_seq(0, finp, s)
        each_seq(False, False, pair, body)

    def attn_fwd_rev():
        @pl.loop(0, 4)
        def _(s):
            attn_fwd_seq(1, finr, s)

    def e1(slot, c):
        return remote(pbuf.at[c, 0], e1r.at[slot, c], e1s_s.at[slot, c], e1r_s.at[slot, c], core_peer)

    def e2(t, c):
        return remote(xs.at[t, c], xr.at[t, c], e2s_s.at[t, c], e2r_s.at[t, c], x_peer)

    def part_g(slot, ver, c, mode, e1_slot=None):
        for i, s in enumerate((theirs(c), mine(c))):
            d_act = dot(d2b[ver, rows(s), :], wu[slot], NT)
            dh = (d_act * gp[rows(s), :]).astype(BF)
            dhb[rows(s), :] = dh
            part = dot(dh, wi[slot], NT)
            pbuf[c, i] = pbuf[c, i] + part if mode == "add" else part
            if mode != "hold" and i == 0:
                e1(e1_slot, c).start()

    def part_f(slot, c, e1_slot):
        each = range(heads)
        for i, s in enumerate((theirs(c), mine(c))):
            cols = rows(s)
            do_t = dot(wo[slot], d1b[cols, :], NT).astype(BF)
            do = [do_t[h * hdim:(h + 1) * hdim] for h in each]
            part = lambda j, h: qkvt[j * qw + h * hdim:j * qw + (h + 1) * hdim, cols]
            probs = [pt[s * heads + h] for h in each]
            dps = [dot(part(2, h), do[h], TN) for h in each]
            dv = [dot(do[h], probs[h].astype(BF), NT).astype(BF) for h in each]
            ds = []
            for h in each:
                inner = jnp.sum(probs[h] * dps[h], axis=0, keepdims=True)
                ds.append((probs[h] * (dps[h] - inner) * (hdim ** -0.5)).astype(BF))
            dq = [dot(part(1, h), ds[h], NN).astype(BF) for h in each]
            dk = [dot(part(0, h), ds[h], NT).astype(BF) for h in each]
            d_qkv = jnp.concatenate(dq + dk + dv, axis=0)
            dqkvt[:, cols] = d_qkv
            pbuf[c, i] = dot(d_qkv, wq[slot], TN)
            if i == 0:
                e1(e1_slot, c).start()

    def to_x(t, c, e1_slot):
        e1(e1_slot, c).wait()
        xs[t, c] = (pbuf[c, 1] + e1r[e1_slot, c]).astype(BF)
        e2(t, c).start()

    def summed(t, c):
        e2(t, c).wait()
        return xs[t, c].astype(F32) + xr[t, c].astype(F32)

    def e3(kind, c):
        ref = d1b.at[rows(mine(c))] if kind == 0 else d2b.at[kind - 1, rows(mine(c))]
        return remote(ref, ref, e3s_s.at[kind, c], e3r_s.at[kind, c], core_peer)

    def finish(t, c, kind, acc, state):
        total = acc[c] + rms_pull(state, summed(t, c))
        acc[c] = total
        if kind is not None:
            if kind == 0:
                d1b[rows(mine(c)), :] = total.astype(BF)
            else:
                d2b[kind - 1, rows(mine(c)), :] = total.astype(BF)
            e3(kind, c).start()

    def g1(c):
        return remote(gbuf.at[c, 0], g1r.at[c], g1s_s.at[c], g1r_s.at[c], core_peer)

    def g2(k):
        c, q = k // npc, k % npc
        rws = pl.ds(q * prow, prow)
        return remote(gbuf.at[c, 1, rws], g2r.at[c, rws], g2s_s.at[k], g2r_s.at[k], x_peer)

    def g_order(i):
        return 2 * (i // 2) + jnp.where(lax.rem(i, 2) == 0, 1 - ci, ci)

    def g_send_core(i):
        for c in (0, 1):
            @pl.when(i == 2 * c)
            def _():
                g1(c).start()

    def g_part(slot, first, pair, keep):
        def body(i, s, state):
            normed = (state * rms_scale(state)).astype(BF)
            a_g[rows(s), :] = normed
            value, grad = gelu_parts(dot(normed, wi[slot], NN), keep)
            value = value.astype(BF)
            if keep:
                act[rows(s), :] = value
                gp[rows(s), :] = grad
            gbuf[i // 2, lax.rem(i, 2)] = dot(value, wu[slot], NN)
            g_send_core(i)
        each_seq(first, True, pair, body, g_order)

    def f_part(slot):
        @pl.loop(0, 4)
        def _(i):
            gbuf[i // 2, lax.rem(i, 2)] = dot(ot[:, rows(g_order(i))], wo[slot], TN)
            g_send_core(i)

    def g_chip(c):
        g1(c).wait()
        gbuf[c, 1] = gbuf[c, 1] + g1r[c]

    def g_send(*ks):
        for k in ks:
            g2(k).start()

    def g_total(c):
        for q in range(npc):
            g2(c * npc + q).wait()
        return gbuf[c, 1] + g2r[c]

    def g3(c):
        ref = finr.at[rows(mine(c))]
        return remote(ref, ref, g3s_s.at[c], g3r_s.at[c], core_peer)

    def g_finish(c):
        state_wait(x2r.at[c], x2_s.at[c])
        state = x2r[c] - g_total(c)
        x2r[c] = state
        finr[rows(mine(c)), :] = (state * rms_scale(state)).astype(BF)
        g3(c).start()

    def f_out(c):
        return local(gbuf.at[c, 1], fsum.at[c], ol_s.at[0, c])

    def g_credit():
        pl.semaphore_signal(gcred, inc=1, device_id=x_peer, device_id_type=MESH)

    def put(pending, tile, dst, value):
        slot = tile % 3
        height = value.shape[0]
        if pending[slot] is not None:
            pending[slot].wait()
        stage[slot, :height] = value
        cp = local(stage.at[slot, pl.ds(0, height)], dst, st_s.at[slot])
        cp.start()
        pending[slot] = cp

    def flush(pending):
        for cp in pending:
            if cp is not None:
                cp.wait()

    def mlp_grads(blk, ver):
        pending = [None] * 3
        n_t = hid // 256
        for k in range(n_t):
            put(pending, k, gu.at[blk, pl.ds(256 * k, 256)], dot(act[:, 256 * k:256 * (k + 1)], d2b[ver], TN))
        for k in range(n_t):
            put(pending, k, gi.at[blk, pl.ds(256 * k, 256)], dot(a_g[:, 256 * k:256 * (k + 1)], dhb[...], TN))
        flush(pending)

    def attn_grads(blk, fin):
        pending = [None] * 3
        for k in range(3):
            put(pending, k, gq.at[blk, pl.ds(qw * k, qw)], dot(dqkvt[qw * k:qw * (k + 1), :], fin[...], NN))
        put(pending, 3, go.at[blk], dot(ot[...], d1b[...], NN))
        flush(pending)

    def v_start(first, one, pair, c):
        state_start(first, one, pair, rows(mine(c)), vbuf.at[c], v_s.at[c])

    def v_wait(c):
        state_wait(vbuf.at[c], v_s.at[c])

    top = 2 * n_pairs
    w_start(1, top, "iuqo")
    for c in (0, 1):
        v_start(True, True, 0, c)
        state_start(True, False, 0, rows(mine(c)), x2r.at[c], x2_s.at[c])
        local(dy1.at[rows(mine(c))], d1f.at[c], d_s.at[0, c]).start()
        local(dy2.at[rows(mine(c))], d2f.at[c], d_s.at[1, c]).start()
    w_wait(1, "iu")
    g_part(1, True, 0, True)
    for c in (0, 1):
        g_chip(c)
        g_send(*range(npc * c, npc * (c + 1)))
    w_start(0, top - 1, "qoiu")
    for i in range(4):
        local(dy2.at[rows(i)], xl.at[i % 2], xl_s.at[i % 2]).start()
        state_wait(xl.at[i % 2], xl_s.at[i % 2])
        d2b[1, rows(i), :] = xl[i % 2].astype(BF)
    for c in (0, 1):
        local(dy1.at[rows(mine(c))], d1f.at[c], d_s.at[0, c]).wait()
        local(dy2.at[rows(mine(c))], d2f.at[c], d_s.at[1, c]).wait()

    @pl.loop(0, n_pairs + 1)
    def _(it):
        pair = n_pairs - it
        is_top = it == 0
        more = it < n_pairs
        rev = 2 * pair
        even, odd = lax.rem(it, 2), lax.rem(it + 1, 2)

        @pl.when(is_top)
        def _():
            @pl.loop(0, 2)
            def _(c):
                part_g(1, 1, c, "first", odd)
                to_x(1, c, odd)

        @pl.when(it > 0)
        def _():
            @pl.loop(0, 2)
            def _(c):
                v_wait(c)
                finish(0, c, 2, d2f, vbuf[c])
                v_start(False, True, pair, c)
                e3(2, c).wait()
                part_g(1, 1, c, "add", odd)
                to_x(1, c, odd)

        @pl.when(more)
        def _():
            w_start(1, rev - 2, "iu")

        for c in (0, 1):
            g_finish(c)

        @pl.when(more)
        def _():
            g_credit()
        w_wait(1, "qo")
        for c in (0, 1):
            g3(c).wait()
        attn_fwd_rev()

        @pl.loop(0, 2)
        def _(c):
            v_wait(c)
            finish(1, c, 0, d1f, vbuf[c])
            e3(0, c).wait()
            part_f(1, c, even)
            to_x(2, c, even)
        attn_grads(rev, finr)

        @pl.when(more)
        def _():
            w_start(1, rev - 2, "qo")
            for c in (0, 1):
                v_start(False, False, pair - 1, c)
            w_wait(0, "qo")
            attn_fwd_plain(pair - 1)
            @pl.loop(0, 2)
            def _(c):
                part_f(0, c, odd)
                to_x(0, c, odd)
        mlp_grads(rev, 1)

        @pl.when(more)
        def _():
            w_wait(1, "iu")
            g_part(1, False, pair - 1, False)

        @pl.when(jnp.logical_not(more))
        def _():
            f_part(1)

        for c in (0, 1):
            g_chip(c)

        @pl.when(jnp.logical_not(more))
        def _():
            for c in (0, 1):
                f_out(c).start()

        @pl.when(more)
        def _():
            pl.semaphore_wait(gcred, 1)
            g_send(*range(2 * npc))
            w_wait(0, "iu")
            mlp_fwd(0)
            for c in (0, 1):
                finish(2, c, 1, d2f, x2r[c])
                state_start(False, False, pair - 1, rows(mine(c)), x2r.at[c], x2_s.at[c])
            @pl.loop(0, 2)
            def _(c):
                e3(1, c).wait()
                part_g(0, 0, c, "hold")

            @pl.when(it < n_pairs - 1)
            def _():
                w_start(0, rev - 3, "qoiu")
            mlp_grads(rev - 1, 0)
            attn_grads(rev - 1, finp)
            mlp_fwd(1)

    outs = []

    def emit(idx, ref, c, out):
        outs.append(local(ref.at[c], out.at[rows(mine(c))], ol_s.at[idx, c]))
        outs.append(remote(ref.at[c], out.at[rows(mine(c))], os_s.at[idx, c], or_s.at[idx, c], core_peer))
        outs[-2].start()
        outs[-1].start()

    for c in (0, 1):
        finish(2, c, None, d2f, x2r[c])
        emit(3, d2f, c, od2)
        emit(2, d1f, c, od1)
        emit(1, x2r, c, ox2)
    for c in (0, 1):
        f_out(c).wait()
    for cp in outs:
        cp.wait()


def move_kernel(depth, chunk, *refs):
    count = (len(refs) - 3) // 2
    buf, in_s, out_s = refs[-3:]
    jobs = []
    for src, dst in zip(refs[:count], refs[count:2 * count]):
        for lo in range(0, src.shape[0], chunk):
            rws = pl.ds(lo, min(chunk, src.shape[0] - lo))
            slot = len(jobs) % depth
            part = buf.at[slot, pl.ds(0, rws.size)]
            jobs.append((
                pltpu.make_async_copy(src.at[rws], part, in_s.at[slot]),
                pltpu.make_async_copy(part, dst.at[rws], out_s.at[slot]),
            ))
    for load, _ in jobs[:depth]:
        load.start()
    lag = depth // 2
    for k in range(len(jobs)):
        jobs[k][0].wait()
        jobs[k][1].start()
        if k >= lag:
            jobs[k - lag][1].wait()
            if k - lag + depth < len(jobs):
                jobs[k - lag + depth][0].start()
    for k in range(max(len(jobs) - lag, 0), len(jobs)):
        jobs[k][1].wait()


def move(arrays, name, depth=12, chunk=576):
    width = arrays[0].shape[-1]
    size = sum(arr.size for arr in arrays)
    depth = min(depth, sum(-(-arr.shape[0] // chunk) for arr in arrays))
    anyspec = pl.BlockSpec(memory_space=pl.ANY)
    return pl.pallas_call(
        functools.partial(move_kernel, depth, chunk),
        out_shape=[jax.ShapeDtypeStruct(arr.shape, arr.dtype) for arr in arrays],
        in_specs=[anyspec] * len(arrays),
        out_specs=[anyspec] * len(arrays),
        scratch_shapes=[pltpu.VMEM((depth, chunk, width), F32), pltpu.SemaphoreType.DMA((depth,)), pltpu.SemaphoreType.DMA((depth,))],
        name=name,
        cost_estimate=pl.CostEstimate(flops=400 * size, bytes_accessed=8 * size, transcendentals=0),
        compiler_params=pltpu.CompilerParams(vmem_limit_bytes=60 * 2 ** 20),
    )(*arrays)


def join_kernel(y_ref, own_ref, peer_ref, out_ref):
    odd = lax.rem(pl.program_id(0) + lax.axis_index("tp"), 2)

    @pl.when(odd == 0)
    def _():
        out_ref[...] = y_ref[...] - own_ref[...]

    @pl.when(odd != 0)
    def _():
        out_ref[...] = y_ref[...] - peer_ref[...]


def join(y_all, own, peer):
    _, n_seq, seq, hid = y_all.shape
    bottom = pl.BlockSpec((None, 1, seq, hid), lambda s: (0, s, 0, 0))
    whole = pl.BlockSpec((1, seq, hid), lambda s: (s, 0, 0))
    half = pl.BlockSpec((1, seq, hid), lambda s: (s // 2, 0, 0))
    return pl.pallas_call(
        join_kernel,
        out_shape=jax.ShapeDtypeStruct(y_all.shape[1:], F32),
        grid=(n_seq,),
        in_specs=[bottom, half, half],
        out_specs=whole,
        name="join",
    )(y_all, own, peer)


def solution(mesh):
    act_spec = P("dp", None, None)
    saved_spec = P(None, "dp", None, None)
    weight_specs = (P(None, None, None, "tp", None), P(None, "tp", None, None), P(None, None, "tp"), P(None, "tp", None))
    grad_specs = (P("dp", None, None, "tp", None), P("dp", "tp", None, None), P("dp", None, "tp"), P("dp", "tp", None))

    def per_device(y_one, y_two, dy_one, dy_two, saved_one, saved_two, w_qkv, w_o, w_in, w_out):
        n_seq, seq, hid = y_one.shape
        n_layers, _, _, heads, hdim = w_qkv.shape
        n_pairs = saved_one.shape[0]
        ff = w_in.shape[-1]
        tok = n_seq * seq
        qkv_w = 3 * heads * hdim
        flat = lambda arr: arr.reshape(arr.shape[:-3] + (tok, hid))
        wq_t = jnp.transpose(w_qkv, (0, 2, 3, 4, 1)).reshape(n_layers, qkv_w, hid)
        wo_t = w_o.reshape(n_layers, heads * hdim, hid)
        sds = jax.ShapeDtypeStruct
        vm = pltpu.VMEM
        dma = pltpu.SemaphoreType.DMA
        half = (2, seq, hid)
        scratch = [
            vm((2, qkv_w, hid), BF), vm((2, heads * hdim, hid), BF), vm((2, hid, ff), BF), vm((2, ff, hid), BF),
            vm((tok, hid), BF), vm((tok, ff), BF), vm((tok, ff), F32), vm((tok, ff), BF),
            vm((tok, hid), BF), vm((tok, hid), BF), vm((qkv_w, tok), BF), vm((qkv_w, tok), BF),
            vm((n_seq * heads, seq, seq), F32), vm((heads * hdim, tok), BF),
            vm((tok, hid), BF), vm((2, tok, hid), BF), vm(half, F32), vm(half, F32),
            vm(half, F32), vm(half, F32), vm(half, F32),
            vm((2,) + half, F32), vm((2,) + half, F32), vm((3,) + half, BF), vm((3,) + half, BF),
            vm((2,) + half, F32), vm(half, F32), vm(half, F32), vm((3, 256, hid), F32),
            dma((2, 2)), dma((2, 2)), dma((3, 2)), dma((3, 2)), dma((3, 2)), dma((3, 2)),
            dma((2,)), dma((2,)), dma((8,)), dma((8,)), dma((2,)), dma((2,)),
            dma((4, 2)), dma((4, 2)), dma((4, 2)), dma((2, 4)), dma((2,)), dma((2,)), dma((2,)), dma((3,)), dma((2, 2)),
            pltpu.SemaphoreType.REGULAR,
        ]
        anyspec = pl.BlockSpec(memory_space=pl.ANY)
        outs = pl.pallas_call(
            functools.partial(chain_kernel, seq, hid, heads, hdim, n_pairs),
            out_shape=[sds(half, F32)] + [sds((tok, hid), F32)] * 3
            + [sds((n_layers, qkv_w, hid), F32), sds((n_layers, heads * hdim, hid), F32), sds((n_layers, hid, ff), F32), sds((n_layers, ff, hid), F32)],
            in_specs=[anyspec] * 10,
            out_specs=[anyspec] * 8,
            scratch_shapes=scratch,
            name="chain",
            compiler_params=pltpu.CompilerParams(collective_id=0, has_side_effects=True, vmem_limit_bytes=67043328),
        )(flat(y_one), flat(y_two), flat(dy_one), flat(dy_two), flat(saved_one), flat(saved_two), wq_t, wo_t, w_in, w_out)
        f_own = outs[0]
        f_other = lax.ppermute(f_own, "tp", [(0, 2), (2, 0), (1, 3), (3, 1)])
        grads = move([out.reshape(-1, hid) for out in outs[4:]], "move_grads")
        f_other, grads = lax.optimization_barrier((f_other, grads))
        f_sum = f_own + f_other
        f_peer = lax.ppermute(f_sum, "tp", [(0, 1), (1, 0), (2, 3), (3, 2)])
        states = [out.reshape(n_seq, seq, hid) for out in move(outs[1:4], "move_states")]
        x_one = join(saved_one, f_sum, f_peer)
        d_qkv = jnp.transpose(grads[0].reshape(n_layers, 3, heads, hdim, hid), (0, 4, 1, 2, 3))
        d_o = grads[1].reshape(n_layers, heads, hdim, hid)
        return (x_one, *states, d_qkv, d_o, grads[2].reshape(n_layers, hid, ff), grads[3].reshape(n_layers, ff, hid))

    return jax.shard_map(
        per_device,
        mesh=mesh,
        in_specs=(act_spec,) * 4 + (saved_spec,) * 2 + weight_specs,
        out_specs=(act_spec,) * 4 + grad_specs,
        check_vma=False,
    )
```

```python
import functools

import jax
import jax.numpy as jnp
from jax import lax
from jax.experimental import pallas as pl
from jax.experimental.pallas import tpu as pltpu
from jax.sharding import PartitionSpec as P

EPS = 1e-6
BF = jnp.bfloat16
F32 = jnp.float32
MESH = pl.DeviceIdType.MESH
GELU_C = 0.7978845608028654
GELU_A = 0.044715

NN = (((1,), (0,)), ((), ()))
NT = (((1,), (1,)), ((), ()))
TN = (((0,), (0,)), ((), ()))


def dot(lhs, rhs, dims):
    return lax.dot_general(lhs, rhs, dims, preferred_element_type=F32)


def rms_scale(state):
    return lax.rsqrt(jnp.mean(state * state, axis=-1, keepdims=True) + EPS)


def rms_pull(state, grad):
    scale = rms_scale(state)
    normed = state * scale
    return scale * (grad - normed * jnp.mean(normed * grad, axis=-1, keepdims=True))


def gelu_parts(hidden, want_grad):
    sq = hidden * hidden
    tanh = jnp.tanh(GELU_C * (hidden + GELU_A * (sq * hidden)))
    half = 0.5 * (1.0 + tanh)
    value = hidden * half
    if not want_grad:
        return value, None
    grad = half + 0.5 * hidden * (1.0 - tanh * tanh) * (GELU_C * (1.0 + 3.0 * GELU_A * sq))
    return value, grad


def chain_kernel(
    seq, hid, heads, hdim, n_pairs,
    y1, y2, dy1, dy2, s1, s2, wq_h, wo_h, wi_h, wu_h,
    f_own, j_own, fsum, jsum, ox2, od1, od2, gq, go, gi, gu,
    wq, wo, wi, wu, a_g, act, gp, dhb, finp, finr, qkvt, dqkvt, pt, ot,
    d1b, d2b, d1f, d2f, vbuf, x2r, xl, pbuf, e1r, xs, xr, gbuf, g1r, g2r, stage,
    e1s_s, e1r_s, e2s_s, e2r_s, e3s_s, e3r_s, g1s_s, g1r_s, g2s_s, g2r_s, g3s_s, g3r_s,
    os_s, or_s, ol_s, oo_s, w_s, xl_s, v_s, x2_s, st_s, d_s, gcred,
):
    me = lax.axis_index("tp")
    dp = lax.axis_index("dp")
    ci = lax.rem(me, 2)
    core_peer = (dp, me + 1 - 2 * ci)
    x_peer = (dp, lax.rem(me + 2, 4))
    qw = heads * hdim
    npc = 4
    prow = seq // npc

    barrier = pltpu.get_barrier_semaphore()
    pl.semaphore_signal(barrier, inc=1, device_id=core_peer, device_id_type=MESH)
    pl.semaphore_signal(barrier, inc=1, device_id=x_peer, device_id_type=MESH)
    pl.semaphore_wait(barrier, 2)

    def rows(seq_idx):
        return pl.ds(pl.multiple_of(seq_idx * seq, seq), seq)

    def mine(c):
        return 2 * c + ci

    def theirs(c):
        return 2 * c + 1 - ci

    def local(src, dst, sem):
        return pltpu.make_async_copy(src, dst, sem)

    def remote(src, dst, ssem, rsem, dev):
        return pltpu.make_async_remote_copy(src_ref=src, dst_ref=dst, send_sem=ssem, recv_sem=rsem, device_id=dev, device_id_type=MESH)

    def weight_copies(slot, blk, which):
        pairs = {"q": (wq_h, wq), "o": (wo_h, wo), "i": (wi_h, wi), "u": (wu_h, wu)}
        return [local(pairs[k][0].at[blk], pairs[k][1].at[slot], w_s.at[slot, "qoiu".index(k)]) for k in which]

    def w_start(slot, blk, which):
        for cp in weight_copies(slot, blk, which):
            cp.start()

    def w_wait(slot, which):
        for cp in weight_copies(slot, 0, which):
            cp.wait()

    def state_start(first, one, pair, rws, dst, sem):
        top, saved = (y1, s1) if one else (y2, s2)
        if first is True:
            local(top.at[rws], dst, sem).start()
        elif first is False:
            local(saved.at[pair, rws], dst, sem).start()
        else:
            @pl.when(first)
            def _():
                local(top.at[rws], dst, sem).start()

            @pl.when(jnp.logical_not(first))
            def _():
                local(saved.at[jnp.minimum(pair, n_pairs - 1), rws], dst, sem).start()

    def state_wait(dst, sem):
        local(y1.at[rows(0)], dst, sem).wait()

    def each_seq(first, one, pair, body, order=lambda i: i):
        for i in (0, 1):
            state_start(first, one, pair, rows(order(i)), xl.at[i], xl_s.at[i])

        @pl.loop(0, 4)
        def _(i):
            slot = lax.rem(i, 2)
            state_wait(xl.at[slot], xl_s.at[slot])
            body(i, order(i), xl[slot])

            @pl.when(i < 2)
            def _():
                state_start(first, one, pair, rows(order(i + 2)), xl.at[slot], xl_s.at[slot])

    def mlp_fwd(slot):
        @pl.loop(0, 4)
        def _(s):
            value, grad = gelu_parts(dot(a_g[rows(s), :], wi[slot], NN), True)
            act[rows(s), :] = value.astype(BF)
            gp[rows(s), :] = grad

    def attn_fwd_seq(slot, fin, s):
        cols = rows(s)
        qkv = dot(wq[slot], fin[cols, :], NT).astype(BF)
        qkvt[:, cols] = qkv
        part = lambda j, h: qkv[j * qw + h * hdim:j * qw + (h + 1) * hdim]
        scores = [dot(part(1, h), part(0, h), TN) * (hdim ** -0.5) for h in range(heads)]
        exps = [jnp.exp(sc - jnp.max(sc, axis=0, keepdims=True)) for sc in scores]
        probs = [ex * (1.0 / jnp.sum(ex, axis=0, keepdims=True)) for ex in exps]
        for h in range(heads):
            pt[s * heads + h] = probs[h]
        for h in range(heads):
            ot[h * hdim:(h + 1) * hdim, cols] = dot(part(2, h), probs[h].astype(BF), NN).astype(BF)

    def attn_fwd_plain(pair):
        def body(i, s, state):
            finp[rows(s), :] = (state * rms_scale(state)).astype(BF)
            attn_fwd_seq(0, finp, s)
        each_seq(False, False, pair, body)

    def attn_fwd_rev():
        @pl.loop(0, 4)
        def _(s):
            attn_fwd_seq(1, finr, s)

    results = ((xs.at[2], jsum), (gbuf.at[:, 1], fsum), (x2r, ox2), (d1f, od1), (d2f, od2))

    def emit_copies(idx, c):
        ref, out = results[idx]
        rws = out.at[rows(mine(c))]
        return (
            local(ref.at[c], rws, ol_s.at[idx, c]),
            remote(ref.at[c], rws, os_s.at[idx, c], or_s.at[idx, c], core_peer),
        )

    def own_copy(idx, c):
        return local(results[idx][0].at[c], (j_own, f_own)[idx].at[c], oo_s.at[idx, c])

    def emit(idx, c):
        for cp in emit_copies(idx, c):
            cp.start()

    def emit_own(idx, c):
        own_copy(idx, c).start()

    def e1(slot, c):
        return remote(pbuf.at[c, 0], e1r.at[slot, c], e1s_s.at[slot, c], e1r_s.at[slot, c], core_peer)

    def e2(t, c):
        return remote(xs.at[t, c], xr.at[t, c], e2s_s.at[t, c], e2r_s.at[t, c], x_peer)

    def part_g(slot, ver, c, mode, e1_slot=None):
        for i, s in enumerate((theirs(c), mine(c))):
            d_act = dot(d2b[ver, rows(s), :], wu[slot], NT)
            dh = (d_act * gp[rows(s), :]).astype(BF)
            dhb[rows(s), :] = dh
            part = dot(dh, wi[slot], NT)
            pbuf[c, i] = pbuf[c, i] + part if mode == "add" else part
            if mode != "hold" and i == 0:
                e1(e1_slot, c).start()

    def part_f(slot, c, e1_slot):
        each = range(heads)
        for i, s in enumerate((theirs(c), mine(c))):
            cols = rows(s)
            do_t = dot(wo[slot], d1b[cols, :], NT).astype(BF)
            do = [do_t[h * hdim:(h + 1) * hdim] for h in each]
            part = lambda j, h: qkvt[j * qw + h * hdim:j * qw + (h + 1) * hdim, cols]
            probs = [pt[s * heads + h] for h in each]
            dps = [dot(part(2, h), do[h], TN) for h in each]
            dv = [dot(do[h], probs[h].astype(BF), NT).astype(BF) for h in each]
            ds = []
            for h in each:
                inner = jnp.sum(probs[h] * dps[h], axis=0, keepdims=True)
                ds.append((probs[h] * (dps[h] - inner) * (hdim ** -0.5)).astype(BF))
            dq = [dot(part(1, h), ds[h], NN).astype(BF) for h in each]
            dk = [dot(part(0, h), ds[h], NT).astype(BF) for h in each]
            d_qkv = jnp.concatenate(dq + dk + dv, axis=0)
            dqkvt[:, cols] = d_qkv
            pbuf[c, i] = dot(d_qkv, wq[slot], TN)
            if i == 0:
                e1(e1_slot, c).start()

    def to_x(t, c, e1_slot, last=None):
        e1(e1_slot, c).wait()
        xs[t, c] = (pbuf[c, 1] + e1r[e1_slot, c]).astype(BF)
        if last is None:
            e2(t, c).start()
        else:
            @pl.when(jnp.logical_not(last))
            def _():
                e2(t, c).start()

            @pl.when(last)
            def _():
                emit_own(0, c)
                emit(0, c)

    def summed(t, c):
        e2(t, c).wait()
        return xs[t, c].astype(F32) + xr[t, c].astype(F32)

    def e3(kind, c):
        ref = d1b.at[rows(mine(c))] if kind == 0 else d2b.at[kind - 1, rows(mine(c))]
        return remote(ref, ref, e3s_s.at[kind, c], e3r_s.at[kind, c], core_peer)

    def finish(t, c, kind, acc, state):
        total = acc[c] + rms_pull(state, summed(t, c))
        acc[c] = total
        if kind is not None:
            if kind == 0:
                d1b[rows(mine(c)), :] = total.astype(BF)
            else:
                d2b[kind - 1, rows(mine(c)), :] = total.astype(BF)
            e3(kind, c).start()

    def g1(c):
        return remote(gbuf.at[c, 0], g1r.at[c], g1s_s.at[c], g1r_s.at[c], core_peer)

    def g2(k):
        c, q = k // npc, k % npc
        rws = pl.ds(q * prow, prow)
        return remote(gbuf.at[c, 1, rws], g2r.at[c, rws], g2s_s.at[k], g2r_s.at[k], x_peer)

    def g_order(i):
        return 2 * (i // 2) + jnp.where(lax.rem(i, 2) == 0, 1 - ci, ci)

    def g_send_core(i):
        for c in (0, 1):
            @pl.when(i == 2 * c)
            def _():
                g1(c).start()

    def g_part(slot, first, pair, keep):
        def body(i, s, state):
            normed = (state * rms_scale(state)).astype(BF)
            a_g[rows(s), :] = normed
            value, grad = gelu_parts(dot(normed, wi[slot], NN), keep)
            value = value.astype(BF)
            if keep:
                act[rows(s), :] = value
                gp[rows(s), :] = grad
            gbuf[i // 2, lax.rem(i, 2)] = dot(value, wu[slot], NN)
            g_send_core(i)
        each_seq(first, True, pair, body, g_order)

    def f_part(slot):
        @pl.loop(0, 4)
        def _(i):
            gbuf[i // 2, lax.rem(i, 2)] = dot(ot[:, rows(g_order(i))], wo[slot], TN)
            g_send_core(i)

    def g_chip(c):
        g1(c).wait()
        gbuf[c, 1] = gbuf[c, 1] + g1r[c]

    def g_send(*ks):
        for k in ks:
            g2(k).start()

    def g_total(c):
        for q in range(npc):
            g2(c * npc + q).wait()
        return gbuf[c, 1] + g2r[c]

    def g3(c):
        ref = finr.at[rows(mine(c))]
        return remote(ref, ref, g3s_s.at[c], g3r_s.at[c], core_peer)

    def g_finish(c):
        state_wait(x2r.at[c], x2_s.at[c])
        state = x2r[c] - g_total(c)
        x2r[c] = state
        finr[rows(mine(c)), :] = (state * rms_scale(state)).astype(BF)
        g3(c).start()

    def g_credit():
        pl.semaphore_signal(gcred, inc=1, device_id=x_peer, device_id_type=MESH)

    def put(pending, tile, dst, value):
        slot = tile % 3
        height = value.shape[0]
        if pending[slot] is not None:
            pending[slot].wait()
        stage[slot, :height] = value
        cp = local(stage.at[slot, pl.ds(0, height)], dst, st_s.at[slot])
        cp.start()
        pending[slot] = cp

    def flush(pending):
        for cp in pending:
            if cp is not None:
                cp.wait()

    def mlp_grads(blk, ver):
        pending = [None] * 3
        n_t = hid // 256
        for k in range(n_t):
            put(pending, k, gu.at[blk, pl.ds(256 * k, 256)], dot(act[:, 256 * k:256 * (k + 1)], d2b[ver], TN))
        for k in range(n_t):
            put(pending, k, gi.at[blk, pl.ds(256 * k, 256)], dot(a_g[:, 256 * k:256 * (k + 1)], dhb[...], TN))
        flush(pending)

    def attn_grads(blk, fin):
        pending = [None] * 3
        for k in range(3):
            put(pending, k, gq.at[blk, pl.ds(qw * k, qw)], dot(dqkvt[qw * k:qw * (k + 1), :], fin[...], NN))
        put(pending, 3, go.at[blk], dot(ot[...], d1b[...], NN))
        flush(pending)

    def v_start(first, one, pair, c):
        state_start(first, one, pair, rows(mine(c)), vbuf.at[c], v_s.at[c])

    def v_wait(c):
        state_wait(vbuf.at[c], v_s.at[c])

    top = 2 * n_pairs
    w_start(1, top, "iuqo")
    for c in (0, 1):
        v_start(True, True, 0, c)
        state_start(True, False, 0, rows(mine(c)), x2r.at[c], x2_s.at[c])
        local(dy1.at[rows(mine(c))], d1f.at[c], d_s.at[0, c]).start()
        local(dy2.at[rows(mine(c))], d2f.at[c], d_s.at[1, c]).start()
    w_wait(1, "iu")
    g_part(1, True, 0, True)
    for c in (0, 1):
        g_chip(c)
        g_send(*range(npc * c, npc * (c + 1)))
    w_start(0, top - 1, "qoiu")
    for i in range(4):
        local(dy2.at[rows(i)], xl.at[i % 2], xl_s.at[i % 2]).start()
        state_wait(xl.at[i % 2], xl_s.at[i % 2])
        d2b[1, rows(i), :] = xl[i % 2].astype(BF)
    for c in (0, 1):
        local(dy1.at[rows(mine(c))], d1f.at[c], d_s.at[0, c]).wait()
        local(dy2.at[rows(mine(c))], d2f.at[c], d_s.at[1, c]).wait()

    @pl.loop(0, n_pairs + 1)
    def _(it):
        pair = n_pairs - it
        is_top = it == 0
        more = it < n_pairs
        rev = 2 * pair
        even, odd = lax.rem(it, 2), lax.rem(it + 1, 2)

        @pl.when(is_top)
        def _():
            @pl.loop(0, 2)
            def _(c):
                part_g(1, 1, c, "first", odd)
                to_x(1, c, odd)

        @pl.when(it > 0)
        def _():
            @pl.loop(0, 2)
            def _(c):
                v_wait(c)
                finish(0, c, 2, d2f, vbuf[c])
                v_start(False, True, pair, c)
                e3(2, c).wait()
                part_g(1, 1, c, "add", odd)
                to_x(1, c, odd)

        @pl.when(more)
        def _():
            w_start(1, rev - 2, "iu")

        for c in (0, 1):
            g_finish(c)

        @pl.when(more)
        def _():
            g_credit()

        @pl.when(jnp.logical_not(more))
        def _():
            for c in (0, 1):
                emit(2, c)
                emit(4, c)
        w_wait(1, "qo")
        for c in (0, 1):
            g3(c).wait()
        attn_fwd_rev()

        @pl.loop(0, 2)
        def _(c):
            v_wait(c)
            finish(1, c, 0, d1f, vbuf[c])

            @pl.when(jnp.logical_not(more))
            def _():
                emit(3, c)
            e3(0, c).wait()
            part_f(1, c, even)
            to_x(2, c, even, jnp.logical_not(more))
        attn_grads(rev, finr)

        @pl.when(more)
        def _():
            w_start(1, rev - 2, "qo")
            for c in (0, 1):
                v_start(False, False, pair - 1, c)
            w_wait(0, "qo")
            attn_fwd_plain(pair - 1)
            @pl.loop(0, 2)
            def _(c):
                part_f(0, c, odd)
                to_x(0, c, odd)
        @pl.when(jnp.logical_not(more))
        def _():
            f_part(1)
            for c in (0, 1):
                g_chip(c)
                emit_own(1, c)
                emit(1, c)
        mlp_grads(rev, 1)

        @pl.when(more)
        def _():
            w_wait(1, "iu")
            g_part(1, False, pair - 1, False)
            for c in (0, 1):
                g_chip(c)
            pl.semaphore_wait(gcred, 1)
            g_send(*range(2 * npc))
            w_wait(0, "iu")
            mlp_fwd(0)
            for c in (0, 1):
                finish(2, c, 1, d2f, x2r[c])
                state_start(False, False, pair - 1, rows(mine(c)), x2r.at[c], x2_s.at[c])
            @pl.loop(0, 2)
            def _(c):
                e3(1, c).wait()
                part_g(0, 0, c, "hold")

            @pl.when(it < n_pairs - 1)
            def _():
                w_start(0, rev - 3, "qoiu")
            mlp_grads(rev - 1, 0)
            attn_grads(rev - 1, finp)
            mlp_fwd(1)

    for c in (0, 1):
        for idx in (0, 1):
            own_copy(idx, c).wait()
        for idx in range(5):
            for cp in emit_copies(idx, c):
                cp.wait()


def move_kernel(depth, chunk, *refs):
    count = (len(refs) - 3) // 2
    buf, in_s, out_s = refs[-3:]
    jobs = []
    for src, dst in zip(refs[:count], refs[count:2 * count]):
        for lo in range(0, src.shape[0], chunk):
            rws = pl.ds(lo, min(chunk, src.shape[0] - lo))
            slot = len(jobs) % depth
            part = buf.at[slot, pl.ds(0, rws.size)]
            jobs.append((
                pltpu.make_async_copy(src.at[rws], part, in_s.at[slot]),
                pltpu.make_async_copy(part, dst.at[rws], out_s.at[slot]),
            ))
    for load, _ in jobs[:depth]:
        load.start()
    lag = depth // 2
    for k in range(len(jobs)):
        jobs[k][0].wait()
        jobs[k][1].start()
        if k >= lag:
            jobs[k - lag][1].wait()
            if k - lag + depth < len(jobs):
                jobs[k - lag + depth][0].start()
    for k in range(max(len(jobs) - lag, 0), len(jobs)):
        jobs[k][1].wait()


def move(arrays, name, depth=12, chunk=576):
    width = arrays[0].shape[-1]
    size = sum(arr.size for arr in arrays)
    depth = min(depth, sum(-(-arr.shape[0] // chunk) for arr in arrays))
    anyspec = pl.BlockSpec(memory_space=pl.ANY)
    return pl.pallas_call(
        functools.partial(move_kernel, depth, chunk),
        out_shape=[jax.ShapeDtypeStruct(arr.shape, arr.dtype) for arr in arrays],
        in_specs=[anyspec] * len(arrays),
        out_specs=[anyspec] * len(arrays),
        scratch_shapes=[pltpu.VMEM((depth, chunk, width), F32), pltpu.SemaphoreType.DMA((depth,)), pltpu.SemaphoreType.DMA((depth,))],
        name=name,
        cost_estimate=pl.CostEstimate(flops=400 * size, bytes_accessed=8 * size, transcendentals=0),
        compiler_params=pltpu.CompilerParams(vmem_limit_bytes=60 * 2 ** 20),
    )(*arrays)


def take_kernel(finish, *refs):
    *base, near_ref, far_ref, out_ref = refs
    odd = lax.rem(pl.program_id(0) + lax.axis_index("tp"), 2)

    @pl.when(odd == 0)
    def _():
        out_ref[...] = finish(near_ref[...].astype(F32), *[ref[...] for ref in base])

    @pl.when(odd != 0)
    def _():
        out_ref[...] = finish(far_ref[...].astype(F32), *[ref[...] for ref in base])


def take(finish, name, shape, base, near, far, parts=2):
    n_seq, seq, hid = shape
    part = seq // parts
    whole = pl.BlockSpec((1, part, hid), lambda s, r: (s, r, 0))
    bottom = pl.BlockSpec((None, 1, part, hid), lambda s, r: (0, s, r, 0))
    half = pl.BlockSpec((1, part, hid), lambda s, r: (s // 2, r, 0))
    return pl.pallas_call(
        functools.partial(take_kernel, finish),
        out_shape=jax.ShapeDtypeStruct(shape, F32),
        grid=(n_seq, parts),
        in_specs=[whole if arr.ndim == 3 else bottom for arr in base] + [half, half],
        out_specs=whole,
        name=name,
        cost_estimate=pl.CostEstimate(flops=40_000_000, bytes_accessed=16_000_000, transcendentals=0),
    )(*base, near, far)


def finish_x(other, state, own):
    return state - (own + other)


def finish_d(other, grad, state, own):
    return grad + rms_pull(state, own.astype(F32) + other)


def solution(mesh):
    act_spec = P("dp", None, None)
    saved_spec = P(None, "dp", None, None)
    weight_specs = (P(None, None, None, "tp", None), P(None, "tp", None, None), P(None, None, "tp"), P(None, "tp", None))
    grad_specs = (P("dp", None, None, "tp", None), P("dp", "tp", None, None), P("dp", None, "tp"), P("dp", "tp", None))

    def per_device(y_one, y_two, dy_one, dy_two, saved_one, saved_two, w_qkv, w_o, w_in, w_out):
        n_seq, seq, hid = y_one.shape
        n_layers, _, _, heads, hdim = w_qkv.shape
        n_pairs = saved_one.shape[0]
        ff = w_in.shape[-1]
        tok = n_seq * seq
        qkv_w = 3 * heads * hdim
        flat = lambda arr: arr.reshape(arr.shape[:-3] + (tok, hid))
        wq_t = jnp.transpose(w_qkv, (0, 2, 3, 4, 1)).reshape(n_layers, qkv_w, hid)
        wo_t = w_o.reshape(n_layers, heads * hdim, hid)
        sds = jax.ShapeDtypeStruct
        vm = pltpu.VMEM
        dma = pltpu.SemaphoreType.DMA
        half = (2, seq, hid)
        scratch = [
            vm((2, qkv_w, hid), BF), vm((2, heads * hdim, hid), BF), vm((2, hid, ff), BF), vm((2, ff, hid), BF),
            vm((tok, hid), BF), vm((tok, ff), BF), vm((tok, ff), F32), vm((tok, ff), BF),
            vm((tok, hid), BF), vm((tok, hid), BF), vm((qkv_w, tok), BF), vm((qkv_w, tok), BF),
            vm((n_seq * heads, seq, seq), F32), vm((heads * hdim, tok), BF),
            vm((tok, hid), BF), vm((2, tok, hid), BF), vm(half, F32), vm(half, F32),
            vm(half, F32), vm(half, F32), vm(half, F32),
            vm((2,) + half, F32), vm((2,) + half, F32), vm((3,) + half, BF), vm((3,) + half, BF),
            vm((2,) + half, F32), vm(half, F32), vm(half, F32), vm((3, 256, hid), F32),
            dma((2, 2)), dma((2, 2)), dma((3, 2)), dma((3, 2)), dma((3, 2)), dma((3, 2)),
            dma((2,)), dma((2,)), dma((8,)), dma((8,)), dma((2,)), dma((2,)),
            dma((5, 2)), dma((5, 2)), dma((5, 2)), dma((2, 2)), dma((2, 4)), dma((2,)), dma((2,)), dma((2,)), dma((3,)), dma((2, 2)),
            pltpu.SemaphoreType.REGULAR,
        ]
        anyspec = pl.BlockSpec(memory_space=pl.ANY)
        outs = pl.pallas_call(
            functools.partial(chain_kernel, seq, hid, heads, hdim, n_pairs),
            out_shape=[sds(half, F32), sds(half, BF), sds((tok, hid), F32), sds((tok, hid), BF)] + [sds((tok, hid), F32)] * 3
            + [sds((n_layers, qkv_w, hid), F32), sds((n_layers, heads * hdim, hid), F32), sds((n_layers, hid, ff), F32), sds((n_layers, ff, hid), F32)],
            in_specs=[anyspec] * 10,
            out_specs=[anyspec] * 11,
            scratch_shapes=scratch,
            name="chain",
            compiler_params=pltpu.CompilerParams(collective_id=0, has_side_effects=True, vmem_limit_bytes=67043328),
        )(flat(y_one), flat(y_two), flat(dy_one), flat(dy_two), flat(saved_one), flat(saved_two), wq_t, wo_t, w_in, w_out)
        f_own, j_own, f_all, j_all, x_two, d_one, d_two = outs[:7]
        cube = lambda arr: arr.reshape(n_seq, seq, hid)
        over_x = lambda arr: lax.ppermute(arr, "tp", [(0, 2), (2, 0), (1, 3), (3, 1)])
        over_core = lambda arr: lax.ppermute(arr, "tp", [(0, 1), (1, 0), (2, 3), (3, 2)])
        f_near, j_near = over_x(f_own), over_x(j_own)
        grads = move([out.reshape(-1, hid) for out in outs[7:]], "move_grads")
        f_near, j_near, grads = lax.optimization_barrier((f_near, j_near, grads))
        f_far, j_far = over_core(f_near), over_core(j_near)
        states = [cube(out) for out in move([x_two, d_one], "move_states")]
        x_one = take(finish_x, "finish_x", (n_seq, seq, hid), [saved_one, cube(f_all)], f_near, f_far)
        dx_two = take(finish_d, "finish_d", (n_seq, seq, hid), [cube(d_two), cube(x_two), cube(j_all)], j_near, j_far)
        d_qkv = jnp.transpose(grads[0].reshape(n_layers, 3, heads, hdim, hid), (0, 4, 1, 2, 3))
        d_o = grads[1].reshape(n_layers, heads, hdim, hid)
        return (x_one, *states, dx_two, d_qkv, d_o, grads[2].reshape(n_layers, hid, ff), grads[3].reshape(n_layers, ff, hid))

    return jax.shard_map(
        per_device,
        mesh=mesh,
        in_specs=(act_spec,) * 4 + (saved_spec,) * 2 + weight_specs,
        out_specs=(act_spec,) * 4 + grad_specs,
        check_vma=False,
    )
```

```python
import functools

import jax
import jax.numpy as jnp
from jax import lax
from jax.experimental import pallas as pl
from jax.experimental.pallas import tpu as pltpu
from jax.sharding import PartitionSpec as P

EPS = 1e-6
BF = jnp.bfloat16
F32 = jnp.float32
MESH = pl.DeviceIdType.MESH
GELU_C = 0.7978845608028654
GELU_A = 0.044715

NN = (((1,), (0,)), ((), ()))
NT = (((1,), (1,)), ((), ()))
TN = (((0,), (0,)), ((), ()))


def dot(lhs, rhs, dims):
    return lax.dot_general(lhs, rhs, dims, preferred_element_type=F32)


def rms_scale(state):
    return lax.rsqrt(jnp.mean(state * state, axis=-1, keepdims=True) + EPS)


def rms_pull(state, grad):
    scale = rms_scale(state)
    normed = state * scale
    return scale * (grad - normed * jnp.mean(normed * grad, axis=-1, keepdims=True))


def gelu_parts(hidden, want_grad):
    sq = hidden * hidden
    tanh = jnp.tanh(GELU_C * (hidden + GELU_A * (sq * hidden)))
    half = 0.5 * (1.0 + tanh)
    value = hidden * half
    if not want_grad:
        return value, None
    grad = half + 0.5 * hidden * (1.0 - tanh * tanh) * (GELU_C * (1.0 + 3.0 * GELU_A * sq))
    return value, grad


def chain_kernel(
    seq, hid, heads, hdim, n_pairs,
    y1, y2, dy1, dy2, s1, s2, wq_h, wo_h, wi_h, wu_h,
    f_own, j_own, fsum, jsum, ox2, od1, od2, gq, go, gi, gu,
    wq, wo, wi, wu, a_g, act, gp, dhb, finp, finr, qkvt, dqkvt, pt, ot,
    d1b, d2b, d1f, d2f, vbuf, x2r, xl, pbuf, e1r, xs, xr, gbuf, g1r, g2r, stage,
    e1s_s, e1r_s, e2s_s, e2r_s, e3s_s, e3r_s, g1s_s, g1r_s, g2s_s, g2r_s, g3s_s, g3r_s,
    os_s, or_s, ol_s, oo_s, w_s, xl_s, v_s, x2_s, st_s, d_s, gcred,
):
    me = lax.axis_index("tp")
    dp = lax.axis_index("dp")
    ci = lax.rem(me, 2)
    core_peer = (dp, me + 1 - 2 * ci)
    x_peer = (dp, lax.rem(me + 2, 4))
    qw = heads * hdim
    npc = 4
    prow = seq // npc

    barrier = pltpu.get_barrier_semaphore()
    pl.semaphore_signal(barrier, inc=1, device_id=core_peer, device_id_type=MESH)
    pl.semaphore_signal(barrier, inc=1, device_id=x_peer, device_id_type=MESH)

    def rows(seq_idx):
        return pl.ds(pl.multiple_of(seq_idx * seq, seq), seq)

    def mine(c):
        return 2 * c + ci

    def theirs(c):
        return 2 * c + 1 - ci

    def local(src, dst, sem):
        return pltpu.make_async_copy(src, dst, sem)

    def remote(src, dst, ssem, rsem, dev):
        return pltpu.make_async_remote_copy(src_ref=src, dst_ref=dst, send_sem=ssem, recv_sem=rsem, device_id=dev, device_id_type=MESH)

    def weight_copies(slot, blk, which):
        pairs = {"q": (wq_h, wq), "o": (wo_h, wo), "i": (wi_h, wi), "u": (wu_h, wu)}
        return [local(pairs[k][0].at[blk], pairs[k][1].at[slot], w_s.at[slot, "qoiu".index(k)]) for k in which]

    def w_start(slot, blk, which):
        for cp in weight_copies(slot, blk, which):
            cp.start()

    def w_wait(slot, which):
        for cp in weight_copies(slot, 0, which):
            cp.wait()

    def state_start(first, one, pair, rws, dst, sem):
        top, saved = (y1, s1) if one else (y2, s2)
        if first is True:
            local(top.at[rws], dst, sem).start()
        elif first is False:
            local(saved.at[pair, rws], dst, sem).start()
        else:
            @pl.when(first)
            def _():
                local(top.at[rws], dst, sem).start()

            @pl.when(jnp.logical_not(first))
            def _():
                local(saved.at[jnp.minimum(pair, n_pairs - 1), rws], dst, sem).start()

    def state_wait(dst, sem):
        local(y1.at[rows(0)], dst, sem).wait()

    def each_seq(first, one, pair, body, order=lambda i: i):
        for i in (0, 1):
            state_start(first, one, pair, rows(order(i)), xl.at[i], xl_s.at[i])

        @pl.loop(0, 4)
        def _(i):
            slot = lax.rem(i, 2)
            state_wait(xl.at[slot], xl_s.at[slot])
            body(i, order(i), xl[slot])

            @pl.when(i < 2)
            def _():
                state_start(first, one, pair, rows(order(i + 2)), xl.at[slot], xl_s.at[slot])

    def mlp_fwd(slot):
        @pl.loop(0, 4)
        def _(s):
            value, grad = gelu_parts(dot(a_g[rows(s), :], wi[slot], NN), True)
            act[rows(s), :] = value.astype(BF)
            gp[rows(s), :] = grad

    def attn_fwd_seq(slot, fin, s):
        cols = rows(s)
        qkv = dot(wq[slot], fin[cols, :], NT).astype(BF)
        qkvt[:, cols] = qkv
        part = lambda j, h: qkv[j * qw + h * hdim:j * qw + (h + 1) * hdim]
        scores = [dot(part(1, h), part(0, h), TN) * (hdim ** -0.5) for h in range(heads)]
        exps = [jnp.exp(sc - jnp.max(sc, axis=0, keepdims=True)) for sc in scores]
        probs = [ex * (1.0 / jnp.sum(ex, axis=0, keepdims=True)) for ex in exps]
        for h in range(heads):
            pt[s * heads + h] = probs[h]
        for h in range(heads):
            ot[h * hdim:(h + 1) * hdim, cols] = dot(part(2, h), probs[h].astype(BF), NN).astype(BF)

    def attn_fwd_plain(pair):
        def body(i, s, state):
            finp[rows(s), :] = (state * rms_scale(state)).astype(BF)
            attn_fwd_seq(0, finp, s)
        each_seq(False, False, pair, body)

    def attn_fwd_rev():
        @pl.loop(0, 4)
        def _(s):
            attn_fwd_seq(1, finr, s)

    results = ((xs.at[2], jsum), (gbuf.at[:, 1], fsum), (x2r, ox2), (d1f, od1), (d2f, od2))

    def emit_copies(idx, c):
        ref, out = results[idx]
        rws = out.at[rows(mine(c))]
        return (
            local(ref.at[c], rws, ol_s.at[idx, c]),
            remote(ref.at[c], rws, os_s.at[idx, c], or_s.at[idx, c], core_peer),
        )

    def own_copy(c):
        return local(results[0][0].at[c], j_own.at[c], oo_s.at[c]) if c is not None else local(gbuf.at[1, 1], f_own, oo_s.at[2])

    def emit(idx, c):
        for cp in emit_copies(idx, c):
            cp.start()

    def emit_own(c):
        own_copy(c).start()

    def e1(slot, c):
        return remote(pbuf.at[c, 0], e1r.at[slot, c], e1s_s.at[slot, c], e1r_s.at[slot, c], core_peer)

    def e2(t, c):
        return remote(xs.at[t, c], xr.at[t, c], e2s_s.at[t, c], e2r_s.at[t, c], x_peer)

    def part_g(slot, ver, c, mode, e1_slot=None):
        for i, s in enumerate((theirs(c), mine(c))):
            d_act = dot(d2b[ver, rows(s), :], wu[slot], NT)
            dh = (d_act * gp[rows(s), :]).astype(BF)
            dhb[rows(s), :] = dh
            part = dot(dh, wi[slot], NT)
            pbuf[c, i] = pbuf[c, i] + part if mode == "add" else part
            if mode != "hold" and i == 0:
                e1(e1_slot, c).start()

    def part_f(slot, c, e1_slot):
        each = range(heads)
        for i, s in enumerate((theirs(c), mine(c))):
            cols = rows(s)
            do_t = dot(wo[slot], d1b[cols, :], NT).astype(BF)
            do = [do_t[h * hdim:(h + 1) * hdim] for h in each]
            part = lambda j, h: qkvt[j * qw + h * hdim:j * qw + (h + 1) * hdim, cols]
            probs = [pt[s * heads + h] for h in each]
            dps = [dot(part(2, h), do[h], TN) for h in each]
            dv = [dot(do[h], probs[h].astype(BF), NT).astype(BF) for h in each]
            ds = []
            for h in each:
                inner = jnp.sum(probs[h] * dps[h], axis=0, keepdims=True)
                ds.append((probs[h] * (dps[h] - inner) * (hdim ** -0.5)).astype(BF))
            dq = [dot(part(1, h), ds[h], NN).astype(BF) for h in each]
            dk = [dot(part(0, h), ds[h], NT).astype(BF) for h in each]
            d_qkv = jnp.concatenate(dq + dk + dv, axis=0)
            dqkvt[:, cols] = d_qkv
            pbuf[c, i] = dot(d_qkv, wq[slot], TN)
            if i == 0:
                e1(e1_slot, c).start()

    def to_x(t, c, e1_slot, last=None):
        e1(e1_slot, c).wait()
        xs[t, c] = (pbuf[c, 1] + e1r[e1_slot, c]).astype(BF)
        if last is None:
            e2(t, c).start()
        else:
            @pl.when(jnp.logical_not(last))
            def _():
                e2(t, c).start()

            @pl.when(last)
            def _():
                emit_own(c)
                emit(0, c)

    def summed(t, c):
        e2(t, c).wait()
        return xs[t, c].astype(F32) + xr[t, c].astype(F32)

    def e3(kind, c):
        ref = d1b.at[rows(mine(c))] if kind == 0 else d2b.at[kind - 1, rows(mine(c))]
        return remote(ref, ref, e3s_s.at[kind, c], e3r_s.at[kind, c], core_peer)

    def finish(t, c, kind, acc, state):
        total = acc[c] + rms_pull(state, summed(t, c))
        acc[c] = total
        if kind is not None:
            if kind == 0:
                d1b[rows(mine(c)), :] = total.astype(BF)
            else:
                d2b[kind - 1, rows(mine(c)), :] = total.astype(BF)
            e3(kind, c).start()

    def g1(c):
        return remote(gbuf.at[c, 0], g1r.at[c], g1s_s.at[c], g1r_s.at[c], core_peer)

    def g2(k):
        c, q = k // npc, k % npc
        rws = pl.ds(q * prow, prow)
        return remote(gbuf.at[c, 1, rws], g2r.at[c, rws], g2s_s.at[k], g2r_s.at[k], x_peer)

    def g_order(i):
        return 2 * (i // 2) + jnp.where(lax.rem(i, 2) == 0, 1 - ci, ci)

    def g_send_core(i):
        for c in (0, 1):
            @pl.when(i == 2 * c)
            def _():
                g1(c).start()

    def g_part(slot, first, pair, keep):
        def body(i, s, state):
            normed = (state * rms_scale(state)).astype(BF)
            a_g[rows(s), :] = normed
            value, grad = gelu_parts(dot(normed, wi[slot], NN), keep)
            value = value.astype(BF)
            if keep:
                act[rows(s), :] = value
                gp[rows(s), :] = grad
            gbuf[i // 2, lax.rem(i, 2)] = dot(value, wu[slot], NN)
            g_send_core(i)
        each_seq(first, True, pair, body, g_order)

    def f_part(slot):
        @pl.loop(0, 4)
        def _(i):
            gbuf[i // 2, lax.rem(i, 2)] = dot(ot[:, rows(g_order(i))], wo[slot], TN)
            g_send_core(i)

    def g_chip(c):
        g1(c).wait()
        gbuf[c, 1] = gbuf[c, 1] + g1r[c]

    def g_send(*ks):
        for k in ks:
            g2(k).start()

    def g_total(c):
        for q in range(npc):
            g2(c * npc + q).wait()
        return gbuf[c, 1] + g2r[c]

    def g3(c):
        ref = finr.at[rows(mine(c))]
        return remote(ref, ref, g3s_s.at[c], g3r_s.at[c], core_peer)

    def g_finish(c):
        state_wait(x2r.at[c], x2_s.at[c])
        state = x2r[c] - g_total(c)
        x2r[c] = state
        finr[rows(mine(c)), :] = (state * rms_scale(state)).astype(BF)
        g3(c).start()

    def g_credit():
        pl.semaphore_signal(gcred, inc=1, device_id=x_peer, device_id_type=MESH)

    def put(pending, tile, dst, value):
        slot = tile % 3
        height = value.shape[0]
        if pending[slot] is not None:
            pending[slot].wait()
        stage[slot, :height] = value
        cp = local(stage.at[slot, pl.ds(0, height)], dst, st_s.at[slot])
        cp.start()
        pending[slot] = cp

    def flush(pending):
        for cp in pending:
            if cp is not None:
                cp.wait()

    def mlp_grads(blk, ver):
        pending = [None] * 3
        n_t = hid // 256
        for k in range(n_t):
            put(pending, k, gu.at[blk, pl.ds(256 * k, 256)], dot(act[:, 256 * k:256 * (k + 1)], d2b[ver], TN))
        for k in range(n_t):
            put(pending, k, gi.at[blk, pl.ds(256 * k, 256)], dot(a_g[:, 256 * k:256 * (k + 1)], dhb[...], TN))
        flush(pending)

    def attn_grads(blk, fin):
        pending = [None] * 3
        for k in range(3):
            put(pending, k, gq.at[blk, pl.ds(qw * k, qw)], dot(dqkvt[qw * k:qw * (k + 1), :], fin[...], NN))
        put(pending, 3, go.at[blk], dot(ot[...], d1b[...], NN))
        flush(pending)

    def v_start(first, one, pair, c):
        state_start(first, one, pair, rows(mine(c)), vbuf.at[c], v_s.at[c])

    def v_wait(c):
        state_wait(vbuf.at[c], v_s.at[c])

    top = 2 * n_pairs
    w_start(1, top, "iuqo")
    for c in (0, 1):
        v_start(True, True, 0, c)
        state_start(True, False, 0, rows(mine(c)), x2r.at[c], x2_s.at[c])
        local(dy1.at[rows(mine(c))], d1f.at[c], d_s.at[0, c]).start()
        local(dy2.at[rows(mine(c))], d2f.at[c], d_s.at[1, c]).start()
    pl.semaphore_wait(barrier, 2)
    w_wait(1, "iu")
    g_part(1, True, 0, True)
    for c in (0, 1):
        g_chip(c)
        g_send(*range(npc * c, npc * (c + 1)))
    w_start(0, top - 1, "qoiu")
    for i in range(4):
        local(dy2.at[rows(i)], xl.at[i % 2], xl_s.at[i % 2]).start()
        state_wait(xl.at[i % 2], xl_s.at[i % 2])
        d2b[1, rows(i), :] = xl[i % 2].astype(BF)
    for c in (0, 1):
        local(dy1.at[rows(mine(c))], d1f.at[c], d_s.at[0, c]).wait()
        local(dy2.at[rows(mine(c))], d2f.at[c], d_s.at[1, c]).wait()

    @pl.loop(0, n_pairs + 1)
    def _(it):
        pair = n_pairs - it
        is_top = it == 0
        more = it < n_pairs
        rev = 2 * pair
        even, odd = lax.rem(it, 2), lax.rem(it + 1, 2)

        @pl.when(is_top)
        def _():
            @pl.loop(0, 2)
            def _(c):
                part_g(1, 1, c, "first", odd)
                to_x(1, c, odd)

        @pl.when(it > 0)
        def _():
            @pl.loop(0, 2)
            def _(c):
                v_wait(c)
                finish(0, c, 2, d2f, vbuf[c])
                v_start(False, True, pair, c)
                e3(2, c).wait()
                part_g(1, 1, c, "add", odd)
                to_x(1, c, odd)

        @pl.when(more)
        def _():
            w_start(1, rev - 2, "iu")

        for c in (0, 1):
            g_finish(c)

        g_credit()

        @pl.when(jnp.logical_not(more))
        def _():
            for c in (0, 1):
                emit(2, c)
                emit(4, c)
        w_wait(1, "qo")
        for c in (0, 1):
            g3(c).wait()
        attn_fwd_rev()

        @pl.when(jnp.logical_not(more))
        def _():
            f_part(1)
            g_chip(0)
            pl.semaphore_wait(gcred, 1)
            g_send(*range(npc))
            g_chip(1)
            emit_own(None)
            emit(1, 1)

        @pl.loop(0, 2)
        def _(c):
            v_wait(c)
            finish(1, c, 0, d1f, vbuf[c])

            @pl.when(jnp.logical_not(more))
            def _():
                emit(3, c)
            e3(0, c).wait()
            part_f(1, c, even)
            to_x(2, c, even, jnp.logical_not(more))
        attn_grads(rev, finr)

        @pl.when(more)
        def _():
            w_start(1, rev - 2, "qo")
            for c in (0, 1):
                v_start(False, False, pair - 1, c)
            w_wait(0, "qo")
            attn_fwd_plain(pair - 1)
            @pl.loop(0, 2)
            def _(c):
                part_f(0, c, odd)
                to_x(0, c, odd)
        mlp_grads(rev, 1)

        @pl.when(more)
        def _():
            w_wait(1, "iu")
            g_part(1, False, pair - 1, False)
            for c in (0, 1):
                g_chip(c)
            pl.semaphore_wait(gcred, 1)
            g_send(*range(2 * npc))
            w_wait(0, "iu")
            mlp_fwd(0)
            for c in (0, 1):
                finish(2, c, 1, d2f, x2r[c])
                state_start(False, False, pair - 1, rows(mine(c)), x2r.at[c], x2_s.at[c])
            @pl.loop(0, 2)
            def _(c):
                e3(1, c).wait()
                part_g(0, 0, c, "hold")

            @pl.when(it < n_pairs - 1)
            def _():
                w_start(0, rev - 3, "qoiu")
            mlp_grads(rev - 1, 0)
            attn_grads(rev - 1, finp)
            mlp_fwd(1)

    gbuf[0, 1] = g_total(0)
    emit(1, 0)
    for c in (0, 1, None):
        own_copy(c).wait()
    for c in (0, 1):
        for idx in range(5):
            for cp in emit_copies(idx, c):
                cp.wait()


def move_kernel(depth, chunk, *refs):
    count = (len(refs) - 3) // 2
    buf, in_s, out_s = refs[-3:]
    jobs = []
    for src, dst in zip(refs[:count], refs[count:2 * count]):
        for lo in range(0, src.shape[0], chunk):
            rws = pl.ds(lo, min(chunk, src.shape[0] - lo))
            slot = len(jobs) % depth
            part = buf.at[slot, pl.ds(0, rws.size)]
            jobs.append((
                pltpu.make_async_copy(src.at[rws], part, in_s.at[slot]),
                pltpu.make_async_copy(part, dst.at[rws], out_s.at[slot]),
            ))
    for load, _ in jobs[:depth]:
        load.start()
    lag = depth // 2
    for k in range(len(jobs)):
        jobs[k][0].wait()
        jobs[k][1].start()
        if k >= lag:
            jobs[k - lag][1].wait()
            if k - lag + depth < len(jobs):
                jobs[k - lag + depth][0].start()
    for k in range(max(len(jobs) - lag, 0), len(jobs)):
        jobs[k][1].wait()


def move(arrays, name, depth=12, chunk=576):
    width = arrays[0].shape[-1]
    size = sum(arr.size for arr in arrays)
    depth = min(depth, sum(-(-arr.shape[0] // chunk) for arr in arrays))
    anyspec = pl.BlockSpec(memory_space=pl.ANY)
    return pl.pallas_call(
        functools.partial(move_kernel, depth, chunk),
        out_shape=[jax.ShapeDtypeStruct(arr.shape, arr.dtype) for arr in arrays],
        in_specs=[anyspec] * len(arrays),
        out_specs=[anyspec] * len(arrays),
        scratch_shapes=[pltpu.VMEM((depth, chunk, width), F32), pltpu.SemaphoreType.DMA((depth,)), pltpu.SemaphoreType.DMA((depth,))],
        name=name,
        cost_estimate=pl.CostEstimate(flops=400 * size, bytes_accessed=8 * size, transcendentals=0),
        compiler_params=pltpu.CompilerParams(vmem_limit_bytes=60 * 2 ** 20),
    )(*arrays)


def take_kernel(finish, first, *refs):
    *base, near_ref, far_ref, out_ref = refs
    seq_idx = pl.program_id(0)
    odd = lax.rem(seq_idx + lax.axis_index("tp"), 2)
    ready = seq_idx < first

    @pl.when(ready)
    def _():
        out_ref[...] = finish(None, *[ref[...] for ref in base])

    @pl.when(jnp.logical_not(ready) & (odd == 0))
    def _():
        out_ref[...] = finish(near_ref[...].astype(F32), *[ref[...] for ref in base])

    @pl.when(jnp.logical_not(ready) & (odd != 0))
    def _():
        out_ref[...] = finish(far_ref[...].astype(F32), *[ref[...] for ref in base])


def take(finish, first, name, shape, base, near, far):
    n_seq, seq, hid = shape
    whole = pl.BlockSpec((1, seq, hid), lambda s: (s, 0, 0))
    bottom = pl.BlockSpec((None, 1, seq, hid), lambda s: (0, s, 0, 0))
    half = pl.BlockSpec((1, seq, hid), lambda s: (jnp.maximum(s - first, 0) // 2, 0, 0))
    return pl.pallas_call(
        functools.partial(take_kernel, finish, first),
        out_shape=jax.ShapeDtypeStruct(shape, F32),
        grid=(n_seq,),
        in_specs=[whole if arr.ndim == 3 else bottom for arr in base] + [half, half],
        out_specs=whole,
        name=name,
        cost_estimate=pl.CostEstimate(flops=40_000_000, bytes_accessed=16_000_000, transcendentals=0),
    )(*base, near, far)


def finish_x(other, state, own):
    return state - (own if other is None else own + other)


def finish_d(other, grad, state, own):
    own = own.astype(F32)
    return grad + rms_pull(state, own if other is None else own + other)


def solution(mesh):
    act_spec = P("dp", None, None)
    saved_spec = P(None, "dp", None, None)
    weight_specs = (P(None, None, None, "tp", None), P(None, "tp", None, None), P(None, None, "tp"), P(None, "tp", None))
    grad_specs = (P("dp", None, None, "tp", None), P("dp", "tp", None, None), P("dp", None, "tp"), P("dp", "tp", None))

    def per_device(y_one, y_two, dy_one, dy_two, saved_one, saved_two, w_qkv, w_o, w_in, w_out):
        n_seq, seq, hid = y_one.shape
        n_layers, _, _, heads, hdim = w_qkv.shape
        n_pairs = saved_one.shape[0]
        ff = w_in.shape[-1]
        tok = n_seq * seq
        qkv_w = 3 * heads * hdim
        flat = lambda arr: arr.reshape(arr.shape[:-3] + (tok, hid))
        wq_t = jnp.transpose(w_qkv, (0, 2, 3, 4, 1)).reshape(n_layers, qkv_w, hid)
        wo_t = w_o.reshape(n_layers, heads * hdim, hid)
        sds = jax.ShapeDtypeStruct
        vm = pltpu.VMEM
        dma = pltpu.SemaphoreType.DMA
        half = (2, seq, hid)
        scratch = [
            vm((2, qkv_w, hid), BF), vm((2, heads * hdim, hid), BF), vm((2, hid, ff), BF), vm((2, ff, hid), BF),
            vm((tok, hid), BF), vm((tok, ff), BF), vm((tok, ff), F32), vm((tok, ff), BF),
            vm((tok, hid), BF), vm((tok, hid), BF), vm((qkv_w, tok), BF), vm((qkv_w, tok), BF),
            vm((n_seq * heads, seq, seq), F32), vm((heads * hdim, tok), BF),
            vm((tok, hid), BF), vm((2, tok, hid), BF), vm(half, F32), vm(half, F32),
            vm(half, F32), vm(half, F32), vm(half, F32),
            vm((2,) + half, F32), vm((2,) + half, F32), vm((3,) + half, BF), vm((3,) + half, BF),
            vm((2,) + half, F32), vm(half, F32), vm(half, F32), vm((3, 256, hid), F32),
            dma((2, 2)), dma((2, 2)), dma((3, 2)), dma((3, 2)), dma((3, 2)), dma((3, 2)),
            dma((2,)), dma((2,)), dma((8,)), dma((8,)), dma((2,)), dma((2,)),
            dma((5, 2)), dma((5, 2)), dma((5, 2)), dma((3,)), dma((2, 4)), dma((2,)), dma((2,)), dma((2,)), dma((3,)), dma((2, 2)),
            pltpu.SemaphoreType.REGULAR,
        ]
        anyspec = pl.BlockSpec(memory_space=pl.ANY)
        outs = pl.pallas_call(
            functools.partial(chain_kernel, seq, hid, heads, hdim, n_pairs),
            out_shape=[sds(half[1:], F32), sds(half, BF), sds((tok, hid), F32), sds((tok, hid), BF)] + [sds((tok, hid), F32)] * 3
            + [sds((n_layers, qkv_w, hid), F32), sds((n_layers, heads * hdim, hid), F32), sds((n_layers, hid, ff), F32), sds((n_layers, ff, hid), F32)],
            in_specs=[anyspec] * 10,
            out_specs=[anyspec] * 11,
            scratch_shapes=scratch,
            name="chain",
            compiler_params=pltpu.CompilerParams(collective_id=0, has_side_effects=True, vmem_limit_bytes=67043328),
        )(flat(y_one), flat(y_two), flat(dy_one), flat(dy_two), flat(saved_one), flat(saved_two), wq_t, wo_t, w_in, w_out)
        f_own, j_own, f_all, j_all, x_two, d_one, d_two = outs[:7]
        cube = lambda arr: arr.reshape(n_seq, seq, hid)
        over_x = lambda arr: lax.ppermute(arr, "tp", [(0, 2), (2, 0), (1, 3), (3, 1)])
        over_core = lambda arr: lax.ppermute(arr, "tp", [(0, 1), (1, 0), (2, 3), (3, 2)])
        f_near, j_near = over_x(f_own), over_x(j_own)
        grads = move([out.reshape(-1, hid) for out in outs[7:]], "move_grads")
        f_near, j_near, grads = lax.optimization_barrier((f_near, j_near, grads))
        f_far, j_far = over_core(f_near), over_core(j_near)
        states = [cube(out) for out in move([x_two, d_one], "move_states")]
        x_one = take(finish_x, 2, "finish_x", (n_seq, seq, hid), [saved_one, cube(f_all)], f_near[None], f_far[None])
        dx_two = take(finish_d, 0, "finish_d", (n_seq, seq, hid), [cube(d_two), cube(x_two), cube(j_all)], j_near, j_far)
        d_qkv = jnp.transpose(grads[0].reshape(n_layers, 3, heads, hdim, hid), (0, 4, 1, 2, 3))
        d_o = grads[1].reshape(n_layers, heads, hdim, hid)
        return (x_one, *states, dx_two, d_qkv, d_o, grads[2].reshape(n_layers, hid, ff), grads[3].reshape(n_layers, ff, hid))

    return jax.shard_map(
        per_device,
        mesh=mesh,
        in_specs=(act_spec,) * 4 + (saved_spec,) * 2 + weight_specs,
        out_specs=(act_spec,) * 4 + grad_specs,
        check_vma=False,
    )
```

```python
import functools

import jax
import jax.numpy as jnp
from jax import lax
from jax.experimental import pallas as pl
from jax.experimental.pallas import tpu as pltpu
from jax.sharding import PartitionSpec as P

EPS = 1e-6
BF = jnp.bfloat16
F32 = jnp.float32
MESH = pl.DeviceIdType.MESH
GELU_C = 0.7978845608028654
GELU_A = 0.044715

NN = (((1,), (0,)), ((), ()))
NT = (((1,), (1,)), ((), ()))
TN = (((0,), (0,)), ((), ()))


def dot(lhs, rhs, dims):
    return lax.dot_general(lhs, rhs, dims, preferred_element_type=F32)


def rms_scale(state):
    return lax.rsqrt(jnp.mean(state * state, axis=-1, keepdims=True) + EPS)


def rms_pull(state, grad):
    scale = rms_scale(state)
    normed = state * scale
    return scale * (grad - normed * jnp.mean(normed * grad, axis=-1, keepdims=True))


def gelu_parts(hidden, want_grad):
    sq = hidden * hidden
    tanh = jnp.tanh(GELU_C * (hidden + GELU_A * (sq * hidden)))
    half = 0.5 * (1.0 + tanh)
    value = hidden * half
    if not want_grad:
        return value, None
    grad = half + 0.5 * hidden * (1.0 - tanh * tanh) * (GELU_C * (1.0 + 3.0 * GELU_A * sq))
    return value, grad


def chain_kernel(
    seq, hid, heads, hdim, n_pairs,
    y1, y2, dy1, dy2, s1, s2, wq_h, wo_h, wi_h, wu_h,
    f_own, j_own, fsum, jsum, ox2, od1, od2, gq, go, gi, gu,
    wq, wo, wi, wu, a_g, act, gp, dhb, finp, finr, qkvt, dqkvt, pt, ot,
    d1b, d2b, d1f, d2f, vbuf, x2r, xl, pbuf, e1r, xs, xr, gbuf, g1r, g2r, stage,
    e1s_s, e1r_s, e2s_s, e2r_s, e3s_s, e3r_s, g1s_s, g1r_s, g2s_s, g2r_s, g3s_s, g3r_s,
    os_s, or_s, ol_s, oo_s, w_s, xl_s, v_s, x2_s, st_s, d_s, gcred,
):
    me = lax.axis_index("tp")
    dp = lax.axis_index("dp")
    ci = lax.rem(me, 2)
    core_peer = (dp, me + 1 - 2 * ci)
    x_peer = (dp, lax.rem(me + 2, 4))
    qw = heads * hdim
    npc = 4
    prow = seq // npc

    barrier = pltpu.get_barrier_semaphore()
    pl.semaphore_signal(barrier, inc=1, device_id=core_peer, device_id_type=MESH)
    pl.semaphore_signal(barrier, inc=1, device_id=x_peer, device_id_type=MESH)

    def rows(seq_idx):
        return pl.ds(pl.multiple_of(seq_idx * seq, seq), seq)

    def mine(c):
        return 2 * c + ci

    def theirs(c):
        return 2 * c + 1 - ci

    def local(src, dst, sem):
        return pltpu.make_async_copy(src, dst, sem)

    def remote(src, dst, ssem, rsem, dev):
        return pltpu.make_async_remote_copy(src_ref=src, dst_ref=dst, send_sem=ssem, recv_sem=rsem, device_id=dev, device_id_type=MESH)

    def weight_copies(slot, blk, which):
        pairs = {"q": (wq_h, wq), "o": (wo_h, wo), "i": (wi_h, wi), "u": (wu_h, wu)}
        return [local(pairs[k][0].at[blk], pairs[k][1].at[slot], w_s.at[slot, "qoiu".index(k)]) for k in which]

    def w_start(slot, blk, which):
        for cp in weight_copies(slot, blk, which):
            cp.start()

    def w_wait(slot, which):
        for cp in weight_copies(slot, 0, which):
            cp.wait()

    def state_start(first, one, pair, rws, dst, sem):
        top, saved = (y1, s1) if one else (y2, s2)
        if first is True:
            local(top.at[rws], dst, sem).start()
        elif first is False:
            local(saved.at[pair, rws], dst, sem).start()
        else:
            @pl.when(first)
            def _():
                local(top.at[rws], dst, sem).start()

            @pl.when(jnp.logical_not(first))
            def _():
                local(saved.at[jnp.minimum(pair, n_pairs - 1), rws], dst, sem).start()

    def state_wait(dst, sem):
        local(y1.at[rows(0)], dst, sem).wait()

    def seq_start(first, one, pair, order=lambda i: i):
        for i in (0, 1):
            state_start(first, one, pair, rows(order(i)), xl.at[i], xl_s.at[i])

    def each_seq(first, one, pair, body, order=lambda i: i):
        @pl.loop(0, 4)
        def _(i):
            slot = lax.rem(i, 2)
            state_wait(xl.at[slot], xl_s.at[slot])
            body(i, order(i), xl[slot])

            @pl.when(i < 2)
            def _():
                state_start(first, one, pair, rows(order(i + 2)), xl.at[slot], xl_s.at[slot])

    def mlp_fwd(slot, lo=0, hi=4):
        @pl.loop(lo, hi)
        def _(s):
            value, grad = gelu_parts(dot(a_g[rows(s), :], wi[slot], NN), True)
            act[rows(s), :] = value.astype(BF)
            gp[rows(s), :] = grad

    def attn_fwd_seq(slot, fin, s):
        cols = rows(s)
        qkv = dot(wq[slot], fin[cols, :], NT).astype(BF)
        qkvt[:, cols] = qkv
        part = lambda j, h: qkv[j * qw + h * hdim:j * qw + (h + 1) * hdim]
        scores = [dot(part(1, h), part(0, h), TN) * (hdim ** -0.5) for h in range(heads)]
        exps = [jnp.exp(sc - jnp.max(sc, axis=0, keepdims=True)) for sc in scores]
        probs = [ex * (1.0 / jnp.sum(ex, axis=0, keepdims=True)) for ex in exps]
        for h in range(heads):
            pt[s * heads + h] = probs[h]
        for h in range(heads):
            ot[h * hdim:(h + 1) * hdim, cols] = dot(part(2, h), probs[h].astype(BF), NN).astype(BF)

    def attn_fwd_plain(pair):
        def body(i, s, state):
            finp[rows(s), :] = (state * rms_scale(state)).astype(BF)
            attn_fwd_seq(0, finp, s)
        each_seq(False, False, pair, body)

    def attn_fwd_rev():
        @pl.loop(0, 4)
        def _(s):
            attn_fwd_seq(1, finr, s)

    results = ((xs.at[2], jsum), (gbuf.at[:, 1], fsum), (x2r, ox2), (d1f, od1), (d2f, od2))

    def emit_copies(idx, c):
        ref, out = results[idx]
        rws = out.at[rows(mine(c))]
        return (
            local(ref.at[c], rws, ol_s.at[idx, c]),
            remote(ref.at[c], rws, os_s.at[idx, c], or_s.at[idx, c], core_peer),
        )

    def own_copy(c):
        return local(results[0][0].at[c], j_own.at[c], oo_s.at[c]) if c is not None else local(gbuf.at[1, 1], f_own, oo_s.at[2])

    def emit(idx, c):
        for cp in emit_copies(idx, c):
            cp.start()

    def emit_own(c):
        own_copy(c).start()

    def e1(slot, c):
        return remote(pbuf.at[c, 0], e1r.at[slot, c], e1s_s.at[slot, c], e1r_s.at[slot, c], core_peer)

    def e2(t, c):
        return remote(xs.at[t, c], xr.at[t, c], e2s_s.at[t, c], e2r_s.at[t, c], x_peer)

    def part_g(slot, ver, c, mode, e1_slot=None):
        for i, s in enumerate((theirs(c), mine(c))):
            d_act = dot(d2b[ver, rows(s), :], wu[slot], NT)
            dh = (d_act * gp[rows(s), :]).astype(BF)
            dhb[rows(s), :] = dh
            part = dot(dh, wi[slot], NT)
            pbuf[c, i] = pbuf[c, i] + part if mode == "add" else part
            if mode != "hold" and i == 0:
                e1(e1_slot, c).start()

    def part_f(slot, c, e1_slot):
        each = range(heads)
        for i, s in enumerate((theirs(c), mine(c))):
            cols = rows(s)
            do_t = dot(wo[slot], d1b[cols, :], NT).astype(BF)
            do = [do_t[h * hdim:(h + 1) * hdim] for h in each]
            part = lambda j, h: qkvt[j * qw + h * hdim:j * qw + (h + 1) * hdim, cols]
            probs = [pt[s * heads + h] for h in each]
            dps = [dot(part(2, h), do[h], TN) for h in each]
            dv = [dot(do[h], probs[h].astype(BF), NT).astype(BF) for h in each]
            ds = []
            for h in each:
                inner = jnp.sum(probs[h] * dps[h], axis=0, keepdims=True)
                ds.append((probs[h] * (dps[h] - inner) * (hdim ** -0.5)).astype(BF))
            dq = [dot(part(1, h), ds[h], NN).astype(BF) for h in each]
            dk = [dot(part(0, h), ds[h], NT).astype(BF) for h in each]
            d_qkv = jnp.concatenate(dq + dk + dv, axis=0)
            dqkvt[:, cols] = d_qkv
            pbuf[c, i] = dot(d_qkv, wq[slot], TN)
            if i == 0:
                e1(e1_slot, c).start()

    def to_x(t, c, e1_slot, last=None):
        e1(e1_slot, c).wait()
        xs[t, c] = (pbuf[c, 1] + e1r[e1_slot, c]).astype(BF)
        if last is None:
            e2(t, c).start()
        else:
            @pl.when(jnp.logical_not(last))
            def _():
                e2(t, c).start()

            @pl.when(last)
            def _():
                emit_own(c)
                emit(0, c)

    def summed(t, c):
        e2(t, c).wait()
        return xs[t, c].astype(F32) + xr[t, c].astype(F32)

    def e3(kind, c):
        ref = d1b.at[rows(mine(c))] if kind == 0 else d2b.at[kind - 1, rows(mine(c))]
        return remote(ref, ref, e3s_s.at[kind, c], e3r_s.at[kind, c], core_peer)

    def finish(t, c, kind, acc, state):
        total = acc[c] + rms_pull(state, summed(t, c))
        acc[c] = total
        if kind is not None:
            if kind == 0:
                d1b[rows(mine(c)), :] = total.astype(BF)
            else:
                d2b[kind - 1, rows(mine(c)), :] = total.astype(BF)
            e3(kind, c).start()

    def g1(c):
        return remote(gbuf.at[c, 0], g1r.at[c], g1s_s.at[c], g1r_s.at[c], core_peer)

    def g2(k):
        c, q = k // npc, k % npc
        rws = pl.ds(q * prow, prow)
        return remote(gbuf.at[c, 1, rws], g2r.at[c, rws], g2s_s.at[k], g2r_s.at[k], x_peer)

    def g_order(i):
        return 2 * (i // 2) + jnp.where(lax.rem(i, 2) == 0, 1 - ci, ci)

    def g_send_core(i):
        for c in (0, 1):
            @pl.when(i == 2 * c)
            def _():
                g1(c).start()

    def g_part(slot, first, pair, keep):
        def body(i, s, state):
            normed = (state * rms_scale(state)).astype(BF)
            a_g[rows(s), :] = normed
            value, grad = gelu_parts(dot(normed, wi[slot], NN), keep)
            value = value.astype(BF)
            if keep:
                act[rows(s), :] = value
                gp[rows(s), :] = grad
            gbuf[i // 2, lax.rem(i, 2)] = dot(value, wu[slot], NN)
            g_send_core(i)

            @pl.when(i == 2)
            def _():
                g_chip(0)
                g_send(*range(npc))
        each_seq(first, True, pair, body, g_order)
        g_chip(1)
        g_send(*range(npc, 2 * npc))

    def f_part(slot):
        @pl.loop(0, 4)
        def _(i):
            gbuf[i // 2, lax.rem(i, 2)] = dot(ot[:, rows(g_order(i))], wo[slot], TN)
            g_send_core(i)

    def g_chip(c):
        g1(c).wait()
        gbuf[c, 1] = gbuf[c, 1] + g1r[c]

    def g_send(*ks):
        for k in ks:
            g2(k).start()

    def g_total(c):
        for q in range(npc):
            g2(c * npc + q).wait()
        return gbuf[c, 1] + g2r[c]

    def g3(c):
        ref = finr.at[rows(mine(c))]
        return remote(ref, ref, g3s_s.at[c], g3r_s.at[c], core_peer)

    def g_finish(c):
        state_wait(x2r.at[c], x2_s.at[c])
        state = x2r[c] - g_total(c)
        x2r[c] = state
        finr[rows(mine(c)), :] = (state * rms_scale(state)).astype(BF)
        g3(c).start()

    def g_credit():
        pl.semaphore_signal(gcred, inc=1, device_id=x_peer, device_id_type=MESH)

    def put(pending, tile, dst, value):
        slot = tile % 3
        height = value.shape[0]
        if pending[slot] is not None:
            pending[slot].wait()
        stage[slot, :height] = value
        cp = local(stage.at[slot, pl.ds(0, height)], dst, st_s.at[slot])
        cp.start()
        pending[slot] = cp

    def flush(pending):
        for cp in pending:
            if cp is not None:
                cp.wait()

    def mlp_out_grads(blk, ver, pending):
        for k in range(hid // 256):
            put(pending, k, gu.at[blk, pl.ds(256 * k, 256)], dot(act[:, 256 * k:256 * (k + 1)], d2b[ver], TN))

    def mlp_in_grads(blk, pending):
        for k in range(hid // 256):
            put(pending, k, gi.at[blk, pl.ds(256 * k, 256)], dot(a_g[:, 256 * k:256 * (k + 1)], dhb[...], TN))

    def attn_grads(blk, fin, pending):
        for k in range(3):
            put(pending, k, gq.at[blk, pl.ds(qw * k, qw)], dot(dqkvt[qw * k:qw * (k + 1), :], fin[...], NN))
        put(pending, 3, go.at[blk], dot(ot[...], d1b[...], NN))

    def v_start(first, one, pair, c):
        state_start(first, one, pair, rows(mine(c)), vbuf.at[c], v_s.at[c])

    def v_wait(c):
        state_wait(vbuf.at[c], v_s.at[c])

    top = 2 * n_pairs
    w_start(1, top, "iu")
    seq_start(True, True, 0, g_order)
    for c in (0, 1):
        v_start(True, True, 0, c)
        state_start(True, False, 0, rows(mine(c)), x2r.at[c], x2_s.at[c])
        local(dy1.at[rows(mine(c))], d1f.at[c], d_s.at[0, c]).start()
        local(dy2.at[rows(mine(c))], d2f.at[c], d_s.at[1, c]).start()
    pl.semaphore_wait(barrier, 2)
    w_wait(1, "iu")
    w_start(1, top, "qo")
    g_part(1, True, 0, True)
    w_start(0, top - 1, "qoiu")
    for i in range(4):
        local(dy2.at[rows(i)], xl.at[i % 2], xl_s.at[i % 2]).start()
        state_wait(xl.at[i % 2], xl_s.at[i % 2])
        d2b[1, rows(i), :] = xl[i % 2].astype(BF)
    for c in (0, 1):
        local(dy1.at[rows(mine(c))], d1f.at[c], d_s.at[0, c]).wait()
        local(dy2.at[rows(mine(c))], d2f.at[c], d_s.at[1, c]).wait()

    @pl.loop(0, n_pairs + 1)
    def _(it):
        pair = n_pairs - it
        is_top = it == 0
        more = it < n_pairs
        rev = 2 * pair
        even, odd = lax.rem(it, 2), lax.rem(it + 1, 2)

        @pl.when(is_top)
        def _():
            @pl.loop(0, 2)
            def _(c):
                part_g(1, 1, c, "first", odd)
                to_x(1, c, odd)

        @pl.when(it > 0)
        def _():
            @pl.loop(0, 2)
            def _(c):
                v_wait(c)
                finish(0, c, 2, d2f, vbuf[c])
                v_start(False, True, pair, c)
                mlp_fwd(1, 2 * c, 2 * c + 2)
                e3(2, c).wait()
                part_g(1, 1, c, "add", odd)
                to_x(1, c, odd)

        @pl.when(more)
        def _():
            w_start(1, rev - 2, "iu")

        for c in (0, 1):
            g_finish(c)

        g_credit()

        @pl.when(jnp.logical_not(more))
        def _():
            for c in (0, 1):
                emit(2, c)
                emit(4, c)
        w_wait(1, "qo")
        for c in (0, 1):
            g3(c).wait()
        attn_fwd_rev()

        @pl.when(jnp.logical_not(more))
        def _():
            f_part(1)
            g_chip(0)
            pl.semaphore_wait(gcred, 1)
            g_send(*range(npc))
            g_chip(1)
            emit_own(None)
            emit(1, 1)

        pending = [None] * 3
        for c in (0, 1):
            v_wait(c)
            finish(1, c, 0, d1f, vbuf[c])

            @pl.when(jnp.logical_not(more))
            def _():
                emit(3, c)
            if c == 0:
                mlp_out_grads(rev, 1, pending)
            else:
                mlp_in_grads(rev, pending)
            e3(0, c).wait()
            part_f(1, c, even)
            to_x(2, c, even, jnp.logical_not(more))

        @pl.when(more)
        def _():
            seq_start(False, False, pair - 1)
        attn_grads(rev, finr, pending)
        flush(pending)

        @pl.when(more)
        def _():
            w_start(1, rev - 2, "qo")
            for c in (0, 1):
                v_start(False, False, pair - 1, c)
            w_wait(0, "qo")
            attn_fwd_plain(pair - 1)
            seq_start(False, True, pair - 1, g_order)

            @pl.loop(0, 2)
            def _(c):
                part_f(0, c, odd)
                to_x(0, c, odd)
            w_wait(1, "iu")
            pl.semaphore_wait(gcred, 1)
            g_part(1, False, pair - 1, False)
            w_wait(0, "iu")
            mlp_fwd(0)
            for c in (0, 1):
                finish(2, c, 1, d2f, x2r[c])
                state_start(False, False, pair - 1, rows(mine(c)), x2r.at[c], x2_s.at[c])
            @pl.loop(0, 2)
            def _(c):
                e3(1, c).wait()
                part_g(0, 0, c, "hold")

            @pl.when(it < n_pairs - 1)
            def _():
                w_start(0, rev - 3, "qoiu")
            later = [None] * 3
            mlp_out_grads(rev - 1, 0, later)
            mlp_in_grads(rev - 1, later)
            attn_grads(rev - 1, finp, later)
            flush(later)

    gbuf[0, 1] = g_total(0)
    emit(1, 0)
    for c in (0, 1, None):
        own_copy(c).wait()
    for c in (0, 1):
        for idx in range(5):
            for cp in emit_copies(idx, c):
                cp.wait()


def move_kernel(depth, chunk, *refs):
    count = (len(refs) - 3) // 2
    buf, in_s, out_s = refs[-3:]
    jobs = []
    for src, dst in zip(refs[:count], refs[count:2 * count]):
        for lo in range(0, src.shape[0], chunk):
            rws = pl.ds(lo, min(chunk, src.shape[0] - lo))
            slot = len(jobs) % depth
            part = buf.at[slot, pl.ds(0, rws.size)]
            jobs.append((
                pltpu.make_async_copy(src.at[rws], part, in_s.at[slot]),
                pltpu.make_async_copy(part, dst.at[rws], out_s.at[slot]),
            ))
    for load, _ in jobs[:depth]:
        load.start()
    lag = depth // 2
    for k in range(len(jobs)):
        jobs[k][0].wait()
        jobs[k][1].start()
        if k >= lag:
            jobs[k - lag][1].wait()
            if k - lag + depth < len(jobs):
                jobs[k - lag + depth][0].start()
    for k in range(max(len(jobs) - lag, 0), len(jobs)):
        jobs[k][1].wait()


def move(arrays, name, depth=12, chunk=576):
    width = arrays[0].shape[-1]
    size = sum(arr.size for arr in arrays)
    depth = min(depth, sum(-(-arr.shape[0] // chunk) for arr in arrays))
    anyspec = pl.BlockSpec(memory_space=pl.ANY)
    return pl.pallas_call(
        functools.partial(move_kernel, depth, chunk),
        out_shape=[jax.ShapeDtypeStruct(arr.shape, arr.dtype) for arr in arrays],
        in_specs=[anyspec] * len(arrays),
        out_specs=[anyspec] * len(arrays),
        scratch_shapes=[pltpu.VMEM((depth, chunk, width), F32), pltpu.SemaphoreType.DMA((depth,)), pltpu.SemaphoreType.DMA((depth,))],
        name=name,
        cost_estimate=pl.CostEstimate(flops=400 * size, bytes_accessed=8 * size, transcendentals=0),
        compiler_params=pltpu.CompilerParams(vmem_limit_bytes=depth * chunk * width * 4 + 2 ** 20),
    )(*arrays)


def take_kernel(finish, first, *refs):
    *base, near_ref, far_ref, out_ref = refs
    seq_idx = pl.program_id(0)
    odd = lax.rem(seq_idx + lax.axis_index("tp"), 2)
    ready = seq_idx < first

    @pl.when(ready)
    def _():
        out_ref[...] = finish(None, *[ref[...] for ref in base])

    @pl.when(jnp.logical_not(ready) & (odd == 0))
    def _():
        out_ref[...] = finish(near_ref[...].astype(F32), *[ref[...] for ref in base])

    @pl.when(jnp.logical_not(ready) & (odd != 0))
    def _():
        out_ref[...] = finish(far_ref[...].astype(F32), *[ref[...] for ref in base])


def take(finish, first, name, shape, base, near, far):
    n_seq, seq, hid = shape
    whole = pl.BlockSpec((1, seq, hid), lambda s: (s, 0, 0))
    bottom = pl.BlockSpec((None, 1, seq, hid), lambda s: (0, s, 0, 0))
    half = pl.BlockSpec((1, seq, hid), lambda s: (jnp.maximum(s - first, 0) // 2, 0, 0))
    return pl.pallas_call(
        functools.partial(take_kernel, finish, first),
        out_shape=jax.ShapeDtypeStruct(shape, F32),
        grid=(n_seq,),
        in_specs=[whole if arr.ndim == 3 else bottom for arr in base] + [half, half],
        out_specs=whole,
        name=name,
        cost_estimate=pl.CostEstimate(flops=40_000_000, bytes_accessed=16_000_000, transcendentals=0),
    )(*base, near, far)


def finish_x(other, state, own):
    return state - (own if other is None else own + other)


def finish_d(other, grad, state, own):
    own = own.astype(F32)
    return grad + rms_pull(state, own if other is None else own + other)


def solution(mesh):
    act_spec = P("dp", None, None)
    saved_spec = P(None, "dp", None, None)
    weight_specs = (P(None, None, None, "tp", None), P(None, "tp", None, None), P(None, None, "tp"), P(None, "tp", None))
    grad_specs = (P("dp", None, None, "tp", None), P("dp", "tp", None, None), P("dp", None, "tp"), P("dp", "tp", None))

    def per_device(y_one, y_two, dy_one, dy_two, saved_one, saved_two, w_qkv, w_o, w_in, w_out):
        n_seq, seq, hid = y_one.shape
        n_layers, _, _, heads, hdim = w_qkv.shape
        n_pairs = saved_one.shape[0]
        ff = w_in.shape[-1]
        tok = n_seq * seq
        qkv_w = 3 * heads * hdim
        flat = lambda arr: arr.reshape(arr.shape[:-3] + (tok, hid))
        wq_t = jnp.transpose(w_qkv, (0, 2, 3, 4, 1)).reshape(n_layers, qkv_w, hid)
        wo_t = w_o.reshape(n_layers, heads * hdim, hid)
        sds = jax.ShapeDtypeStruct
        vm = pltpu.VMEM
        dma = pltpu.SemaphoreType.DMA
        half = (2, seq, hid)
        scratch = [
            vm((2, qkv_w, hid), BF), vm((2, heads * hdim, hid), BF), vm((2, hid, ff), BF), vm((2, ff, hid), BF),
            vm((tok, hid), BF), vm((tok, ff), BF), vm((tok, ff), F32), vm((tok, ff), BF),
            vm((tok, hid), BF), vm((tok, hid), BF), vm((qkv_w, tok), BF), vm((qkv_w, tok), BF),
            vm((n_seq * heads, seq, seq), F32), vm((heads * hdim, tok), BF),
            vm((tok, hid), BF), vm((2, tok, hid), BF), vm(half, F32), vm(half, F32),
            vm(half, F32), vm(half, F32), vm(half, F32),
            vm((2,) + half, F32), vm((2,) + half, F32), vm((3,) + half, BF), vm((3,) + half, BF),
            vm((2,) + half, F32), vm(half, F32), vm(half, F32), vm((3, 256, hid), F32),
            dma((2, 2)), dma((2, 2)), dma((3, 2)), dma((3, 2)), dma((3, 2)), dma((3, 2)),
            dma((2,)), dma((2,)), dma((8,)), dma((8,)), dma((2,)), dma((2,)),
            dma((5, 2)), dma((5, 2)), dma((5, 2)), dma((3,)), dma((2, 4)), dma((2,)), dma((2,)), dma((2,)), dma((3,)), dma((2, 2)),
            pltpu.SemaphoreType.REGULAR,
        ]
        anyspec = pl.BlockSpec(memory_space=pl.ANY)
        outs = pl.pallas_call(
            functools.partial(chain_kernel, seq, hid, heads, hdim, n_pairs),
            out_shape=[sds(half[1:], F32), sds(half, BF), sds((tok, hid), F32), sds((tok, hid), BF)] + [sds((tok, hid), F32)] * 3
            + [sds((n_layers, qkv_w, hid), F32), sds((n_layers, heads * hdim, hid), F32), sds((n_layers, hid, ff), F32), sds((n_layers, ff, hid), F32)],
            in_specs=[anyspec] * 10,
            out_specs=[anyspec] * 11,
            scratch_shapes=scratch,
            name="chain",
            compiler_params=pltpu.CompilerParams(collective_id=0, has_side_effects=True, vmem_limit_bytes=67043328),
        )(flat(y_one), flat(y_two), flat(dy_one), flat(dy_two), flat(saved_one), flat(saved_two), wq_t, wo_t, w_in, w_out)
        f_own, j_own, f_all, j_all, x_two, d_one, d_two = outs[:7]
        cube = lambda arr: arr.reshape(n_seq, seq, hid)
        over_x = lambda arr: lax.ppermute(arr, "tp", [(0, 2), (2, 0), (1, 3), (3, 1)])
        over_core = lambda arr: lax.ppermute(arr, "tp", [(0, 1), (1, 0), (2, 3), (3, 2)])
        f_near, j_near = over_x(f_own), over_x(j_own)
        grads = move([out.reshape(-1, hid) for out in outs[7:]], "move_grads")
        f_near, j_near, grads = lax.optimization_barrier((f_near, j_near, grads))
        f_far, j_far = over_core(f_near), over_core(j_near)
        states = [cube(out) for out in move([x_two, d_one], "move_states")]
        x_one = take(finish_x, 2, "finish_x", (n_seq, seq, hid), [saved_one, cube(f_all)], f_near[None], f_far[None])
        dx_two = take(finish_d, 0, "finish_d", (n_seq, seq, hid), [cube(d_two), cube(x_two), cube(j_all)], j_near, j_far)
        d_qkv = jnp.transpose(grads[0].reshape(n_layers, 3, heads, hdim, hid), (0, 4, 1, 2, 3))
        d_o = grads[1].reshape(n_layers, heads, hdim, hid)
        return (x_one, *states, dx_two, d_qkv, d_o, grads[2].reshape(n_layers, hid, ff), grads[3].reshape(n_layers, ff, hid))

    return jax.shard_map(
        per_device,
        mesh=mesh,
        in_specs=(act_spec,) * 4 + (saved_spec,) * 2 + weight_specs,
        out_specs=(act_spec,) * 4 + grad_specs,
        check_vma=False,
    )
```

```python
import functools

import jax
import jax.numpy as jnp
from jax import lax
from jax.experimental import pallas as pl
from jax.experimental.pallas import tpu as pltpu
from jax.sharding import PartitionSpec as P

EPS = 1e-6
BF = jnp.bfloat16
F32 = jnp.float32
MESH = pl.DeviceIdType.MESH
GELU_C = 0.7978845608028654
GELU_A = 0.044715
GRANT = 40

NN = (((1,), (0,)), ((), ()))
NT = (((1,), (1,)), ((), ()))
TN = (((0,), (0,)), ((), ()))


def dot(lhs, rhs, dims):
    return lax.dot_general(lhs, rhs, dims, preferred_element_type=F32)


def rms_scale(state):
    return lax.rsqrt(jnp.mean(state * state, axis=-1, keepdims=True) + EPS)


def rms_pull(state, grad):
    scale = rms_scale(state)
    normed = state * scale
    return scale * (grad - normed * jnp.mean(normed * grad, axis=-1, keepdims=True))


def gelu_parts(hidden, want_grad):
    sq = hidden * hidden
    tanh = jnp.tanh(GELU_C * (hidden + GELU_A * (sq * hidden)))
    half = 0.5 * (1.0 + tanh)
    value = hidden * half
    if not want_grad:
        return value, None
    grad = half + 0.5 * hidden * (1.0 - tanh * tanh) * (GELU_C * (1.0 + 3.0 * GELU_A * sq))
    return value, grad


def chain_kernel(
    seq, hid, heads, hdim, n_pairs,
    y1, y2, dy1, dy2, s1, s2, wq_h, wo_h, wi_h, wu_h,
    f_own, j_own, fsum, jsum, ox2, od1, od2, gq, go, gi, gu,
    wq, wo, wi, wu, a_g, act, gp, dhb, finp, finr, qkvt, dqkvt, pt, ot,
    d1b, d2b, d1f, d2f, vbuf, x2r, xl, pbuf, e1r, xs, xr, gbuf, g1r, g2r, stage,
    e1s_s, e1r_s, e2s_s, e2r_s, e3s_s, e3r_s, g1s_s, g1r_s, g2s_s, g2r_s, g3s_s, g3r_s,
    os_s, or_s, ol_s, oo_s, w_s, xl_s, v_s, x2_s, st_s, d_s, gcred,
):
    me = lax.axis_index("tp")
    dp = lax.axis_index("dp")
    ci = lax.rem(me, 2)
    core_peer = (dp, me + 1 - 2 * ci)
    x_peer = (dp, lax.rem(me + 2, 4))
    qw = heads * hdim
    npc = 4
    prow = seq // npc

    barrier = pltpu.get_barrier_semaphore()
    pl.semaphore_signal(barrier, inc=1, device_id=core_peer, device_id_type=MESH)
    pl.semaphore_signal(barrier, inc=1, device_id=x_peer, device_id_type=MESH)

    def rows(seq_idx):
        return pl.ds(pl.multiple_of(seq_idx * seq, seq), seq)

    def mine(c):
        return 2 * c + ci

    def theirs(c):
        return 2 * c + 1 - ci

    def local(src, dst, sem):
        return pltpu.make_async_copy(src, dst, sem)

    def remote(src, dst, ssem, rsem, dev):
        return pltpu.make_async_remote_copy(src_ref=src, dst_ref=dst, send_sem=ssem, recv_sem=rsem, device_id=dev, device_id_type=MESH)

    def weight_copies(slot, blk, which):
        pairs = {"q": (wq_h, wq), "o": (wo_h, wo), "i": (wi_h, wi), "u": (wu_h, wu)}
        return [local(pairs[k][0].at[blk], pairs[k][1].at[slot], w_s.at[slot, "qoiu".index(k)]) for k in which]

    def w_start(slot, blk, which):
        for cp in weight_copies(slot, blk, which):
            cp.start()

    def w_wait(slot, which):
        for cp in weight_copies(slot, 0, which):
            cp.wait()

    def state_start(first, one, pair, rws, dst, sem):
        top, saved = (y1, s1) if one else (y2, s2)
        if first is True:
            local(top.at[rws], dst, sem).start()
        elif first is False:
            local(saved.at[pair, rws], dst, sem).start()
        else:
            @pl.when(first)
            def _():
                local(top.at[rws], dst, sem).start()

            @pl.when(jnp.logical_not(first))
            def _():
                local(saved.at[jnp.minimum(pair, n_pairs - 1), rws], dst, sem).start()

    def state_wait(dst, sem):
        local(y1.at[rows(0)], dst, sem).wait()

    def seq_start(first, one, pair, order=lambda i: i):
        for i in (0, 1):
            state_start(first, one, pair, rows(order(i)), xl.at[i], xl_s.at[i])

    def each_seq(first, one, pair, body, order=lambda i: i):
        @pl.loop(0, 4)
        def _(i):
            slot = lax.rem(i, 2)
            state_wait(xl.at[slot], xl_s.at[slot])
            body(i, order(i), xl[slot])

            @pl.when(i < 2)
            def _():
                state_start(first, one, pair, rows(order(i + 2)), xl.at[slot], xl_s.at[slot])

    def mlp_fwd(slot, lo=0, hi=4):
        @pl.loop(lo, hi)
        def _(s):
            value, grad = gelu_parts(dot(a_g[rows(s), :], wi[slot], NN), True)
            act[rows(s), :] = value.astype(BF)
            gp[rows(s), :] = grad

    def attn_fwd_seq(slot, fin, s):
        cols = rows(s)
        qkv = dot(wq[slot], fin[cols, :], NT).astype(BF)
        qkvt[:, cols] = qkv
        part = lambda j, h: qkv[j * qw + h * hdim:j * qw + (h + 1) * hdim]
        scores = [dot(part(1, h), part(0, h), TN) * (hdim ** -0.5) for h in range(heads)]
        exps = [jnp.exp(sc - jnp.max(sc, axis=0, keepdims=True)) for sc in scores]
        probs = [ex * (1.0 / jnp.sum(ex, axis=0, keepdims=True)) for ex in exps]
        for h in range(heads):
            pt[s * heads + h] = probs[h]
        for h in range(heads):
            ot[h * hdim:(h + 1) * hdim, cols] = dot(part(2, h), probs[h].astype(BF), NN).astype(BF)

    def attn_fwd_plain(pair):
        def body(i, s, state):
            finp[rows(s), :] = (state * rms_scale(state)).astype(BF)
            attn_fwd_seq(0, finp, s)
        each_seq(False, False, pair, body)

    def attn_fwd_rev():
        @pl.loop(0, 4)
        def _(s):
            attn_fwd_seq(1, finr, s)

    results = ((xs.at[2], jsum), (gbuf.at[:, 1], fsum), (x2r, ox2), (d1f, od1), (d2f, od2))

    def emit_copies(idx, c):
        ref, out = results[idx]
        rws = out.at[rows(mine(c))]
        return (
            local(ref.at[c], rws, ol_s.at[idx, c]),
            remote(ref.at[c], rws, os_s.at[idx, c], or_s.at[idx, c], core_peer),
        )

    def own_copy(c):
        return local(results[0][0].at[c], j_own.at[c], oo_s.at[c]) if c is not None else local(gbuf.at[1, 1], f_own, oo_s.at[2])

    def emit(idx, c):
        for cp in emit_copies(idx, c):
            cp.start()

    def emit_own(c):
        own_copy(c).start()

    def e1(slot, c):
        return remote(pbuf.at[c, 0], e1r.at[slot, c], e1s_s.at[slot, c], e1r_s.at[slot, c], core_peer)

    def e2(t, c):
        return remote(xs.at[t, c], xr.at[t, c], e2s_s.at[t, c], e2r_s.at[t, c], x_peer)

    def part_g(slot, ver, c, mode, e1_slot=None):
        for i, s in enumerate((theirs(c), mine(c))):
            d_act = dot(d2b[ver, rows(s), :], wu[slot], NT)
            dh = (d_act * gp[rows(s), :]).astype(BF)
            dhb[rows(s), :] = dh
            part = dot(dh, wi[slot], NT)
            pbuf[c, i] = pbuf[c, i] + part if mode == "add" else part
            if mode != "hold" and i == 0:
                e1(e1_slot, c).start()

    def part_f(slot, c, e1_slot):
        each = range(heads)
        for i, s in enumerate((theirs(c), mine(c))):
            cols = rows(s)
            do_t = dot(wo[slot], d1b[cols, :], NT).astype(BF)
            do = [do_t[h * hdim:(h + 1) * hdim] for h in each]
            part = lambda j, h: qkvt[j * qw + h * hdim:j * qw + (h + 1) * hdim, cols]
            probs = [pt[s * heads + h] for h in each]
            dps = [dot(part(2, h), do[h], TN) for h in each]
            dv = [dot(do[h], probs[h].astype(BF), NT).astype(BF) for h in each]
            ds = []
            for h in each:
                inner = jnp.sum(probs[h] * dps[h], axis=0, keepdims=True)
                ds.append((probs[h] * (dps[h] - inner) * (hdim ** -0.5)).astype(BF))
            dq = [dot(part(1, h), ds[h], NN).astype(BF) for h in each]
            dk = [dot(part(0, h), ds[h], NT).astype(BF) for h in each]
            d_qkv = jnp.concatenate(dq + dk + dv, axis=0)
            dqkvt[:, cols] = d_qkv
            pbuf[c, i] = dot(d_qkv, wq[slot], TN)
            if i == 0:
                e1(e1_slot, c).start()

    def to_x(t, c, e1_slot, last=None):
        e1(e1_slot, c).wait()
        xs[t, c] = (pbuf[c, 1] + e1r[e1_slot, c]).astype(BF)
        if last is None:
            e2(t, c).start()
        else:
            @pl.when(jnp.logical_not(last))
            def _():
                e2(t, c).start()

            @pl.when(last)
            def _():
                emit_own(c)
                emit(0, c)

    def summed(t, c):
        e2(t, c).wait()
        return xs[t, c].astype(F32) + xr[t, c].astype(F32)

    def e3(kind, c):
        ref = d1b.at[rows(mine(c))] if kind == 0 else d2b.at[kind - 1, rows(mine(c))]
        return remote(ref, ref, e3s_s.at[kind, c], e3r_s.at[kind, c], core_peer)

    def finish(t, c, kind, acc, state):
        total = acc[c] + rms_pull(state, summed(t, c))
        acc[c] = total
        if kind is not None:
            if kind == 0:
                d1b[rows(mine(c)), :] = total.astype(BF)
            else:
                d2b[kind - 1, rows(mine(c)), :] = total.astype(BF)
            e3(kind, c).start()

    def g1(c):
        return remote(gbuf.at[c, 0], g1r.at[c], g1s_s.at[c], g1r_s.at[c], core_peer)

    def g2(k):
        c, q = k // npc, k % npc
        rws = pl.ds(q * prow, prow)
        return remote(gbuf.at[c, 1, rws], g2r.at[c, rws], g2s_s.at[k], g2r_s.at[k], x_peer)

    def g_order(i):
        return 2 * (i // 2) + jnp.where(lax.rem(i, 2) == 0, 1 - ci, ci)

    def g_send_core(i):
        for c in (0, 1):
            @pl.when(i == 2 * c)
            def _():
                g1(c).start()

    def g_part(slot, first, pair, keep):
        def body(i, s, state):
            normed = (state * rms_scale(state)).astype(BF)
            a_g[rows(s), :] = normed
            value, grad = gelu_parts(dot(normed, wi[slot], NN), keep)
            value = value.astype(BF)
            if keep:
                act[rows(s), :] = value
                gp[rows(s), :] = grad
            gbuf[i // 2, lax.rem(i, 2)] = dot(value, wu[slot], NN)
            g_send_core(i)

            @pl.when(i == 2)
            def _():
                g_chip(0)
                g_send(*range(npc))
        each_seq(first, True, pair, body, g_order)
        g_chip(1)
        g_send(*range(npc, 2 * npc))

    def f_part(slot):
        @pl.loop(0, 4)
        def _(i):
            gbuf[i // 2, lax.rem(i, 2)] = dot(ot[:, rows(g_order(i))], wo[slot], TN)
            g_send_core(i)

    def g_chip(c):
        g1(c).wait()
        gbuf[c, 1] = gbuf[c, 1] + g1r[c]

    def g_send(*ks):
        for k in ks:
            g2(k).start()

    def g_total(c):
        for q in range(npc):
            g2(c * npc + q).wait()
        return gbuf[c, 1] + g2r[c]

    def g3(c):
        ref = finr.at[rows(mine(c))]
        return remote(ref, ref, g3s_s.at[c], g3r_s.at[c], core_peer)

    def g_finish(c):
        state_wait(x2r.at[c], x2_s.at[c])
        state = x2r[c] - g_total(c)
        x2r[c] = state
        finr[rows(mine(c)), :] = (state * rms_scale(state)).astype(BF)
        g3(c).start()

    def g_credit():
        pl.semaphore_signal(gcred, inc=1, device_id=x_peer, device_id_type=MESH)

    def put(pending, tile, dst, value):
        slot = tile % 3
        height = value.shape[0]
        if pending[slot] is not None:
            pending[slot].wait()
        stage[slot, :height] = value
        cp = local(stage.at[slot, pl.ds(0, height)], dst, st_s.at[slot])
        cp.start()
        pending[slot] = cp

    def flush(pending):
        for cp in pending:
            if cp is not None:
                cp.wait()

    def mlp_out_grads(blk, ver, pending):
        for k in range(hid // 256):
            put(pending, k, gu.at[blk, pl.ds(256 * k, 256)], dot(act[:, 256 * k:256 * (k + 1)], d2b[ver], TN))

    def mlp_in_grads(blk, pending):
        for k in range(hid // 256):
            put(pending, k, gi.at[blk, pl.ds(256 * k, 256)], dot(a_g[:, 256 * k:256 * (k + 1)], dhb[...], TN))

    def attn_grads(blk, fin, pending):
        for k in range(3):
            put(pending, k, gq.at[blk, pl.ds(qw * k, qw)], dot(dqkvt[qw * k:qw * (k + 1), :], fin[...], NN))
        put(pending, 3, go.at[blk], dot(ot[...], d1b[...], NN))

    def v_start(first, one, pair, c):
        state_start(first, one, pair, rows(mine(c)), vbuf.at[c], v_s.at[c])

    def v_wait(c):
        state_wait(vbuf.at[c], v_s.at[c])

    top = 2 * n_pairs
    w_start(1, top, "iu")
    seq_start(True, True, 0, g_order)
    for c in (0, 1):
        v_start(True, True, 0, c)
        state_start(True, False, 0, rows(mine(c)), x2r.at[c], x2_s.at[c])
        local(dy1.at[rows(mine(c))], d1f.at[c], d_s.at[0, c]).start()
        local(dy2.at[rows(mine(c))], d2f.at[c], d_s.at[1, c]).start()
    pl.semaphore_wait(barrier, 2)
    w_wait(1, "iu")
    w_start(1, top, "qo")
    g_part(1, True, 0, True)
    w_start(0, top - 1, "qoiu")
    for i in range(4):
        local(dy2.at[rows(i)], xl.at[i % 2], xl_s.at[i % 2]).start()
        state_wait(xl.at[i % 2], xl_s.at[i % 2])
        d2b[1, rows(i), :] = xl[i % 2].astype(BF)
    for c in (0, 1):
        local(dy1.at[rows(mine(c))], d1f.at[c], d_s.at[0, c]).wait()
        local(dy2.at[rows(mine(c))], d2f.at[c], d_s.at[1, c]).wait()

    @pl.loop(0, n_pairs + 1)
    def _(it):
        pair = n_pairs - it
        is_top = it == 0
        more = it < n_pairs
        rev = 2 * pair
        even, odd = lax.rem(it, 2), lax.rem(it + 1, 2)

        @pl.when(is_top)
        def _():
            @pl.loop(0, 2)
            def _(c):
                part_g(1, 1, c, "first", odd)
                to_x(1, c, odd)

        @pl.when(it > 0)
        def _():
            @pl.loop(0, 2)
            def _(c):
                v_wait(c)
                finish(0, c, 2, d2f, vbuf[c])
                v_start(False, True, pair, c)
                mlp_fwd(1, 2 * c, 2 * c + 2)
                e3(2, c).wait()
                part_g(1, 1, c, "add", odd)
                to_x(1, c, odd)

        @pl.when(more)
        def _():
            w_start(1, rev - 2, "iu")

        for c in (0, 1):
            g_finish(c)

        g_credit()

        @pl.when(jnp.logical_not(more))
        def _():
            for c in (0, 1):
                emit(2, c)
                emit(4, c)
        w_wait(1, "qo")
        for c in (0, 1):
            g3(c).wait()
        attn_fwd_rev()

        @pl.when(jnp.logical_not(more))
        def _():
            f_part(1)
            g_chip(0)
            pl.semaphore_wait(gcred, 1)
            g_send(*range(npc))
            g_chip(1)
            emit_own(None)
            emit(1, 1)

        pending = [None] * 3
        for c in (0, 1):
            v_wait(c)
            finish(1, c, 0, d1f, vbuf[c])

            @pl.when(jnp.logical_not(more))
            def _():
                emit(3, c)
            if c == 0:
                mlp_out_grads(rev, 1, pending)
            else:
                mlp_in_grads(rev, pending)
            e3(0, c).wait()
            part_f(1, c, even)
            to_x(2, c, even, jnp.logical_not(more))

        @pl.when(more)
        def _():
            seq_start(False, False, pair - 1)
        attn_grads(rev, finr, pending)
        flush(pending)

        @pl.when(more)
        def _():
            w_start(1, rev - 2, "qo")
            for c in (0, 1):
                v_start(False, False, pair - 1, c)
            w_wait(0, "qo")
            attn_fwd_plain(pair - 1)
            seq_start(False, True, pair - 1, g_order)

            @pl.loop(0, 2)
            def _(c):
                part_f(0, c, odd)
                to_x(0, c, odd)
            w_wait(1, "iu")
            pl.semaphore_wait(gcred, 1)
            g_part(1, False, pair - 1, False)
            w_wait(0, "iu")
            mlp_fwd(0)
            for c in (0, 1):
                finish(2, c, 1, d2f, x2r[c])
                state_start(False, False, pair - 1, rows(mine(c)), x2r.at[c], x2_s.at[c])
            @pl.loop(0, 2)
            def _(c):
                e3(1, c).wait()
                part_g(0, 0, c, "hold")

            @pl.when(it < n_pairs - 1)
            def _():
                w_start(0, rev - 3, "qoiu")
            later = [None] * 3
            mlp_out_grads(rev - 1, 0, later)
            mlp_in_grads(rev - 1, later)
            attn_grads(rev - 1, finp, later)
            flush(later)

    gbuf[0, 1] = g_total(0)
    emit(1, 0)
    for c in (0, 1, None):
        own_copy(c).wait()
    for c in (0, 1):
        for idx in range(5):
            for cp in emit_copies(idx, c):
                cp.wait()


def move_kernel(depth, chunk, *refs):
    count = (len(refs) - 3) // 2
    buf, in_s, out_s = refs[-3:]
    jobs = []
    for src, dst in zip(refs[:count], refs[count:2 * count]):
        for lo in range(0, src.shape[0], chunk):
            rws = pl.ds(lo, min(chunk, src.shape[0] - lo))
            slot = len(jobs) % depth
            part = buf.at[slot, pl.ds(0, rws.size)]
            jobs.append((
                pltpu.make_async_copy(src.at[rws], part, in_s.at[slot]),
                pltpu.make_async_copy(part, dst.at[rws], out_s.at[slot]),
            ))
    for load, _ in jobs[:depth]:
        load.start()
    lag = depth // 2
    for k in range(len(jobs)):
        jobs[k][0].wait()
        jobs[k][1].start()
        if k >= lag:
            jobs[k - lag][1].wait()
            if k - lag + depth < len(jobs):
                jobs[k - lag + depth][0].start()
    for k in range(max(len(jobs) - lag, 0), len(jobs)):
        jobs[k][1].wait()


def move(arrays, name, depth=12, chunk=576):
    width = arrays[0].shape[-1]
    size = sum(arr.size for arr in arrays)
    depth = min(depth, sum(-(-arr.shape[0] // chunk) for arr in arrays))
    anyspec = pl.BlockSpec(memory_space=pl.ANY)
    return pl.pallas_call(
        functools.partial(move_kernel, depth, chunk),
        out_shape=[jax.ShapeDtypeStruct(arr.shape, arr.dtype) for arr in arrays],
        in_specs=[anyspec] * len(arrays),
        out_specs=[anyspec] * len(arrays),
        scratch_shapes=[pltpu.VMEM((depth, chunk, width), F32), pltpu.SemaphoreType.DMA((depth,)), pltpu.SemaphoreType.DMA((depth,))],
        name=name,
        cost_estimate=pl.CostEstimate(flops=400 * size, bytes_accessed=8 * size, transcendentals=0),
        compiler_params=pltpu.CompilerParams(vmem_limit_bytes=60 * 2 ** 20),
    )(*arrays)


def take_kernel(finish, first, *refs):
    *base, near_ref, far_ref, out_ref = refs
    seq_idx = pl.program_id(0)
    odd = lax.rem(seq_idx + lax.axis_index("tp"), 2)
    ready = seq_idx < first

    @pl.when(ready)
    def _():
        out_ref[...] = finish(None, *[ref[...] for ref in base])

    @pl.when(jnp.logical_not(ready) & (odd == 0))
    def _():
        out_ref[...] = finish(near_ref[...].astype(F32), *[ref[...] for ref in base])

    @pl.when(jnp.logical_not(ready) & (odd != 0))
    def _():
        out_ref[...] = finish(far_ref[...].astype(F32), *[ref[...] for ref in base])


def take(finish, first, name, shape, base, near, far):
    n_seq, seq, hid = shape
    whole = pl.BlockSpec((1, seq, hid), lambda s: (s, 0, 0))
    bottom = pl.BlockSpec((None, 1, seq, hid), lambda s: (0, s, 0, 0))
    half = pl.BlockSpec((1, seq, hid), lambda s: (jnp.maximum(s - first, 0) // 2, 0, 0))
    return pl.pallas_call(
        functools.partial(take_kernel, finish, first),
        out_shape=jax.ShapeDtypeStruct(shape, F32),
        grid=(n_seq,),
        in_specs=[whole if arr.ndim == 3 else bottom for arr in base] + [half, half],
        out_specs=whole,
        name=name,
        cost_estimate=pl.CostEstimate(flops=40_000_000, bytes_accessed=16_000_000, transcendentals=0),
        compiler_params=pltpu.CompilerParams(vmem_limit_bytes=GRANT * 2 ** 20),
    )(*base, near, far)


def finish_x(other, state, own):
    return state - (own if other is None else own + other)


def finish_d(other, grad, state, own):
    own = own.astype(F32)
    return grad + rms_pull(state, own if other is None else own + other)


def solution(mesh):
    act_spec = P("dp", None, None)
    saved_spec = P(None, "dp", None, None)
    weight_specs = (P(None, None, None, "tp", None), P(None, "tp", None, None), P(None, None, "tp"), P(None, "tp", None))
    grad_specs = (P("dp", None, None, "tp", None), P("dp", "tp", None, None), P("dp", None, "tp"), P("dp", "tp", None))

    def per_device(y_one, y_two, dy_one, dy_two, saved_one, saved_two, w_qkv, w_o, w_in, w_out):
        n_seq, seq, hid = y_one.shape
        n_layers, _, _, heads, hdim = w_qkv.shape
        n_pairs = saved_one.shape[0]
        ff = w_in.shape[-1]
        tok = n_seq * seq
        qkv_w = 3 * heads * hdim
        flat = lambda arr: arr.reshape(arr.shape[:-3] + (tok, hid))
        wq_t = jnp.transpose(w_qkv, (0, 2, 3, 4, 1)).reshape(n_layers, qkv_w, hid)
        wo_t = w_o.reshape(n_layers, heads * hdim, hid)
        sds = jax.ShapeDtypeStruct
        vm = pltpu.VMEM
        dma = pltpu.SemaphoreType.DMA
        half = (2, seq, hid)
        scratch = [
            vm((2, qkv_w, hid), BF), vm((2, heads * hdim, hid), BF), vm((2, hid, ff), BF), vm((2, ff, hid), BF),
            vm((tok, hid), BF), vm((tok, ff), BF), vm((tok, ff), F32), vm((tok, ff), BF),
            vm((tok, hid), BF), vm((tok, hid), BF), vm((qkv_w, tok), BF), vm((qkv_w, tok), BF),
            vm((n_seq * heads, seq, seq), F32), vm((heads * hdim, tok), BF),
            vm((tok, hid), BF), vm((2, tok, hid), BF), vm(half, F32), vm(half, F32),
            vm(half, F32), vm(half, F32), vm(half, F32),
            vm((2,) + half, F32), vm((2,) + half, F32), vm((3,) + half, BF), vm((3,) + half, BF),
            vm((2,) + half, F32), vm(half, F32), vm(half, F32), vm((3, 256, hid), F32),
            dma((2, 2)), dma((2, 2)), dma((3, 2)), dma((3, 2)), dma((3, 2)), dma((3, 2)),
            dma((2,)), dma((2,)), dma((8,)), dma((8,)), dma((2,)), dma((2,)),
            dma((5, 2)), dma((5, 2)), dma((5, 2)), dma((3,)), dma((2, 4)), dma((2,)), dma((2,)), dma((2,)), dma((3,)), dma((2, 2)),
            pltpu.SemaphoreType.REGULAR,
        ]
        anyspec = pl.BlockSpec(memory_space=pl.ANY)
        outs = pl.pallas_call(
            functools.partial(chain_kernel, seq, hid, heads, hdim, n_pairs),
            out_shape=[sds(half[1:], F32), sds(half, BF), sds((tok, hid), F32), sds((tok, hid), BF)] + [sds((tok, hid), F32)] * 3
            + [sds((n_layers, qkv_w, hid), F32), sds((n_layers, heads * hdim, hid), F32), sds((n_layers, hid, ff), F32), sds((n_layers, ff, hid), F32)],
            in_specs=[anyspec] * 10,
            out_specs=[anyspec] * 11,
            scratch_shapes=scratch,
            name="chain",
            compiler_params=pltpu.CompilerParams(collective_id=0, has_side_effects=True, vmem_limit_bytes=67043328),
        )(flat(y_one), flat(y_two), flat(dy_one), flat(dy_two), flat(saved_one), flat(saved_two), wq_t, wo_t, w_in, w_out)
        f_own, j_own, f_all, j_all, x_two, d_one, d_two = outs[:7]
        cube = lambda arr: arr.reshape(n_seq, seq, hid)
        over_x = lambda arr: lax.ppermute(arr, "tp", [(0, 2), (2, 0), (1, 3), (3, 1)])
        over_core = lambda arr: lax.ppermute(arr, "tp", [(0, 1), (1, 0), (2, 3), (3, 2)])
        f_near, j_near = over_x(f_own), over_x(j_own)
        grads = move([out.reshape(-1, hid) for out in outs[7:]], "move_grads")
        f_near, j_near, grads = lax.optimization_barrier((f_near, j_near, grads))
        f_far, j_far = over_core(f_near), over_core(j_near)
        states = [cube(out) for out in move([x_two, d_one], "move_states")]
        x_one = take(finish_x, 2, "finish_x", (n_seq, seq, hid), [saved_one, cube(f_all)], f_near[None], f_far[None])
        dx_two = take(finish_d, 0, "finish_d", (n_seq, seq, hid), [cube(d_two), cube(x_two), cube(j_all)], j_near, j_far)
        d_qkv = jnp.transpose(grads[0].reshape(n_layers, 3, heads, hdim, hid), (0, 4, 1, 2, 3))
        d_o = grads[1].reshape(n_layers, heads, hdim, hid)
        return (x_one, *states, dx_two, d_qkv, d_o, grads[2].reshape(n_layers, hid, ff), grads[3].reshape(n_layers, ff, hid))

    return jax.shard_map(
        per_device,
        mesh=mesh,
        in_specs=(act_spec,) * 4 + (saved_spec,) * 2 + weight_specs,
        out_specs=(act_spec,) * 4 + grad_specs,
        check_vma=False,
    )
```

```python
import functools

import jax
import jax.numpy as jnp
from jax import lax
from jax.experimental import pallas as pl
from jax.experimental.pallas import tpu as pltpu
from jax.sharding import PartitionSpec as P

EPS = 1e-6
BF = jnp.bfloat16
F32 = jnp.float32
MESH = pl.DeviceIdType.MESH
GELU_C = 0.7978845608028654
GELU_A = 0.044715
GRANT = 40

NN = (((1,), (0,)), ((), ()))
NT = (((1,), (1,)), ((), ()))
TN = (((0,), (0,)), ((), ()))


def dot(lhs, rhs, dims):
    return lax.dot_general(lhs, rhs, dims, preferred_element_type=F32)


def rms_scale(state):
    return lax.rsqrt(jnp.mean(state * state, axis=-1, keepdims=True) + EPS)


def rms_pull(state, grad):
    scale = rms_scale(state)
    normed = state * scale
    return scale * (grad - normed * jnp.mean(normed * grad, axis=-1, keepdims=True))


def gelu_parts(hidden, want_grad):
    sq = hidden * hidden
    tanh = jnp.tanh(GELU_C * (hidden + GELU_A * (sq * hidden)))
    half = 0.5 * (1.0 + tanh)
    value = hidden * half
    if not want_grad:
        return value, None
    grad = half + 0.5 * hidden * (1.0 - tanh * tanh) * (GELU_C * (1.0 + 3.0 * GELU_A * sq))
    return value, grad


def chain_kernel(
    seq, hid, heads, hdim, n_pairs,
    y1, y2, dy1, dy2, s1, s2, wq_h, wo_h, wi_h, wu_h,
    f_own, j_own, fsum, jsum, ox2, od1, od2, gq, go, gi, gu,
    wq, wo, wi, wu, a_g, act, gp, dhb, finp, finr, qkvt, dqkvt, pt, ot,
    d1b, d2b, d1f, d2f, vbuf, x2r, xl, pbuf, e1r, xs, xr, gbuf, g1r, g2r, stage,
    e1s_s, e1r_s, e2s_s, e2r_s, e3s_s, e3r_s, g1s_s, g1r_s, g2s_s, g2r_s, g3s_s, g3r_s,
    os_s, or_s, ol_s, oo_s, w_s, xl_s, v_s, x2_s, st_s, d_s, gcred,
):
    me = lax.axis_index("tp")
    dp = lax.axis_index("dp")
    ci = lax.rem(me, 2)
    core_peer = (dp, me + 1 - 2 * ci)
    x_peer = (dp, lax.rem(me + 2, 4))
    qw = heads * hdim
    npc = 4
    prow = seq // npc

    barrier = pltpu.get_barrier_semaphore()
    pl.semaphore_signal(barrier, inc=1, device_id=core_peer, device_id_type=MESH)
    pl.semaphore_signal(barrier, inc=1, device_id=x_peer, device_id_type=MESH)

    def rows(seq_idx):
        return pl.ds(pl.multiple_of(seq_idx * seq, seq), seq)

    def mine(c):
        return 2 * c + ci

    def theirs(c):
        return 2 * c + 1 - ci

    def local(src, dst, sem):
        return pltpu.make_async_copy(src, dst, sem)

    def remote(src, dst, ssem, rsem, dev):
        return pltpu.make_async_remote_copy(src_ref=src, dst_ref=dst, send_sem=ssem, recv_sem=rsem, device_id=dev, device_id_type=MESH)

    def weight_copies(slot, blk, which):
        pairs = {"q": (wq_h, wq), "o": (wo_h, wo), "i": (wi_h, wi), "u": (wu_h, wu)}
        return [local(pairs[k][0].at[blk], pairs[k][1].at[slot], w_s.at[slot, "qoiu".index(k)]) for k in which]

    def w_start(slot, blk, which):
        for cp in weight_copies(slot, blk, which):
            cp.start()

    def w_wait(slot, which):
        for cp in weight_copies(slot, 0, which):
            cp.wait()

    def state_start(first, one, pair, rws, dst, sem):
        top, saved = (y1, s1) if one else (y2, s2)
        if first is True:
            local(top.at[rws], dst, sem).start()
        elif first is False:
            local(saved.at[pair, rws], dst, sem).start()
        else:
            @pl.when(first)
            def _():
                local(top.at[rws], dst, sem).start()

            @pl.when(jnp.logical_not(first))
            def _():
                local(saved.at[jnp.minimum(pair, n_pairs - 1), rws], dst, sem).start()

    def state_wait(dst, sem):
        local(y1.at[rows(0)], dst, sem).wait()

    def seq_start(first, one, pair, order=lambda i: i):
        for i in (0, 1):
            state_start(first, one, pair, rows(order(i)), xl.at[i], xl_s.at[i])

    def each_seq(first, one, pair, body, order=lambda i: i):
        @pl.loop(0, 4)
        def _(i):
            slot = lax.rem(i, 2)
            state_wait(xl.at[slot], xl_s.at[slot])
            body(i, order(i), xl[slot])

            @pl.when(i < 2)
            def _():
                state_start(first, one, pair, rows(order(i + 2)), xl.at[slot], xl_s.at[slot])

    def mlp_fwd(slot, lo=0, hi=4):
        @pl.loop(lo, hi)
        def _(s):
            value, grad = gelu_parts(dot(a_g[rows(s), :], wi[slot], NN), True)
            act[rows(s), :] = value.astype(BF)
            gp[rows(s), :] = grad

    def attn_fwd_seq(slot, fin, s):
        cols = rows(s)
        qkv = dot(wq[slot], fin[cols, :], NT).astype(BF)
        qkvt[:, cols] = qkv
        part = lambda j, h: qkv[j * qw + h * hdim:j * qw + (h + 1) * hdim]
        scores = [dot(part(1, h), part(0, h), TN) * (hdim ** -0.5) for h in range(heads)]
        exps = [jnp.exp(sc - jnp.max(sc, axis=0, keepdims=True)) for sc in scores]
        probs = [ex * (1.0 / jnp.sum(ex, axis=0, keepdims=True)) for ex in exps]
        for h in range(heads):
            pt[s * heads + h] = probs[h]
        for h in range(heads):
            ot[h * hdim:(h + 1) * hdim, cols] = dot(part(2, h), probs[h].astype(BF), NN).astype(BF)

    def attn_fwd_plain(pair):
        def body(i, s, state):
            finp[rows(s), :] = (state * rms_scale(state)).astype(BF)
            attn_fwd_seq(0, finp, s)
        each_seq(False, False, pair, body)

    def attn_fwd_rev():
        @pl.loop(0, 4)
        def _(s):
            attn_fwd_seq(1, finr, s)

    results = ((xs.at[2], jsum), (gbuf.at[:, 1], fsum), (x2r, ox2), (d1f, od1), (d2f, od2))

    def emit_copies(idx, c):
        ref, out = results[idx]
        rws = out.at[rows(mine(c))]
        return (
            local(ref.at[c], rws, ol_s.at[idx, c]),
            remote(ref.at[c], rws, os_s.at[idx, c], or_s.at[idx, c], core_peer),
        )

    def own_copy(c):
        return local(results[0][0].at[c], j_own.at[c], oo_s.at[c]) if c is not None else local(gbuf.at[1, 1], f_own, oo_s.at[2])

    def emit(idx, c):
        for cp in emit_copies(idx, c):
            cp.start()

    def emit_own(c):
        own_copy(c).start()

    def e1(slot, c):
        return remote(pbuf.at[c, 0], e1r.at[slot, c], e1s_s.at[slot, c], e1r_s.at[slot, c], core_peer)

    def e2(t, c):
        return remote(xs.at[t, c], xr.at[t, c], e2s_s.at[t, c], e2r_s.at[t, c], x_peer)

    def part_g(slot, ver, c, mode, e1_slot=None):
        for i, s in enumerate((theirs(c), mine(c))):
            d_act = dot(d2b[ver, rows(s), :], wu[slot], NT)
            dh = (d_act * gp[rows(s), :]).astype(BF)
            dhb[rows(s), :] = dh
            part = dot(dh, wi[slot], NT)
            pbuf[c, i] = pbuf[c, i] + part if mode == "add" else part
            if mode != "hold" and i == 0:
                e1(e1_slot, c).start()

    def part_f(slot, c, e1_slot):
        each = range(heads)
        for i, s in enumerate((theirs(c), mine(c))):
            cols = rows(s)
            do_t = dot(wo[slot], d1b[cols, :], NT).astype(BF)
            do = [do_t[h * hdim:(h + 1) * hdim] for h in each]
            part = lambda j, h: qkvt[j * qw + h * hdim:j * qw + (h + 1) * hdim, cols]
            probs = [pt[s * heads + h] for h in each]
            dps = [dot(part(2, h), do[h], TN) for h in each]
            dv = [dot(do[h], probs[h].astype(BF), NT).astype(BF) for h in each]
            ds = []
            for h in each:
                inner = jnp.sum(probs[h] * dps[h], axis=0, keepdims=True)
                ds.append((probs[h] * (dps[h] - inner) * (hdim ** -0.5)).astype(BF))
            dq = [dot(part(1, h), ds[h], NN).astype(BF) for h in each]
            dk = [dot(part(0, h), ds[h], NT).astype(BF) for h in each]
            d_qkv = jnp.concatenate(dq + dk + dv, axis=0)
            dqkvt[:, cols] = d_qkv
            pbuf[c, i] = dot(d_qkv, wq[slot], TN)
            if i == 0:
                e1(e1_slot, c).start()

    def to_x(t, c, e1_slot, last=None):
        e1(e1_slot, c).wait()
        xs[t, c] = (pbuf[c, 1] + e1r[e1_slot, c]).astype(BF)
        if last is None:
            e2(t, c).start()
        else:
            @pl.when(jnp.logical_not(last))
            def _():
                e2(t, c).start()

            @pl.when(last)
            def _():
                emit_own(c)
                emit(0, c)

    def summed(t, c):
        e2(t, c).wait()
        return xs[t, c].astype(F32) + xr[t, c].astype(F32)

    def e3(kind, c):
        ref = d1b.at[rows(mine(c))] if kind == 0 else d2b.at[kind - 1, rows(mine(c))]
        return remote(ref, ref, e3s_s.at[kind, c], e3r_s.at[kind, c], core_peer)

    def finish(t, c, kind, acc, state):
        total = acc[c] + rms_pull(state, summed(t, c))
        acc[c] = total
        if kind is not None:
            if kind == 0:
                d1b[rows(mine(c)), :] = total.astype(BF)
            else:
                d2b[kind - 1, rows(mine(c)), :] = total.astype(BF)
            e3(kind, c).start()

    def g1(c):
        return remote(gbuf.at[c, 0], g1r.at[c], g1s_s.at[c], g1r_s.at[c], core_peer)

    def g2(k):
        c, q = k // npc, k % npc
        rws = pl.ds(q * prow, prow)
        return remote(gbuf.at[c, 1, rws], g2r.at[c, rws], g2s_s.at[k], g2r_s.at[k], x_peer)

    def g_order(i):
        return 2 * (i // 2) + jnp.where(lax.rem(i, 2) == 0, 1 - ci, ci)

    def g_send_core(i):
        for c in (0, 1):
            @pl.when(i == 2 * c)
            def _():
                g1(c).start()

    def g_part(slot, first, pair, keep):
        def body(i, s, state):
            normed = (state * rms_scale(state)).astype(BF)
            a_g[rows(s), :] = normed
            value, grad = gelu_parts(dot(normed, wi[slot], NN), keep)
            value = value.astype(BF)
            if keep:
                act[rows(s), :] = value
                gp[rows(s), :] = grad
            gbuf[i // 2, lax.rem(i, 2)] = dot(value, wu[slot], NN)
            g_send_core(i)

            @pl.when(i == 2)
            def _():
                g_chip(0)
                g_send(*range(npc))
        each_seq(first, True, pair, body, g_order)
        g_chip(1)
        g_send(*range(npc, 2 * npc))

    def f_part(slot):
        @pl.loop(0, 4)
        def _(i):
            gbuf[i // 2, lax.rem(i, 2)] = dot(ot[:, rows(g_order(i))], wo[slot], TN)
            g_send_core(i)

    def g_chip(c):
        g1(c).wait()
        gbuf[c, 1] = gbuf[c, 1] + g1r[c]

    def g_send(*ks):
        for k in ks:
            g2(k).start()

    def g_total(c):
        for q in range(npc):
            g2(c * npc + q).wait()
        return gbuf[c, 1] + g2r[c]

    def g3(c):
        ref = finr.at[rows(mine(c))]
        return remote(ref, ref, g3s_s.at[c], g3r_s.at[c], core_peer)

    def g_finish(c):
        state_wait(x2r.at[c], x2_s.at[c])
        state = x2r[c] - g_total(c)
        x2r[c] = state
        finr[rows(mine(c)), :] = (state * rms_scale(state)).astype(BF)
        g3(c).start()

    def g_credit():
        pl.semaphore_signal(gcred, inc=1, device_id=x_peer, device_id_type=MESH)

    def put(pending, tile, dst, value):
        slot = tile % 3
        height = value.shape[0]
        if pending[slot] is not None:
            pending[slot].wait()
        stage[slot, :height] = value
        cp = local(stage.at[slot, pl.ds(0, height)], dst, st_s.at[slot])
        cp.start()
        pending[slot] = cp

    def flush(pending):
        for cp in pending:
            if cp is not None:
                cp.wait()

    def mlp_out_grads(blk, ver, pending):
        for k in range(hid // 256):
            put(pending, k, gu.at[blk, pl.ds(256 * k, 256)], dot(act[:, 256 * k:256 * (k + 1)], d2b[ver], TN))

    def mlp_in_grads(blk, pending):
        for k in range(hid // 256):
            put(pending, k, gi.at[blk, pl.ds(256 * k, 256)], dot(a_g[:, 256 * k:256 * (k + 1)], dhb[...], TN))

    def attn_grads(blk, fin, pending):
        for k in range(3):
            put(pending, k, gq.at[blk, pl.ds(qw * k, qw)], dot(dqkvt[qw * k:qw * (k + 1), :], fin[...], NN))
        put(pending, 3, go.at[blk], dot(ot[...], d1b[...], NN))

    def v_start(first, one, pair, c):
        state_start(first, one, pair, rows(mine(c)), vbuf.at[c], v_s.at[c])

    def v_wait(c):
        state_wait(vbuf.at[c], v_s.at[c])

    top = 2 * n_pairs
    w_start(1, top, "iu")
    seq_start(True, True, 0, g_order)
    for c in (0, 1):
        v_start(True, True, 0, c)
        state_start(True, False, 0, rows(mine(c)), x2r.at[c], x2_s.at[c])
        local(dy1.at[rows(mine(c))], d1f.at[c], d_s.at[0, c]).start()
        local(dy2.at[rows(mine(c))], d2f.at[c], d_s.at[1, c]).start()
    pl.semaphore_wait(barrier, 2)
    w_wait(1, "iu")
    w_start(1, top, "qo")
    g_part(1, True, 0, True)
    w_start(0, top - 1, "qoiu")
    for i in range(4):
        local(dy2.at[rows(i)], xl.at[i % 2], xl_s.at[i % 2]).start()
        state_wait(xl.at[i % 2], xl_s.at[i % 2])
        d2b[1, rows(i), :] = xl[i % 2].astype(BF)
    for c in (0, 1):
        local(dy1.at[rows(mine(c))], d1f.at[c], d_s.at[0, c]).wait()
        local(dy2.at[rows(mine(c))], d2f.at[c], d_s.at[1, c]).wait()

    @pl.loop(0, n_pairs + 1)
    def _(it):
        pair = n_pairs - it
        is_top = it == 0
        more = it < n_pairs
        rev = 2 * pair
        even, odd = lax.rem(it, 2), lax.rem(it + 1, 2)

        @pl.when(is_top)
        def _():
            @pl.loop(0, 2)
            def _(c):
                part_g(1, 1, c, "first", odd)
                to_x(1, c, odd)

        @pl.when(it > 0)
        def _():
            @pl.loop(0, 2)
            def _(c):
                v_wait(c)
                finish(0, c, 2, d2f, vbuf[c])
                v_start(False, True, pair, c)
                mlp_fwd(1, 2 * c, 2 * c + 2)
                e3(2, c).wait()
                part_g(1, 1, c, "add", odd)
                to_x(1, c, odd)

        @pl.when(more)
        def _():
            w_start(1, rev - 2, "iu")

        for c in (0, 1):
            g_finish(c)

        g_credit()

        @pl.when(jnp.logical_not(more))
        def _():
            for c in (0, 1):
                emit(2, c)
                emit(4, c)
        w_wait(1, "qo")
        for c in (0, 1):
            g3(c).wait()
        attn_fwd_rev()

        @pl.when(jnp.logical_not(more))
        def _():
            f_part(1)
            g_chip(0)
            pl.semaphore_wait(gcred, 1)
            g_send(*range(npc))
            g_chip(1)
            emit_own(None)
            emit(1, 1)

        pending = [None] * 3
        for c in (0, 1):
            v_wait(c)
            finish(1, c, 0, d1f, vbuf[c])

            @pl.when(jnp.logical_not(more))
            def _():
                emit(3, c)
            if c == 0:
                mlp_out_grads(rev, 1, pending)
            else:
                mlp_in_grads(rev, pending)
            e3(0, c).wait()
            part_f(1, c, even)
            to_x(2, c, even, jnp.logical_not(more))

        @pl.when(more)
        def _():
            seq_start(False, False, pair - 1)
        attn_grads(rev, finr, pending)
        flush(pending)

        @pl.when(more)
        def _():
            w_start(1, rev - 2, "qo")
            for c in (0, 1):
                v_start(False, False, pair - 1, c)
            w_wait(0, "qo")
            attn_fwd_plain(pair - 1)
            seq_start(False, True, pair - 1, g_order)

            @pl.loop(0, 2)
            def _(c):
                part_f(0, c, odd)
                to_x(0, c, odd)
            w_wait(1, "iu")
            pl.semaphore_wait(gcred, 1)
            g_part(1, False, pair - 1, False)
            w_wait(0, "iu")
            mlp_fwd(0)
            for c in (0, 1):
                finish(2, c, 1, d2f, x2r[c])
                state_start(False, False, pair - 1, rows(mine(c)), x2r.at[c], x2_s.at[c])
            @pl.loop(0, 2)
            def _(c):
                e3(1, c).wait()
                part_g(0, 0, c, "hold")

            @pl.when(it < n_pairs - 1)
            def _():
                w_start(0, rev - 3, "qoiu")
            later = [None] * 3
            mlp_out_grads(rev - 1, 0, later)
            mlp_in_grads(rev - 1, later)
            attn_grads(rev - 1, finp, later)
            flush(later)

    gbuf[0, 1] = g_total(0)
    emit(1, 0)
    for c in (0, 1, None):
        own_copy(c).wait()
    for c in (0, 1):
        for idx in range(5):
            for cp in emit_copies(idx, c):
                cp.wait()


def move_kernel(depth, chunk, *refs):
    count = (len(refs) - 3) // 2
    buf, in_s, out_s = refs[-3:]
    jobs = []
    for src, dst in zip(refs[:count], refs[count:2 * count]):
        for lo in range(0, src.shape[0], chunk):
            rws = pl.ds(lo, min(chunk, src.shape[0] - lo))
            slot = len(jobs) % depth
            part = buf.at[slot, pl.ds(0, rws.size)]
            jobs.append((
                pltpu.make_async_copy(src.at[rws], part, in_s.at[slot]),
                pltpu.make_async_copy(part, dst.at[rws], out_s.at[slot]),
            ))
    for load, _ in jobs[:depth]:
        load.start()
    lag = depth // 2
    for k in range(len(jobs)):
        jobs[k][0].wait()
        jobs[k][1].start()
        if k >= lag:
            jobs[k - lag][1].wait()
            if k - lag + depth < len(jobs):
                jobs[k - lag + depth][0].start()
    for k in range(max(len(jobs) - lag, 0), len(jobs)):
        jobs[k][1].wait()


def move(arrays, name, depth=12, chunk=576):
    width = arrays[0].shape[-1]
    size = sum(arr.size for arr in arrays)
    depth = min(depth, sum(-(-arr.shape[0] // chunk) for arr in arrays))
    anyspec = pl.BlockSpec(memory_space=pl.ANY)
    return pl.pallas_call(
        functools.partial(move_kernel, depth, chunk),
        out_shape=[jax.ShapeDtypeStruct(arr.shape, arr.dtype) for arr in arrays],
        in_specs=[anyspec] * len(arrays),
        out_specs=[anyspec] * len(arrays),
        scratch_shapes=[pltpu.VMEM((depth, chunk, width), F32), pltpu.SemaphoreType.DMA((depth,)), pltpu.SemaphoreType.DMA((depth,))],
        name=name,
        cost_estimate=pl.CostEstimate(flops=400 * size, bytes_accessed=8 * size, transcendentals=0),
        compiler_params=pltpu.CompilerParams(vmem_limit_bytes=60 * 2 ** 20),
    )(*arrays)


def take_kernel(finish, first, keep, *refs):
    *base, near_ref, far_ref, out_ref = refs[:-1] if keep else refs
    if keep:
        refs[-1][...] = base[1][...]
    seq_idx = pl.program_id(0)
    odd = lax.rem(seq_idx + lax.axis_index("tp"), 2)
    ready = seq_idx < first

    @pl.when(ready)
    def _():
        out_ref[...] = finish(None, *[ref[...] for ref in base])

    @pl.when(jnp.logical_not(ready) & (odd == 0))
    def _():
        out_ref[...] = finish(near_ref[...].astype(F32), *[ref[...] for ref in base])

    @pl.when(jnp.logical_not(ready) & (odd != 0))
    def _():
        out_ref[...] = finish(far_ref[...].astype(F32), *[ref[...] for ref in base])


def take(finish, first, name, shape, base, near, far, keep=False):
    n_seq, seq, hid = shape
    whole = pl.BlockSpec((1, seq, hid), lambda s: (s, 0, 0))
    bottom = pl.BlockSpec((None, 1, seq, hid), lambda s: (0, s, 0, 0))
    half = pl.BlockSpec((1, seq, hid), lambda s: (jnp.maximum(s - first, 0) // 2, 0, 0))
    return pl.pallas_call(
        functools.partial(take_kernel, finish, first, keep),
        out_shape=[jax.ShapeDtypeStruct(shape, F32)] * (1 + keep),
        grid=(n_seq,),
        in_specs=[whole if arr.ndim == 3 else bottom for arr in base] + [half, half],
        out_specs=[whole] * (1 + keep),
        name=name,
        cost_estimate=pl.CostEstimate(flops=40_000_000, bytes_accessed=16_000_000, transcendentals=0),
        compiler_params=pltpu.CompilerParams(vmem_limit_bytes=GRANT * 2 ** 20),
    )(*base, near, far)


def finish_x(other, state, own):
    return state - (own if other is None else own + other)


def finish_d(other, grad, state, own):
    own = own.astype(F32)
    return grad + rms_pull(state, own if other is None else own + other)


def solution(mesh):
    act_spec = P("dp", None, None)
    saved_spec = P(None, "dp", None, None)
    weight_specs = (P(None, None, None, "tp", None), P(None, "tp", None, None), P(None, None, "tp"), P(None, "tp", None))
    grad_specs = (P("dp", None, None, "tp", None), P("dp", "tp", None, None), P("dp", None, "tp"), P("dp", "tp", None))

    def per_device(y_one, y_two, dy_one, dy_two, saved_one, saved_two, w_qkv, w_o, w_in, w_out):
        n_seq, seq, hid = y_one.shape
        n_layers, _, _, heads, hdim = w_qkv.shape
        n_pairs = saved_one.shape[0]
        ff = w_in.shape[-1]
        tok = n_seq * seq
        qkv_w = 3 * heads * hdim
        flat = lambda arr: arr.reshape(arr.shape[:-3] + (tok, hid))
        wq_t = jnp.transpose(w_qkv, (0, 2, 3, 4, 1)).reshape(n_layers, qkv_w, hid)
        wo_t = w_o.reshape(n_layers, heads * hdim, hid)
        sds = jax.ShapeDtypeStruct
        vm = pltpu.VMEM
        dma = pltpu.SemaphoreType.DMA
        half = (2, seq, hid)
        scratch = [
            vm((2, qkv_w, hid), BF), vm((2, heads * hdim, hid), BF), vm((2, hid, ff), BF), vm((2, ff, hid), BF),
            vm((tok, hid), BF), vm((tok, ff), BF), vm((tok, ff), F32), vm((tok, ff), BF),
            vm((tok, hid), BF), vm((tok, hid), BF), vm((qkv_w, tok), BF), vm((qkv_w, tok), BF),
            vm((n_seq * heads, seq, seq), F32), vm((heads * hdim, tok), BF),
            vm((tok, hid), BF), vm((2, tok, hid), BF), vm(half, F32), vm(half, F32),
            vm(half, F32), vm(half, F32), vm(half, F32),
            vm((2,) + half, F32), vm((2,) + half, F32), vm((3,) + half, BF), vm((3,) + half, BF),
            vm((2,) + half, F32), vm(half, F32), vm(half, F32), vm((3, 256, hid), F32),
            dma((2, 2)), dma((2, 2)), dma((3, 2)), dma((3, 2)), dma((3, 2)), dma((3, 2)),
            dma((2,)), dma((2,)), dma((8,)), dma((8,)), dma((2,)), dma((2,)),
            dma((5, 2)), dma((5, 2)), dma((5, 2)), dma((3,)), dma((2, 4)), dma((2,)), dma((2,)), dma((2,)), dma((3,)), dma((2, 2)),
            pltpu.SemaphoreType.REGULAR,
        ]
        anyspec = pl.BlockSpec(memory_space=pl.ANY)
        outs = pl.pallas_call(
            functools.partial(chain_kernel, seq, hid, heads, hdim, n_pairs),
            out_shape=[sds(half[1:], F32), sds(half, BF), sds((tok, hid), F32), sds((tok, hid), BF)] + [sds((tok, hid), F32)] * 3
            + [sds((n_layers, qkv_w, hid), F32), sds((n_layers, heads * hdim, hid), F32), sds((n_layers, hid, ff), F32), sds((n_layers, ff, hid), F32)],
            in_specs=[anyspec] * 10,
            out_specs=[anyspec] * 11,
            scratch_shapes=scratch,
            name="chain",
            compiler_params=pltpu.CompilerParams(collective_id=0, has_side_effects=True, vmem_limit_bytes=67043328),
        )(flat(y_one), flat(y_two), flat(dy_one), flat(dy_two), flat(saved_one), flat(saved_two), wq_t, wo_t, w_in, w_out)
        f_own, j_own, f_all, j_all, x_two, d_one, d_two = outs[:7]
        cube = lambda arr: arr.reshape(n_seq, seq, hid)
        over_x = lambda arr: lax.ppermute(arr, "tp", [(0, 2), (2, 0), (1, 3), (3, 1)])
        over_core = lambda arr: lax.ppermute(arr, "tp", [(0, 1), (1, 0), (2, 3), (3, 2)])
        f_near, j_near = over_x(f_own), over_x(j_own)
        grads = move([out.reshape(-1, hid) for out in outs[7:]], "move_grads")
        f_near, j_near, grads = lax.optimization_barrier((f_near, j_near, grads))
        f_far, j_far = over_core(f_near), over_core(j_near)
        d_one = cube(move([d_one], "move_states")[0])
        x_one, = take(finish_x, 2, "finish_x", (n_seq, seq, hid), [saved_one, cube(f_all)], f_near[None], f_far[None])
        dx_two, x_two = take(finish_d, 0, "finish_d", (n_seq, seq, hid), [cube(d_two), cube(x_two), cube(j_all)], j_near, j_far, keep=True)
        d_qkv = jnp.transpose(grads[0].reshape(n_layers, 3, heads, hdim, hid), (0, 4, 1, 2, 3))
        d_o = grads[1].reshape(n_layers, heads, hdim, hid)
        return (x_one, x_two, d_one, dx_two, d_qkv, d_o, grads[2].reshape(n_layers, hid, ff), grads[3].reshape(n_layers, ff, hid))

    return jax.shard_map(
        per_device,
        mesh=mesh,
        in_specs=(act_spec,) * 4 + (saved_spec,) * 2 + weight_specs,
        out_specs=(act_spec,) * 4 + grad_specs,
        check_vma=False,
    )
```
